256 devices in a mesh: dp: 8 (over z), seq: 32 (over x, y, core).
Axes of the slice: x: 4, y: 4, z: 8, core: 2. Of those that a mesh axis runs over, the one named last changes fastest.
Arguments:
- queries: bfloat16 [8, 8192, 512], P('dp', 'seq'), may hold values from -0.62890625 to 0.62890625
- keys: bfloat16 [8, 8192, 512], P('dp', 'seq'), may hold values from -0.62890625 to 0.62890625
- values: bfloat16 [8, 8192, 512], P('dp', 'seq'), may hold values from -6 to 6
- level_weights: float32 [8, 8, 4, 8192], P('dp', None, None, 'seq'), may hold values from 0.25 to 4
- proj: bfloat16 [512, 2048], P(None, 'seq'), may hold values from -0.25 to 0.25
- out_grad: bfloat16 [8, 8192, 2048], P('dp', 'seq'), may hold values from -0.59765625 to 0.59765625
Outputs:
- attended_out: bfloat16 [8, 8192, 2048], P('dp', 'seq')
- grad_queries: bfloat16 [8, 8192, 512], P('dp', 'seq')
- grad_keys: bfloat16 [8, 8192, 512], P('dp', 'seq')
- grad_values: bfloat16 [8, 8192, 512], P('dp', 'seq')
- grad_levels: float32 [8, 8, 4, 8192], P('dp', None, None, 'seq')
- grad_proj: float32 [512, 2048], P(None, 'seq')
The draws below stay inside these ranges and needn't reach their ends.
All inputs are finite; a program needn't handle non-finite values.
Results may differ from the reference program's by a relative error of at most 0.0064.
Values may be sent and summed in bfloat16 or wider, within the bound.
A program may use at most 64 MiB of HBM per device.

```python
import math
import jax
import jax.numpy as jnp
from jax import lax

HEADS = 4
HEAD_DIM = 128
DOUT = 2048
LOCAL_BITS = 2
STRETCH = 64
WIDTH = 512
TOK_DEV = 256
DEV_BITS = 5
LEVELS = 8
TOKENS = 8192
BATCH = 8
N_SEQ = 32


def with_spikes(array, rng, source, target, shards_of, factor):
    def block_of(dim):
        return (jnp.arange(array.shape[dim]) // (array.shape[dim] // shards_of)).reshape((-1,) + (1,) * (array.ndim - 1 - dim))

    near = jax.random.permutation(rng, shards_of)[block_of(target)]
    far = (block_of(target) + shards_of // 2) % shards_of
    return jnp.where((block_of(source) == near) | (block_of(source) == far), factor * array, array)


def levels(rng, extent, cuts, low, high):
    def one(axis_at, shards_of):
        heights = jax.random.uniform(jax.random.fold_in(jax.random.fold_in(rng, 6), axis_at), (shards_of,), jnp.float32, low / len(cuts), high / len(cuts))
        return jnp.repeat(jnp.exp(heights), extent[axis_at] // shards_of).reshape((-1,) + (1,) * (len(extent) - axis_at - 1))

    loudness = one(*cuts[0])
    for cut in cuts[1:]:
        loudness = loudness * one(*cut)
    return loudness


def noise(stream_key, dims, spread, bound, split=(), dtype=jnp.bfloat16):
    factor_of = levels(stream_key, dims, split, -0.22, 0.18) if split else 1.0
    array = jax.random.normal(stream_key, dims, jnp.float32) * spread * factor_of
    return jnp.minimum(jnp.maximum(array, -bound), bound).astype(dtype)


def gaussian_with(own_key, shape, deviation, most, split, heavy, dtype=jnp.bfloat16):
    result = deviation * jax.random.normal(own_key, shape, jnp.float32)
    if split:
        result = result * levels(own_key, shape, split, -0.22, 0.18)
    return jnp.clip(with_spikes(result, jax.random.fold_in(own_key, 3), *heavy), -most, most).astype(dtype)


def setup_inputs(seed: int = 0) -> dict:
    streams_of = jax.random.split(jax.random.key(seed), 7)
    queries = noise(streams_of[0], (BATCH, TOKENS, WIDTH), (1.0 / TOKENS ** 0.25), 0.62890625, ((0, 8), (1, 32)))
    keys = noise(streams_of[1], (BATCH, TOKENS, WIDTH), (1.0 / TOKENS ** 0.25), 0.62890625, ((0, 8), (1, 32)))
    values = noise(streams_of[2], (BATCH, TOKENS, WIDTH), 1.0, 6.0, ((0, 8), (1, 32)))
    level_weights = jnp.clip(jnp.exp(math.log(4.0) - 2.7725887 * jax.random.uniform(streams_of[3], (BATCH, LEVELS, HEADS, TOKENS), jnp.float32) ** levels(streams_of[3], (BATCH, LEVELS, HEADS, TOKENS), ((0, 8), (3, 32)), -0.2, 0.2)), 0.25, 4.0)
    proj = noise(streams_of[4], (WIDTH, DOUT), WIDTH ** -0.5, 0.25, ((1, 32),))
    out_grad = gaussian_with(streams_of[5], (BATCH, TOKENS, DOUT), 0.1, 0.59765625, ((0, 8), (1, 32)), (1, 2, 32, 2.75))
    return {"queries": queries, "keys": keys, "values": values, "level_weights": level_weights, "proj": proj, "out_grad": out_grad}


def level_table(length, stretch, local_bits):
    place = lax.iota(jnp.int32, length)
    blocks = place // stretch
    apart = jnp.bitwise_xor(blocks[:, None], blocks[None, :])
    table = jnp.zeros((length, length), jnp.int32)
    for bit in range(local_bits):
        table = table + (apart >= (1 << bit)).astype(jnp.int32)
    causal = place[:, None] >= place[None, :]
    return table, causal


def local_weights(lam, table, causal, local_bits):
    weights = jnp.zeros((lam.shape[1], table.shape[0], table.shape[1]), jnp.float32)
    for level in range(local_bits + 1):
        weights = weights + jnp.where(table[None] == level, lam[level][:, :, None], jnp.float32(0))
    return jnp.where(causal[None], weights, jnp.float32(0))


def bucket_masks(count, bits):
    spans = lax.iota(jnp.int32, count)
    rows = []
    for bit in range(bits):
        upper = jnp.right_shift(spans, bit + 1)
        marked = jnp.bitwise_and(jnp.right_shift(spans, bit), 1)
        inside = (upper[:, None] == upper[None, :]) & (marked[:, None] == 1) & (marked[None, :] == 0)
        rows.append(inside.astype(jnp.float32))
    return jnp.stack(rows)


def span_forward(query, key, value, lam, states):
    scale = HEAD_DIM ** -0.5
    table, causal = level_table(TOK_DEV, STRETCH, LOCAL_BITS)
    qf = query.astype(jnp.float32)
    kf = key.astype(jnp.float32)
    vf = value.astype(jnp.float32)
    scores = jnp.einsum('thd,shd->hts', qf, kf)
    weights = local_weights(lam, table, causal, LOCAL_BITS)
    probs = (scale * weights * scores).astype(jnp.bfloat16)
    total = jnp.einsum('hts,shd->thd', probs.astype(jnp.float32), vf)
    cross = jnp.zeros_like(total)
    mapped = []
    for bit in range(DEV_BITS):
        image = jnp.einsum('thi,hij->thj', qf, states[bit].astype(jnp.float32))
        mapped.append(image)
        cross = cross + lam[LOCAL_BITS + 1 + bit].T[:, :, None] * image
    attended = (total + scale * cross).astype(jnp.bfloat16)
    return attended, scores, weights, probs, mapped, table, causal


def span_backward(query, key, value, lam, states, grad_att):
    scale = HEAD_DIM ** -0.5
    attended, scores, weights, probs, mapped, table, causal = span_forward(query, key, value, lam, states)
    qf = query.astype(jnp.float32)
    kf = key.astype(jnp.float32)
    vf = value.astype(jnp.float32)
    gf = grad_att.astype(jnp.float32)
    dprob = jnp.einsum('thd,shd->hts', gf, vf)
    product = jnp.where(causal[None], scale * scores * dprob, jnp.float32(0))
    grads = [jnp.sum(jnp.where(table[None] == level, product, jnp.float32(0)), axis=2) for level in range(LOCAL_BITS + 1)]
    dscore = (scale * weights * dprob).astype(jnp.bfloat16)
    dq = jnp.einsum('hts,shd->thd', dscore.astype(jnp.float32), kf)
    dk = jnp.einsum('hts,thd->shd', dscore.astype(jnp.float32), qf)
    dv = jnp.einsum('hts,thd->shd', probs.astype(jnp.float32), gf)
    updates = []
    for bit in range(DEV_BITS):
        grads.append(scale * jnp.sum(gf * mapped[bit], axis=2).T)
        weighted = (scale * lam[LOCAL_BITS + 1 + bit].T[:, :, None] * gf).astype(jnp.bfloat16)
        updates.append(jnp.einsum('thi,thj->hij', qf, weighted.astype(jnp.float32)))
        dq = dq + jnp.einsum('thj,hij->thi', weighted.astype(jnp.float32), states[bit].astype(jnp.float32))
    return dq, dk, dv, jnp.stack(grads), jnp.stack(updates)


def one_sequence(query, key, value, lam, grad_out, proj):
    shape = (N_SEQ, TOK_DEV, HEADS, HEAD_DIM)
    qs = query.reshape(shape)
    ks = key.reshape(shape)
    vs = value.reshape(shape)
    lams = lam.reshape(LEVELS, HEADS, N_SEQ, TOK_DEV).transpose(2, 0, 1, 3)
    totals = jnp.einsum('nshi,nshj->nhij', ks.astype(jnp.float32), vs.astype(jnp.float32))
    masks = bucket_masks(N_SEQ, DEV_BITS)
    states = jnp.einsum('bnm,mhij->nbhij', masks, totals, precision=lax.Precision.HIGHEST).astype(jnp.bfloat16)
    attended = lax.map(lambda x: span_forward(*x)[0], (qs, ks, vs, lams, states))
    attended = attended.reshape(TOKENS, WIDTH)
    out = jnp.dot(attended, proj, preferred_element_type=jnp.float32).astype(jnp.bfloat16)
    grad_att = lax.dot_general(grad_out, proj, (((1,), (1,)), ((), ())), preferred_element_type=jnp.float32).astype(jnp.bfloat16)
    grad_proj = lax.dot_general(attended, grad_out, (((0,), (0,)), ((), ())), preferred_element_type=jnp.float32)
    dq, dk, dv, dlam, updates = lax.map(lambda x: span_backward(*x), (qs, ks, vs, lams, states, grad_att.reshape(shape)))
    returned = jnp.einsum('bnm,nbhij->mhij', masks, updates, precision=lax.Precision.HIGHEST).astype(jnp.bfloat16)
    dk = dk + jnp.einsum('nshj,nhij->nshi', vs.astype(jnp.float32), returned.astype(jnp.float32))
    dv = dv + jnp.einsum('nshi,nhij->nshj', ks.astype(jnp.float32), returned.astype(jnp.float32))
    dlam = dlam.transpose(1, 2, 0, 3).reshape(LEVELS, HEADS, TOKENS)
    return (out, dq.astype(jnp.bfloat16).reshape(TOKENS, WIDTH), dk.astype(jnp.bfloat16).reshape(TOKENS, WIDTH),
            dv.astype(jnp.bfloat16).reshape(TOKENS, WIDTH), dlam, grad_proj)


def reference(queries, keys, values, level_weights, proj, out_grad):
    out, dq, dk, dv, dlam, pieces = lax.map(lambda x: one_sequence(x[0], x[1], x[2], x[3], x[4], proj),
                                            (queries, keys, values, level_weights, out_grad))
    return out, dq, dk, dv, dlam, jnp.sum(pieces, axis=0)
```

```python
import functools

import jax
import jax.numpy as jnp
from jax import lax
from jax.experimental import pallas as pl
from jax.experimental.pallas import tpu as pltpu
from jax.sharding import PartitionSpec as P

BF = jnp.bfloat16
F32 = jnp.float32
MESH = pl.DeviceIdType.MESH
COL = 8
PIECES = 16


def place():
    s = lax.axis_index("seq")
    bits = [lax.rem(lax.div(s, 2**b), 2) for b in range(5)]
    return s, bits


def flipped(s, bits, mask):
    peer = s
    for b in range(5):
        if mask >> b & 1:
            peer = peer + 2**b * (1 - 2 * bits[b])
    return peer


def chip_offsets(s, bits):
    c, y0, y1, x0, x1 = bits
    dy0, dy1 = 2 * (1 - 2 * y0), 4 * (1 - 2 * y1)
    dx0, dx1 = 8 * (1 - 2 * x0), 16 * (1 - 2 * x1)
    da0, da1 = dy0 * (1 - c) + dx0 * c, dy1 * (1 - c) + dx1 * c
    db0, db1 = dx0 * (1 - c) + dy0 * c, dx1 * (1 - c) + dy1 * c

    def off(a, b):
        return s + (a & 1) * da0 + (a >> 1) * da1 + (b & 1) * db0 + (b >> 1) * db1

    return off


def rows(index, count):
    return pl.ds(pl.multiple_of(index * count, count), count)


def send(src, dst, ssem, rsem, device):
    return pltpu.make_async_remote_copy(
        src_ref=src, dst_ref=dst, send_sem=ssem, recv_sem=rsem, device_id=device, device_id_type=MESH
    )


def greet(devices):
    barrier = pltpu.get_barrier_semaphore()
    for device in devices:
        pl.semaphore_signal(barrier, inc=1, device_id=device, device_id_type=MESH)
    pl.semaphore_wait(barrier, len(devices))


def bit_of(bits, b, mask):
    return 1 - bits[b] if mask >> b & 1 else bits[b]


def kernel_a(
    k_ref, v_ref, shard_ref, full_ref, states_ref,
    tot, col, pair, quad, csum, xin, s3buf, s4buf,
    ag_s, ag_r, c1_s, c1_r, st_s, st_r, x_s, x_r, sib_s, sib_r,
):
    s, bits = place()
    c, y0, y1, x0, x1 = bits
    r = lax.rem(s, COL)
    off = chip_offsets(s, bits)
    greet(
        [{"seq": flipped(s, bits, m)} for m in range(1, 8)]
        + [{"seq": flipped(s, bits, m << 3)} for m in range(1, 4)]
    )
    sibling = {"seq": flipped(s, bits, 1)}
    open_sends = []

    def block(index):
        return full_ref.at[rows(index, 64)]

    def ag(slot, src, index, device):
        cp = send(src, block(index), ag_s.at[slot], ag_r.at[slot], device)
        cp.start()
        open_sends.append(cp)

    def ag_arrived(slot):
        send(shard_ref, block(s), ag_s.at[slot], ag_r.at[slot], sibling).wait_recv()

    full_ref[rows(s, 64)] = shard_ref[...]
    for a in (1, 3, 2):
        ag(a, shard_ref, s, {"seq": off(a, 0)})
    for b in (1, 3):
        ag(4 + b, shard_ref, s, {"seq": off(0, b)})
    ag(20, shard_ref, s, sibling)

    for h in range(4):
        lanes = pl.ds(128 * h, 128)
        tot[pl.ds(128 * h, 128)] = lax.dot_general(
            k_ref[:, lanes], v_ref[:, lanes], (((0,), (0,)), ((), ())), preferred_element_type=F32
        ).astype(BF)
    first = []
    for m in (4, 5, 2, 3, 6, 7, 1):
        peer = flipped(s, bits, m)
        cp = send(tot.at[rows(lax.rem(peer, COL), 64)], col.at[m], c1_s.at[m], c1_r.at[m], {"seq": peer})
        cp.start()
        first.append(cp)
    sib = send(tot, states_ref.at[0], sib_s, sib_r, sibling)

    @pl.when(c == 0)
    def _():
        sib.start()

    for a in (1, 3, 2):
        ag_arrived(a)
        for b in (1, 3):
            ag(4 + 4 * a + b, block(off(a, 0)), off(a, 0), {"seq": off(0, b)})
        ag(20 + 4 * a, block(off(a, 0)), off(a, 0), sibling)

    for cp in first:
        cp.wait_recv()
    col[0] = tot[rows(r, 64)]
    t = [col[m].astype(F32) for m in range(COL)]
    p = [t[2 * i] + t[2 * i + 1] for i in range(4)]
    q = [p[0] + p[1], p[2] + p[3]]
    csum[...] = q[0] + q[1]
    xsend = []
    for m in range(1, 4):
        cp = send(csum, xin.at[m], x_s.at[m], x_r.at[m], {"seq": flipped(s, bits, m << 3)})
        xsend.append(cp)
    x_out = [x0 == 0, x1 == 0, x1 == 0]
    x_into = [x0 == 1, x1 == 1, x1 == 1]
    for cp, cond in zip(xsend, x_out):

        @pl.when(cond)
        def _(cp=cp):
            cp.start()

    for i in range(4):
        pair[i] = p[i].astype(BF)
    for i in range(2):
        quad[i] = q[i].astype(BF)

    mine = rows(r, 64)

    def spread(j, m, src):
        return send(
            src, states_ref.at[j, mine], st_s.at[j, m], st_r.at[j, m], {"seq": flipped(s, bits, m)}
        )

    order = (1, 4, 5, 2, 3, 6, 7)
    early = []
    for m in order:
        early.append((spread(1, m, pair.at[(m >> 1) ^ 1]), bit_of(bits, 1, m) == 1))
        early.append((spread(2, m, quad.at[(m >> 2) ^ 1]), bit_of(bits, 2, m) == 1))
    for cp, cond in early:

        @pl.when(cond)
        def _(cp=cp):
            cp.start()

    have = [c == 1, y0 == 1, y1 == 1, x0 == 1, x1 == 1]
    for j in range(5):

        @pl.when(jnp.logical_not(have[j]))
        def _(j=j):
            states_ref[j] = jnp.zeros((512, 128), BF)

    @pl.when(have[1])
    def _():
        states_ref[1, mine] = pair[1]

    @pl.when(have[2])
    def _():
        states_ref[2, mine] = quad[1]

    def second(a):
        for b in (1, 3):
            ag_arrived(4 + 4 * a + b)
            if (b == 1) == (a < 2):
                ag(4 + 4 * a + 2, block(off(a, b)), off(a, b), {"seq": off(0, 4 - b)})
            ag(20 + 4 * a + b, block(off(a, b)), off(a, b), sibling)

    second(0)

    late3 = [spread(3, m, s3buf) for m in order]
    late4 = [spread(4, m, s4buf) for m in order]

    @pl.when(have[3])
    def _():
        xsend[0].wait_recv()
        s3buf[...] = xin[1].astype(BF)
        for cp in late3:
            cp.start()
        states_ref[3, mine] = s3buf[...]

    @pl.when(have[4])
    def _():
        xsend[1].wait_recv()
        xsend[2].wait_recv()
        s4buf[...] = (xin[2] + xin[3]).astype(BF)
        for cp in late4:
            cp.start()
        states_ref[4, mine] = s4buf[...]

    for a in (1, 3, 2):
        second(a)
    for a in (0, 1, 3, 2):
        ag_arrived(4 + 4 * a + 2)
        ag(20 + 4 * a + 2, block(off(a, 2)), off(a, 2), sibling)

    @pl.when(have[0])
    def _():
        sib.wait_recv()

    @pl.when(c == 0)
    def _():
        sib.wait_send()

    for cp, cond in early:

        @pl.when(cond)
        def _(cp=cp):
            cp.wait_send()

    for j in range(1, 5):

        @pl.when(have[j])
        def _(j=j):
            for m in order:
                spread(j, m, s4buf).wait_recv()
            if j == 3:
                for cp in late3:
                    cp.wait_send()
            if j == 4:
                for cp in late4:
                    cp.wait_send()

    for cp, cond in zip(xsend, x_out):

        @pl.when(cond)
        def _(cp=cp):
            cp.wait_send()

    for cp in first:
        cp.wait_send()
    for a in range(4):
        for b in range(4):
            ag_arrived(20 + 4 * a + b)
    for cp in open_sends:
        cp.wait_send()


def vmem():
    return pl.BlockSpec(memory_space=pltpu.VMEM)


def gather_states(key, value, shard):
    dma = pltpu.SemaphoreType.DMA
    return pl.pallas_call(
        kernel_a,
        out_shape=(
            jax.ShapeDtypeStruct((2048, 512), BF),
            jax.ShapeDtypeStruct((5, 512, 128), BF),
        ),
        in_specs=[vmem()] * 3,
        out_specs=(vmem(), vmem()),
        scratch_shapes=[
            pltpu.VMEM((512, 128), BF),
            pltpu.VMEM((COL, 64, 128), BF),
            pltpu.VMEM((4, 64, 128), BF),
            pltpu.VMEM((2, 64, 128), BF),
            pltpu.VMEM((64, 128), F32),
            pltpu.VMEM((4, 64, 128), F32),
            pltpu.VMEM((64, 128), BF),
            pltpu.VMEM((64, 128), BF),
            dma((36,)), dma((36,)), dma((COL,)), dma((COL,)),
            dma((5, COL)), dma((5, COL)), dma((4,)), dma((4,)), dma, dma,
        ],
        compiler_params=pltpu.CompilerParams(collective_id=0, has_side_effects=True),
        name="gather_states",
    )(key, value, shard)


def kernel_b(
    u_ref, g_ref, ret_ref, gp_ref,
    ucol, asend, xin, rsend, rcol, usib,
    gsib, hbuf, rel, fin, gbuf, xg, zf, zsend, zin, zall,
    u_s, u_r, ux_s, ux_r, ur_s, ur_r, us_s, us_r,
    gs_s, gs_r, rl_s, rl_r, fn_s, fn_r, gx_s, gx_r, z1_s, z1_r, z2_s, z2_r,
):
    s, bits = place()
    c, y0, y1, x0, x1 = bits
    z = lax.axis_index("dp")
    zbits = [lax.rem(lax.div(z, 2**b), 2) for b in range(3)] + [0, 0]
    r = lax.rem(s, COL)
    off = chip_offsets(s, bits)
    greet(
        [{"seq": flipped(s, bits, m)} for m in range(1, 8)]
        + [{"seq": flipped(s, bits, m << 3)} for m in range(1, 4)]
        + [{"dp": flipped(z, zbits, m)} for m in range(1, 8)]
    )
    sib_index = flipped(s, bits, 1)
    sibling = {"seq": sib_index}
    flip = sib_index - s

    gs = []
    for a in (2, 1, 3, 0):
        for b in range(4):
            slot = 4 * b + a
            cp = send(
                g_ref.at[rows(off(a, b) + flip, 64)], gsib.at[slot], gs_s.at[slot], gs_r.at[slot], sibling
            )
            cp.start()
            gs.append(cp)

    order = (4, 5, 2, 3, 6, 7, 1)
    have = [c == 1, y0 == 1, y1 == 1, x0 == 1, x1 == 1]
    usend = send(u_ref.at[0], usib, us_s, us_r, sibling)

    @pl.when(have[0])
    def _():
        usend.start()

    def slice_to(j, m):
        peer = flipped(s, bits, m)
        return send(
            u_ref.at[j, rows(lax.rem(peer, COL), 64)], ucol.at[j - 1, m], u_s.at[j - 1, m], u_r.at[j - 1, m], {"seq": peer}
        )

    for j in (4, 3, 2, 1):

        @pl.when(have[j])
        def _(j=j):
            for m in order:
                slice_to(j, m).start()

    def gs_arrived(a, b):
        slot = 4 * a + b
        send(g_ref.at[pl.ds(0, 64)], gsib.at[slot], gs_s.at[slot], gs_r.at[slot], sibling).wait_recv()

    def h_make(a, b):
        gs_arrived(a, b)
        hbuf[a, b] = (g_ref[rows(off(a, b), 64)].astype(F32) + gsib[4 * a + b].astype(F32)).astype(BF)

    dev_a = {1: {"seq": off(1, 0)}, 3: {"seq": off(3, 0)}}
    for b in range(4):
        h_make(2, b)
    rl = {
        1: send(hbuf.at[2, pl.ds(0, 2)], rel.at[0], rl_s.at[0], rl_r.at[0], dev_a[1]),
        3: send(hbuf.at[2, pl.ds(2, 2)], rel.at[1], rl_s.at[1], rl_r.at[1], dev_a[3]),
    }
    rl[1].start()
    rl[3].start()

    def final(m, half):
        k = 2 * (m // 2) + half
        return send(
            hbuf.at[m, pl.ds(2 * half, 2)], fin.at[m // 2, pl.ds(2 * half, 2)], fn_s.at[k], fn_r.at[k], dev_a[m]
        )

    h_make(1, 0)
    h_make(1, 1)
    f10 = final(1, 0)
    f10.start()
    h_make(3, 2)
    h_make(3, 3)
    f31 = final(3, 1)
    f31.start()

    for j in range(1, 5):
        for m in range(COL):
            if j == 1:
                cond = bit_of(bits, 1, m) == 1
            elif j == 2:
                cond = bit_of(bits, 2, m) == 1
            else:
                cond = have[j]

            @pl.when(cond)
            def _(j=j, m=m):
                if m:
                    slice_to(j, m).wait_recv()
                else:
                    ucol[j - 1, 0] = u_ref[j, rows(r, 64)]

            @pl.when(jnp.logical_not(cond))
            def _(j=j, m=m):
                ucol[j - 1, m] = jnp.zeros((64, 128), BF)

    def total(j, ms):
        value = ucol[j - 1, ms[0]].astype(F32)
        for m in ms[1:]:
            value = value + ucol[j - 1, m].astype(F32)
        return value

    asend[0] = total(3, list(range(COL)))
    asend[1] = total(4, list(range(COL)))
    ux = [
        send(asend.at[0 if m == 1 else 1], xin.at[m], ux_s.at[m], ux_r.at[m], {"seq": flipped(s, bits, m << 3)})
        for m in range(1, 4)
    ]
    ux_out = [x0 == 1, x1 == 1, x1 == 1]
    for cp, cond in zip(ux, ux_out):

        @pl.when(cond)
        def _(cp=cp):
            cp.start()

    for b in range(2):
        h_make(3, b)
    rl[1].wait_recv()
    for b in range(2):
        hbuf[3, b] = (hbuf[3, b].astype(F32) + rel[0, b].astype(F32)).astype(BF)
    f30 = final(3, 0)
    f30.start()
    for b in range(2):
        h_make(1, 2 + b)
    rl[3].wait_recv()
    for b in range(2):
        hbuf[1, 2 + b] = (hbuf[1, 2 + b].astype(F32) + rel[1, b].astype(F32)).astype(BF)
    f11 = final(1, 1)
    f11.start()

    for cp, cond, m in zip(ux, ux_out, range(1, 4)):

        @pl.when(jnp.logical_not(cond))
        def _(cp=cp):
            cp.wait_recv()

        @pl.when(cond)
        def _(m=m):
            xin[m] = jnp.zeros((64, 128), F32)

    far = xin[1] + xin[2] + xin[3]
    for i in range(4):
        near = total(1, [2 * (i ^ 1), 2 * (i ^ 1) + 1])
        k = 4 * ((i >> 1) ^ 1)
        mid = total(2, [k, k + 1, k + 2, k + 3])
        rsend[i] = (far + near + mid).astype(BF)
    mine = rows(r, 64)
    rc = []
    for m in order:
        cp = send(rsend.at[m >> 1], rcol.at[mine], ur_s.at[m], ur_r.at[m], {"seq": flipped(s, bits, m)})
        cp.start()
        rc.append(cp)
    rcol[mine] = rsend[0]

    for b in range(4):
        h_make(0, b)
    for k, cp in ((0, f10), (1, f11), (2, f30), (3, f31)):
        cp.wait_recv()
    for b in range(4):
        gbuf[b] = (hbuf[0, b].astype(F32) + fin[0, b].astype(F32) + fin[1, b].astype(F32)).astype(BF)
    gx = []
    for b in (2, 1, 3):
        cp = send(gbuf.at[b], xg.at[b], gx_s.at[b], gx_r.at[b], {"seq": off(0, b)})
        cp.start()
        gx.append(cp)

    for cp in rc:
        cp.wait_recv()

    @pl.when(c == 0)
    def _():
        usend.wait_recv()

    @pl.when(have[0])
    def _():
        usib[...] = jnp.zeros((512, 128), BF)

    ret_ref[...] = (rcol[...].astype(F32) + usib[...].astype(F32)).astype(BF)

    for cp in gx:
        cp.wait_recv()
    mean = gbuf[0].astype(F32) + xg[1].astype(F32) + xg[2].astype(F32) + xg[3].astype(F32)
    for i in range(8):
        part = mean[16 * (i // 2) : 16 * (i // 2) + 16, 256 * (i % 2) : 256 * (i % 2) + 256]
        zf[i] = part
        zsend[i] = part.astype(BF)
    z1 = []
    for m in (4, 3, 5, 2, 6, 1, 7):
        peer = flipped(z, zbits, m)
        cp = send(zsend.at[peer], zin.at[m], z1_s.at[m], z1_r.at[m], {"dp": peer})
        cp.start()
        z1.append(cp)
    for cp in z1:
        cp.wait_recv()
    value = zf[z]
    for m in range(1, 8):
        value = value + zin[m].astype(F32)
    zall[z] = value.astype(BF)
    z2 = []
    for m in (4, 3, 5, 2, 6, 1, 7):
        cp = send(zall.at[z], zall.at[z], z2_s.at[m], z2_r.at[m], {"dp": flipped(z, zbits, m)})
        cp.start()
        z2.append(cp)
    for cp in z2:
        cp.wait_recv()
    for i in range(8):
        gp_ref[pl.ds(16 * (i // 2), 16), pl.ds(256 * (i % 2), 256)] = zall[i].astype(F32)

    for cp in gs + [rl[1], rl[3], f10, f11, f30, f31] + rc + gx + z1 + z2:
        cp.wait_send()
    for cp, cond in zip(ux, ux_out):

        @pl.when(cond)
        def _(cp=cp):
            cp.wait_send()

    @pl.when(have[0])
    def _():
        usend.wait_send()

    for j in range(1, 5):

        @pl.when(have[j])
        def _(j=j):
            for m in order:
                slice_to(j, m).wait_send()


def return_states(updates, partial):
    dma = pltpu.SemaphoreType.DMA
    return pl.pallas_call(
        kernel_b,
        out_shape=(
            jax.ShapeDtypeStruct((512, 128), BF),
            jax.ShapeDtypeStruct((64, 512), F32),
        ),
        in_specs=[vmem()] * 2,
        out_specs=(vmem(), vmem()),
        scratch_shapes=[
            pltpu.VMEM((4, COL, 64, 128), BF),
            pltpu.VMEM((2, 64, 128), F32),
            pltpu.VMEM((4, 64, 128), F32),
            pltpu.VMEM((4, 64, 128), BF),
            pltpu.VMEM((512, 128), BF),
            pltpu.VMEM((512, 128), BF),
            pltpu.VMEM((PIECES, 64, 512), BF),
            pltpu.VMEM((4, 4, 64, 512), BF),
            pltpu.VMEM((2, 2, 64, 512), BF),
            pltpu.VMEM((2, 4, 64, 512), BF),
            pltpu.VMEM((4, 64, 512), BF),
            pltpu.VMEM((4, 64, 512), BF),
            pltpu.VMEM((8, 16, 256), F32),
            pltpu.VMEM((8, 16, 256), BF),
            pltpu.VMEM((8, 16, 256), BF),
            pltpu.VMEM((8, 16, 256), BF),
            dma((4, COL)), dma((4, COL)), dma((4,)), dma((4,)), dma((COL,)), dma((COL,)), dma, dma,
            dma((PIECES,)), dma((PIECES,)), dma((2,)), dma((2,)), dma((4,)), dma((4,)),
            dma((4,)), dma((4,)), dma((8,)), dma((8,)), dma((8,)), dma((8,)),
        ],
        compiler_params=pltpu.CompilerParams(collective_id=1, has_side_effects=True),
        name="return_states",
    )(updates, partial)


def level_table(length, stretch, local_bits):
    place = lax.iota(jnp.int32, length)
    blocks = place // stretch
    apart = jnp.bitwise_xor(blocks[:, None], blocks[None, :])
    table = jnp.zeros((length, length), jnp.int32)
    for bit in range(local_bits):
        table = table + (apart >= 1 << bit).astype(jnp.int32)
    causal = place[:, None] >= place[None, :]
    return (table, causal)


def local_weights(lam, table, causal, local_bits):
    weights = jnp.zeros((lam.shape[1], table.shape[0], table.shape[1]), jnp.float32)
    for level in range(local_bits + 1):
        weights = weights + jnp.where(table[None] == level, lam[level][:, :, None], jnp.float32(0))
    return jnp.where(causal[None], weights, jnp.float32(0))


def shards(queries, keys, values, level_weights, proj, out_grad):
    tokens_here, width = queries.shape[1:]
    heads, size, dev_bits, local_bits, stretch = 4, 128, 5, 2, 64
    scale = size ** (-0.5)
    shape = (tokens_here, heads, size)
    query = queries[0].reshape(shape)
    key = keys[0].reshape(shape)
    value = values[0].reshape(shape)
    lam = level_weights[0]
    grad_out = out_grad[0]
    full_t, states = gather_states(keys[0], values[0], proj.T)
    states = states.reshape(dev_bits, heads, size, size)
    table, causal = level_table(tokens_here, stretch, local_bits)
    scores = jnp.einsum("thd,shd->hts", query, key, preferred_element_type=jnp.float32)
    weights = local_weights(lam, table, causal, local_bits)
    probs = (scale * weights * scores).astype(jnp.bfloat16)
    total = jnp.einsum("hts,shd->thd", probs, value, preferred_element_type=jnp.float32)
    cross = jnp.zeros_like(total)
    mapped = []
    for bit in range(dev_bits):
        image = jnp.einsum("thi,hij->thj", query, states[bit], preferred_element_type=jnp.float32)
        mapped.append(image)
        cross = cross + lam[local_bits + 1 + bit].T[:, :, None] * image
    attended = (total + scale * cross).astype(jnp.bfloat16).reshape(tokens_here, width)
    out = lax.dot_general(
        attended, full_t, (((1,), (1,)), ((), ())), preferred_element_type=jnp.float32
    ).astype(jnp.bfloat16)
    grad_att = jnp.dot(grad_out, full_t, preferred_element_type=jnp.float32).astype(jnp.bfloat16)
    grad_heads = grad_att.reshape(shape)
    dprob = jnp.einsum("thd,shd->hts", grad_heads, value, preferred_element_type=jnp.float32)
    product = jnp.where(causal[None], scale * scores * dprob, jnp.float32(0))
    grads = [
        jnp.sum(jnp.where(table[None] == level, product, jnp.float32(0)), axis=2)
        for level in range(local_bits + 1)
    ]
    dscore = (scale * weights * dprob).astype(jnp.bfloat16)
    grad_q = jnp.einsum("hts,shd->thd", dscore, key, preferred_element_type=jnp.float32)
    grad_k = jnp.einsum("hts,thd->shd", dscore, query, preferred_element_type=jnp.float32)
    grad_v = jnp.einsum("hts,thd->shd", probs, grad_heads, preferred_element_type=jnp.float32)
    updates = []
    for bit in range(dev_bits):
        grads.append(scale * jnp.sum(grad_heads.astype(jnp.float32) * mapped[bit], axis=2).T)
        weighted = (
            scale * lam[local_bits + 1 + bit].T[:, :, None] * grad_heads.astype(jnp.float32)
        ).astype(jnp.bfloat16)
        updates.append(
            jnp.einsum("thi,thj->hij", query, weighted, preferred_element_type=jnp.float32).astype(BF)
        )
        grad_q = grad_q + jnp.einsum(
            "thj,hij->thi", weighted, states[bit], preferred_element_type=jnp.float32
        )
    partial = lax.dot_general(
        grad_out, attended, (((0,), (0,)), ((), ())), preferred_element_type=jnp.float32
    ).astype(BF)
    returned, shard = return_states(jnp.stack(updates).reshape(dev_bits, width, size), partial)
    returned = returned.reshape(heads, size, size)
    grad_k = grad_k + jnp.einsum(
        "shj,hij->shi", value, returned, preferred_element_type=jnp.float32
    )
    grad_v = grad_v + jnp.einsum("shi,hij->shj", key, returned, preferred_element_type=jnp.float32)
    grad_levels = jnp.stack(grads)[None]
    return (
        out[None],
        grad_q.astype(jnp.bfloat16).reshape(1, tokens_here, width),
        grad_k.astype(jnp.bfloat16).reshape(1, tokens_here, width),
        grad_v.astype(jnp.bfloat16).reshape(1, tokens_here, width),
        grad_levels,
        shard.T,
    )


def solution(mesh):
    return jax.shard_map(
        shards,
        mesh=mesh,
        in_specs=(
            P("dp", "seq", None),
            P("dp", "seq", None),
            P("dp", "seq", None),
            P("dp", None, None, "seq"),
            P(None, "seq"),
            P("dp", "seq", None),
        ),
        out_specs=(
            P("dp", "seq", None),
            P("dp", "seq", None),
            P("dp", "seq", None),
            P("dp", "seq", None),
            P("dp", None, None, "seq"),
            P(None, "seq"),
        ),
        check_vma=False,
    )
```

```python
import jax
import jax.numpy as jnp
from jax import lax
from jax.experimental import pallas as pl
from jax.experimental.pallas import tpu as pltpu
from jax.sharding import PartitionSpec as P

BF = jnp.bfloat16
F32 = jnp.float32
MESH = pl.DeviceIdType.MESH
COL = 8
PIECES = 16


def place():
    s = lax.axis_index("seq")
    bits = [lax.rem(lax.div(s, 2**b), 2) for b in range(5)]
    return s, bits


def flipped(s, bits, mask):
    peer = s
    for b in range(5):
        if mask >> b & 1:
            peer = peer + 2**b * (1 - 2 * bits[b])
    return peer


def chip_offsets(s, bits):
    c, y0, y1, x0, x1 = bits
    dy0, dy1 = 2 * (1 - 2 * y0), 4 * (1 - 2 * y1)
    dx0, dx1 = 8 * (1 - 2 * x0), 16 * (1 - 2 * x1)
    da0, da1 = dy0 * (1 - c) + dx0 * c, dy1 * (1 - c) + dx1 * c
    db0, db1 = dx0 * (1 - c) + dy0 * c, dx1 * (1 - c) + dy1 * c

    def off(a, b):
        return s + (a & 1) * da0 + (a >> 1) * da1 + (b & 1) * db0 + (b >> 1) * db1

    return off


def rows(index, count):
    return pl.ds(pl.multiple_of(index * count, count), count)


def send(src, dst, ssem, rsem, device):
    return pltpu.make_async_remote_copy(
        src_ref=src, dst_ref=dst, send_sem=ssem, recv_sem=rsem, device_id=device, device_id_type=MESH
    )


def bit_of(bits, b, mask):
    return 1 - bits[b] if mask >> b & 1 else bits[b]


def dot(x, y, dims):
    return lax.dot_general(x, y, (dims, ((), ())), preferred_element_type=F32)


NN, NT, TN = ((1,), (0,)), ((1,), (1,)), ((0,), (0,))
SCALE = 128**-0.5
ORDER = (4, 5, 2, 3, 6, 7, 1)
TILES = ((0, 0), (1, 1), (1, 0))


def step_kernel(
    q_hbm, k_hbm, v_hbm, lam_ref, proj_ref, og_hbm,
    out_ref, gq_ref, gk_ref, gv_ref, gl_ref, gp_ref,
    q, k, v, og, lamt, glt, shard_buf, full, states, score, prob, att32, att, mapped, ga, wt, gk32, gv32,
    tot, col, pair, quad, csum, xin, s3buf, s4buf,
    ubuf, ucol, asend, uxin, rsend, rcol, usib,
    g32, gbf, gsib, hbuf, rel, fin, gbuf, xg, zf, zsend, zin, zall,
    ld, ag_s, ag_r, c1_s, c1_r, st_s, st_r, x_s, x_r, sib_s, sib_r,
    u_s, u_r, ux_s, ux_r, ur_s, ur_r, us_s, us_r,
    gs_s, gs_r, rl_s, rl_r, fn_s, fn_r, gx_s, gx_r, z1_s, z1_r, z2_s, z2_r,
):
    s, bits = place()
    c, y0, y1, x0, x1 = bits
    z = lax.axis_index("dp")
    zbits = [lax.rem(lax.div(z, 2**b), 2) for b in range(3)] + [0, 0]
    r = lax.rem(s, COL)
    mine = rows(r, 64)
    off = chip_offsets(s, bits)
    have = [c == 1, y0 == 1, y1 == 1, x0 == 1, x1 == 1]
    sib_index = flipped(s, bits, 1)
    sibling = {"seq": sib_index}
    flip = sib_index - s

    loads = [
        pltpu.make_async_copy(src, dst, ld.at[i])
        for i, (src, dst) in enumerate(((k_hbm, k), (v_hbm, v), (q_hbm, q), (og_hbm, og)))
    ]
    for cp in loads:
        cp.start()

    greeted = (
        [{"seq": flipped(s, bits, m)} for m in range(1, 8)]
        + [{"seq": flipped(s, bits, m << 3)} for m in range(1, 4)]
        + [{"dp": flipped(z, zbits, m)} for m in range(1, 8)]
    )
    barrier = pltpu.get_barrier_semaphore()
    for device in greeted:
        pl.semaphore_signal(barrier, inc=1, device_id=device, device_id_type=MESH)

    def lanes(h):
        return pl.ds(128 * h, 128)

    shard_buf[...] = proj_ref[...]
    lamt[...] = lam_ref[...].T
    loads[0].wait()
    loads[1].wait()
    for h in range(4):
        tot[lanes(h)] = dot(k[:, lanes(h)], v[:, lanes(h)], TN).astype(BF)
    pl.semaphore_wait(barrier, len(greeted))

    first = []
    for m in ORDER:
        peer = flipped(s, bits, m)
        cp = send(tot.at[rows(lax.rem(peer, COL), 64)], col.at[m], c1_s.at[m], c1_r.at[m], {"seq": peer})
        cp.start()
        first.append(cp)
    sib = send(tot, states.at[0], sib_s, sib_r, sibling)

    @pl.when(c == 0)
    def _():
        sib.start()

    open_sends = []

    def block(index):
        return full.at[rows(index, 64)]

    def ag(slot, src, index, device):
        cp = send(src, block(index), ag_s.at[slot], ag_r.at[slot], device)
        cp.start()
        open_sends.append(cp)

    def ag_arrived(slot):
        send(shard_buf, block(s), ag_s.at[slot], ag_r.at[slot], sibling).wait_recv()

    full[rows(s, 64)] = shard_buf[...]
    for a in (1, 3, 2):
        ag(a, shard_buf, s, {"seq": off(a, 0)})
    for b in (1, 3):
        ag(4 + b, shard_buf, s, {"seq": off(0, b)})
    ag(20, shard_buf, s, sibling)

    row = lax.broadcasted_iota(jnp.int32, (128, 128), 0)
    column = lax.broadcasted_iota(jnp.int32, (128, 128), 1)
    causal = column <= row
    near = causal & ((row < 64) | (column >= 64))
    far = causal & (row >= 64) & (column < 64)

    def half(i):
        return pl.ds(128 * i, 128)

    def lam(level, h, where):
        return lamt[where, pl.ds(4 * level + h, 1)]

    def weight(h, i, j):
        if i != j:
            return SCALE * lam(2, h, half(i))
        return SCALE * jnp.where(near, lam(0, h, half(i)), jnp.where(far, lam(1, h, half(i)), 0.0))

    def inside(h):
        for n, (i, j) in enumerate(TILES):
            value = dot(q[half(i), lanes(h)], k[half(j), lanes(h)], NT)
            score[h, n] = value
            prob[h, n] = (weight(h, i, j) * value).astype(BF)
        att32[half(0), lanes(h)] = dot(prob[h, 0], v[half(0), lanes(h)], NN)
        att32[half(1), lanes(h)] = dot(prob[h, 1], v[half(1), lanes(h)], NN) + dot(
            prob[h, 2], v[half(0), lanes(h)], NN
        )

    loads[2].wait()
    inside(0)
    inside(1)

    for cp in first:
        cp.wait_recv()
    col[0] = tot[mine]
    t = [col[m].astype(F32) for m in range(COL)]
    p = [t[2 * i] + t[2 * i + 1] for i in range(4)]
    qd = [p[0] + p[1], p[2] + p[3]]
    csum[...] = qd[0] + qd[1]
    xsend = [
        send(csum, xin.at[m], x_s.at[m], x_r.at[m], {"seq": flipped(s, bits, m << 3)}) for m in range(1, 4)
    ]
    x_out = [x0 == 0, x1 == 0, x1 == 0]
    for cp, cond in zip(xsend, x_out):

        @pl.when(cond)
        def _(cp=cp):
            cp.start()

    for i in range(4):
        pair[i] = p[i].astype(BF)
    for i in range(2):
        quad[i] = qd[i].astype(BF)

    def spread(j, m, src):
        return send(src, states.at[j, mine], st_s.at[j, m], st_r.at[j, m], {"seq": flipped(s, bits, m)})

    early = []
    for m in ORDER:
        early.append((spread(1, m, pair.at[(m >> 1) ^ 1]), bit_of(bits, 1, m) == 1))
        early.append((spread(2, m, quad.at[(m >> 2) ^ 1]), bit_of(bits, 2, m) == 1))
    for cp, cond in early:

        @pl.when(cond)
        def _(cp=cp):
            cp.start()

    for j in range(5):

        @pl.when(jnp.logical_not(have[j]))
        def _(j=j):
            states[j] = jnp.zeros((512, 128), BF)

    @pl.when(have[1])
    def _():
        states[1, mine] = pair[1]

    @pl.when(have[2])
    def _():
        states[2, mine] = quad[1]

    inside(2)
    inside(3)

    late3 = [spread(3, m, s3buf) for m in ORDER]
    late4 = [spread(4, m, s4buf) for m in ORDER]

    @pl.when(have[3])
    def _():
        xsend[0].wait_recv()
        s3buf[...] = xin[1].astype(BF)
        for cp in late3:
            cp.start()
        states[3, mine] = s3buf[...]

    @pl.when(have[4])
    def _():
        xsend[1].wait_recv()
        xsend[2].wait_recv()
        s4buf[...] = (xin[2] + xin[3]).astype(BF)
        for cp in late4:
            cp.start()
        states[4, mine] = s4buf[...]

    for a in (1, 3, 2):
        ag_arrived(a)
        for b in (1, 3):
            ag(4 + 4 * a + b, block(off(a, 0)), off(a, 0), {"seq": off(0, b)})
        ag(20 + 4 * a, block(off(a, 0)), off(a, 0), sibling)

    @pl.when(have[0])
    def _():
        sib.wait_recv()

    for j in range(1, 5):

        @pl.when(have[j])
        def _(j=j):
            for m in ORDER:
                spread(j, m, s4buf).wait_recv()

    for h in range(4):
        cross = jnp.zeros((256, 128), F32)
        for j in range(5):
            image = dot(q[:, lanes(h)], states[j, lanes(h)], NN)
            mapped[h, j] = image
            cross = cross + lam(3 + j, h, pl.ds(0, 256)) * image
        att[:, lanes(h)] = (att32[:, lanes(h)] + SCALE * cross).astype(BF)

    loads[3].wait()
    gs = []
    for a in (2, 1, 3, 0):
        for b in range(4):
            chip = lax.div(off(a, b), 2)
            at = rows(chip, 128)
            value = dot(og[:, rows(chip, 128)], att[...], TN)
            g32[at] = value
            gbf[at] = value.astype(BF)
            slot = 4 * b + a
            cp = send(gbf.at[rows(off(a, b) + flip, 64)], gsib.at[slot], gs_s.at[slot], gs_r.at[slot], sibling)
            cp.start()
            gs.append(cp)

    def second(a):
        for b in (1, 3):
            ag_arrived(4 + 4 * a + b)
            if (b == 1) == (a < 2):
                ag(4 + 4 * a + 2, block(off(a, b)), off(a, b), {"seq": off(0, 4 - b)})
            ag(20 + 4 * a + b, block(off(a, b)), off(a, b), sibling)

    for a in (0, 1, 3, 2):
        second(a)

    def h_make(a, b):
        slot = 4 * a + b
        send(gbf.at[pl.ds(0, 64)], gsib.at[slot], gs_s.at[slot], gs_r.at[slot], sibling).wait_recv()
        hbuf[a, b] = (g32[rows(off(a, b), 64)] + gsib[slot].astype(F32)).astype(BF)

    dev_a = {1: {"seq": off(1, 0)}, 3: {"seq": off(3, 0)}}
    for b in range(4):
        h_make(2, b)
    rl = {
        1: send(hbuf.at[2, pl.ds(0, 2)], rel.at[0], rl_s.at[0], rl_r.at[0], dev_a[1]),
        3: send(hbuf.at[2, pl.ds(2, 2)], rel.at[1], rl_s.at[1], rl_r.at[1], dev_a[3]),
    }
    rl[1].start()
    rl[3].start()

    def final(m, part):
        n = 2 * (m // 2) + part
        return send(
            hbuf.at[m, pl.ds(2 * part, 2)], fin.at[m // 2, pl.ds(2 * part, 2)], fn_s.at[n], fn_r.at[n], dev_a[m]
        )

    h_make(1, 0)
    h_make(1, 1)
    f10 = final(1, 0)
    f10.start()
    h_make(3, 2)
    h_make(3, 3)
    f31 = final(3, 1)
    f31.start()

    for a in (0, 1, 3, 2):
        ag_arrived(4 + 4 * a + 2)
        ag(20 + 4 * a + 2, block(off(a, 2)), off(a, 2), sibling)
    for a in range(4):
        for b in range(4):
            ag_arrived(20 + 4 * a + b)
    ga[...] = dot(og[...], full[...], NN).astype(BF)
    for h in range(4):
        g = ga[:, lanes(h)].astype(F32)
        for j in range(5):
            wt[h, j] = (SCALE * lam(3 + j, h, pl.ds(0, 256)) * g).astype(BF)
            ubuf[j, lanes(h)] = dot(q[:, lanes(h)], wt[h, j], TN).astype(BF)

    usend = send(ubuf.at[0], usib, us_s, us_r, sibling)

    @pl.when(have[0])
    def _():
        usend.start()

    def slice_to(j, m):
        peer = flipped(s, bits, m)
        return send(
            ubuf.at[j, rows(lax.rem(peer, COL), 64)],
            ucol.at[j - 1, m],
            u_s.at[j - 1, m],
            u_r.at[j - 1, m],
            {"seq": peer},
        )

    for j in (4, 3, 2, 1):

        @pl.when(have[j])
        def _(j=j):
            for m in ORDER:
                slice_to(j, m).start()

    for b in range(2):
        h_make(3, b)
    rl[1].wait_recv()
    for b in range(2):
        hbuf[3, b] = (hbuf[3, b].astype(F32) + rel[0, b].astype(F32)).astype(BF)
    f30 = final(3, 0)
    f30.start()
    for b in range(2):
        h_make(1, 2 + b)
    rl[3].wait_recv()
    for b in range(2):
        hbuf[1, 2 + b] = (hbuf[1, 2 + b].astype(F32) + rel[1, b].astype(F32)).astype(BF)
    f11 = final(1, 1)
    f11.start()

    place_of = lax.broadcasted_iota(jnp.int32, (128, 128), 1)

    def sums(value):
        return jnp.sum(value, axis=1, keepdims=True)

    def backward(h):
        ds = []
        got = {}
        for n, (i, j) in enumerate(TILES):
            dp = dot(ga[half(i), lanes(h)], v[half(j), lanes(h)], NT)
            ds.append((weight(h, i, j) * dp).astype(BF))
            product = SCALE * score[h, n] * dp
            if i != j:
                got[2, i] = sums(product)
            else:
                got[0, i] = sums(jnp.where(near, product, 0.0))
                got[1, i] = sums(jnp.where(far, product, 0.0))
        for i in range(2):
            g = ga[half(i), lanes(h)].astype(F32)
            acc = glt[half(i)]
            for level in range(8):
                if level > 2:
                    value = SCALE * sums(g * mapped[h, level - 3, half(i)])
                elif (level, i) in got:
                    value = got[level, i]
                else:
                    continue
                acc = jnp.where(place_of == 4 * level + h, value, acc)
            glt[half(i)] = acc
        gq = [dot(ds[0], k[half(0), lanes(h)], NN), dot(ds[1], k[half(1), lanes(h)], NN)]
        gq[1] = gq[1] + dot(ds[2], k[half(0), lanes(h)], NN)
        for i in range(2):
            for j in range(5):
                gq[i] = gq[i] + dot(wt[h, j, half(i)], states[j, lanes(h)], NT)
            gq_ref[half(i), lanes(h)] = gq[i].astype(BF)
        q0, q1 = q[half(0), lanes(h)], q[half(1), lanes(h)]
        g0, g1 = ga[half(0), lanes(h)], ga[half(1), lanes(h)]
        gk32[half(0), lanes(h)] = dot(ds[0], q0, TN) + dot(ds[2], q1, TN)
        gk32[half(1), lanes(h)] = dot(ds[1], q1, TN)
        gv32[half(0), lanes(h)] = dot(prob[h, 0], g0, TN) + dot(prob[h, 2], g1, TN)
        gv32[half(1), lanes(h)] = dot(prob[h, 1], g1, TN)

    glt[...] = jnp.zeros_like(glt)
    backward(0)
    backward(1)

    for j in range(1, 5):
        for m in range(COL):
            cond = bit_of(bits, j, m) == 1 if j < 3 else have[j]

            @pl.when(cond)
            def _(j=j, m=m):
                if m:
                    slice_to(j, m).wait_recv()
                else:
                    ucol[j - 1, 0] = ubuf[j, mine]

            @pl.when(jnp.logical_not(cond))
            def _(j=j, m=m):
                ucol[j - 1, m] = jnp.zeros((64, 128), BF)

    def total(j, ms):
        value = ucol[j - 1, ms[0]].astype(F32)
        for m in ms[1:]:
            value = value + ucol[j - 1, m].astype(F32)
        return value

    asend[0] = total(3, list(range(COL)))
    asend[1] = total(4, list(range(COL)))
    ux = [
        send(asend.at[0 if m == 1 else 1], uxin.at[m], ux_s.at[m], ux_r.at[m], {"seq": flipped(s, bits, m << 3)})
        for m in range(1, 4)
    ]
    ux_out = [x0 == 1, x1 == 1, x1 == 1]
    for cp, cond in zip(ux, ux_out):

        @pl.when(cond)
        def _(cp=cp):
            cp.start()

    for b in range(4):
        h_make(0, b)
    for cp in (f10, f31, f30, f11):
        cp.wait_recv()
    for b in range(4):
        gbuf[b] = (hbuf[0, b].astype(F32) + fin[0, b].astype(F32) + fin[1, b].astype(F32)).astype(BF)
    gx = []
    for b in (2, 1, 3):
        cp = send(gbuf.at[b], xg.at[b], gx_s.at[b], gx_r.at[b], {"seq": off(0, b)})
        cp.start()
        gx.append(cp)

    backward(2)

    for cp, cond, m in zip(ux, ux_out, range(1, 4)):

        @pl.when(jnp.logical_not(cond))
        def _(cp=cp):
            cp.wait_recv()

        @pl.when(cond)
        def _(m=m):
            uxin[m] = jnp.zeros((64, 128), F32)

    beyond = uxin[1] + uxin[2] + uxin[3]
    for i in range(4):
        n = 4 * ((i >> 1) ^ 1)
        rsend[i] = (
            beyond + total(1, [2 * (i ^ 1), 2 * (i ^ 1) + 1]) + total(2, [n, n + 1, n + 2, n + 3])
        ).astype(BF)
    rc = []
    for m in ORDER:
        cp = send(rsend.at[m >> 1], rcol.at[mine], ur_s.at[m], ur_r.at[m], {"seq": flipped(s, bits, m)})
        cp.start()
        rc.append(cp)
    rcol[mine] = rsend[0]

    for cp in gx:
        cp.wait_recv()
    mean = gbuf[0].astype(F32) + xg[1].astype(F32) + xg[2].astype(F32) + xg[3].astype(F32)
    for i in range(8):
        part = mean[16 * (i // 2) : 16 * (i // 2) + 16, 256 * (i % 2) : 256 * (i % 2) + 256]
        zf[i] = part
        zsend[i] = part.astype(BF)
    z1 = []
    for m in ORDER:
        peer = flipped(z, zbits, m)
        cp = send(zsend.at[peer], zin.at[m], z1_s.at[m], z1_r.at[m], {"dp": peer})
        cp.start()
        z1.append(cp)

    backward(3)

    def output(n):
        at = pl.ds(512 * n, 512)
        out_ref[:, at] = dot(att[...], full[at], NT).astype(BF)

    output(0)
    output(1)

    for cp in z1:
        cp.wait_recv()
    value = zf[z]
    for m in range(1, 8):
        value = value + zin[m].astype(F32)
    zall[z] = value.astype(BF)
    z2 = []
    for m in ORDER:
        cp = send(zall.at[z], zall.at[z], z2_s.at[m], z2_r.at[m], {"dp": flipped(z, zbits, m)})
        cp.start()
        z2.append(cp)

    output(2)
    output(3)

    for cp in rc:
        cp.wait_recv()

    @pl.when(c == 0)
    def _():
        usend.wait_recv()

    @pl.when(have[0])
    def _():
        usib[...] = jnp.zeros((512, 128), BF)

    for h in range(4):
        back = (rcol[lanes(h)].astype(F32) + usib[lanes(h)].astype(F32)).astype(BF)
        gk_ref[:, lanes(h)] = (gk32[:, lanes(h)] + dot(v[:, lanes(h)], back, NT)).astype(BF)
        gv_ref[:, lanes(h)] = (gv32[:, lanes(h)] + dot(k[:, lanes(h)], back, NN)).astype(BF)
    gl_ref[...] = glt[...].T[:32]

    for cp in z2:
        cp.wait_recv()
    for i in range(8):
        gp_ref[pl.ds(16 * (i // 2), 16), pl.ds(256 * (i % 2), 256)] = zall[i].astype(F32)

    for cp in first + open_sends + gs + [rl[1], rl[3], f10, f11, f30, f31] + rc + gx + z1 + z2:
        cp.wait_send()
    for cp, cond in early + list(zip(xsend, x_out)) + list(zip(ux, ux_out)):

        @pl.when(cond)
        def _(cp=cp):
            cp.wait_send()

    @pl.when(c == 0)
    def _():
        sib.wait_send()

    @pl.when(have[0])
    def _():
        usend.wait_send()

    for j in range(1, 5):

        @pl.when(have[j])
        def _(j=j):
            for m in ORDER:
                slice_to(j, m).wait_send()
            for cp in {3: late3, 4: late4}.get(j, []):
                cp.wait_send()


def step(query, key, value, lam, proj, grad_out):
    dma = pltpu.SemaphoreType.DMA
    any_space = pl.BlockSpec(memory_space=pl.ANY)
    inner = pl.BlockSpec(memory_space=pltpu.VMEM)
    wide = (256, 512)
    return pl.pallas_call(
        step_kernel,
        out_shape=(
            jax.ShapeDtypeStruct((256, 2048), BF),
            jax.ShapeDtypeStruct(wide, BF),
            jax.ShapeDtypeStruct(wide, BF),
            jax.ShapeDtypeStruct(wide, BF),
            jax.ShapeDtypeStruct((32, 256), F32),
            jax.ShapeDtypeStruct((64, 512), F32),
        ),
        in_specs=[any_space, any_space, any_space, inner, inner, any_space],
        out_specs=(inner,) * 6,
        scratch_shapes=[
            pltpu.VMEM(wide, BF), pltpu.VMEM(wide, BF), pltpu.VMEM(wide, BF),
            pltpu.VMEM((256, 2048), BF),
            pltpu.VMEM((256, 32), F32),
            pltpu.VMEM((256, 128), F32),
            pltpu.VMEM((64, 512), BF),
            pltpu.VMEM((2048, 512), BF),
            pltpu.VMEM((5, 512, 128), BF),
            pltpu.VMEM((4, 3, 128, 128), F32),
            pltpu.VMEM((4, 3, 128, 128), BF),
            pltpu.VMEM(wide, F32),
            pltpu.VMEM(wide, BF),
            pltpu.VMEM((4, 5, 256, 128), F32),
            pltpu.VMEM(wide, BF),
            pltpu.VMEM((4, 5, 256, 128), BF),
            pltpu.VMEM(wide, F32),
            pltpu.VMEM(wide, F32),
            pltpu.VMEM((512, 128), BF),
            pltpu.VMEM((COL, 64, 128), BF),
            pltpu.VMEM((4, 64, 128), BF),
            pltpu.VMEM((2, 64, 128), BF),
            pltpu.VMEM((64, 128), F32),
            pltpu.VMEM((4, 64, 128), F32),
            pltpu.VMEM((64, 128), BF),
            pltpu.VMEM((64, 128), BF),
            pltpu.VMEM((5, 512, 128), BF),
            pltpu.VMEM((4, COL, 64, 128), BF),
            pltpu.VMEM((2, 64, 128), F32),
            pltpu.VMEM((4, 64, 128), F32),
            pltpu.VMEM((4, 64, 128), BF),
            pltpu.VMEM((512, 128), BF),
            pltpu.VMEM((512, 128), BF),
            pltpu.VMEM((2048, 512), F32),
            pltpu.VMEM((2048, 512), BF),
            pltpu.VMEM((PIECES, 64, 512), BF),
            pltpu.VMEM((4, 4, 64, 512), BF),
            pltpu.VMEM((2, 2, 64, 512), BF),
            pltpu.VMEM((2, 4, 64, 512), BF),
            pltpu.VMEM((4, 64, 512), BF),
            pltpu.VMEM((4, 64, 512), BF),
            pltpu.VMEM((8, 16, 256), F32),
            pltpu.VMEM((8, 16, 256), BF),
            pltpu.VMEM((8, 16, 256), BF),
            pltpu.VMEM((8, 16, 256), BF),
            dma((4,)),
            dma((36,)), dma((36,)), dma((COL,)), dma((COL,)),
            dma((5, COL)), dma((5, COL)), dma((4,)), dma((4,)), dma, dma,
            dma((4, COL)), dma((4, COL)), dma((4,)), dma((4,)), dma((COL,)), dma((COL,)), dma, dma,
            dma((PIECES,)), dma((PIECES,)), dma((2,)), dma((2,)), dma((4,)), dma((4,)),
            dma((4,)), dma((4,)), dma((8,)), dma((8,)), dma((8,)), dma((8,)),
        ],
        compiler_params=pltpu.CompilerParams(collective_id=0, has_side_effects=True),
        name="span_step",
    )(query, key, value, lam, proj, grad_out)


def shards(queries, keys, values, level_weights, proj, out_grad):
    out, gq, gk, gv, gl, gp = step(
        queries[0], keys[0], values[0], level_weights[0].reshape(32, 256), proj.T, out_grad[0]
    )
    return out[None], gq[None], gk[None], gv[None], gl.reshape(1, 8, 4, 256), gp.T


def solution(mesh):
    return jax.shard_map(
        shards,
        mesh=mesh,
        in_specs=(
            P("dp", "seq", None),
            P("dp", "seq", None),
            P("dp", "seq", None),
            P("dp", None, None, "seq"),
            P(None, "seq"),
            P("dp", "seq", None),
        ),
        out_specs=(
            P("dp", "seq", None),
            P("dp", "seq", None),
            P("dp", "seq", None),
            P("dp", "seq", None),
            P("dp", None, None, "seq"),
            P(None, "seq"),
        ),
        check_vma=False,
    )
```

```python
import jax
import jax.numpy as jnp
from jax import lax
from jax.experimental import pallas as pl
from jax.experimental.pallas import tpu as pltpu
from jax.sharding import PartitionSpec as P

BF = jnp.bfloat16
F32 = jnp.float32
MESH = pl.DeviceIdType.MESH
COL = 8
PIECES = 16


def place():
    s = lax.axis_index("seq")
    bits = [lax.rem(lax.div(s, 2**b), 2) for b in range(5)]
    return s, bits


def flipped(s, bits, mask):
    peer = s
    for b in range(5):
        if mask >> b & 1:
            peer = peer + 2**b * (1 - 2 * bits[b])
    return peer


def chip_offsets(s, bits):
    c, y0, y1, x0, x1 = bits
    dy0, dy1 = 2 * (1 - 2 * y0), 4 * (1 - 2 * y1)
    dx0, dx1 = 8 * (1 - 2 * x0), 16 * (1 - 2 * x1)
    da0, da1 = dy0 * (1 - c) + dx0 * c, dy1 * (1 - c) + dx1 * c
    db0, db1 = dx0 * (1 - c) + dy0 * c, dx1 * (1 - c) + dy1 * c

    def off(a, b):
        return s + (a & 1) * da0 + (a >> 1) * da1 + (b & 1) * db0 + (b >> 1) * db1

    return off


def rows(index, count):
    return pl.ds(pl.multiple_of(index * count, count), count)


def send(src, dst, ssem, rsem, device):
    return pltpu.make_async_remote_copy(
        src_ref=src, dst_ref=dst, send_sem=ssem, recv_sem=rsem, device_id=device, device_id_type=MESH
    )


def bit_of(bits, b, mask):
    return 1 - bits[b] if mask >> b & 1 else bits[b]


def dot(x, y, dims):
    return lax.dot_general(x, y, (dims, ((), ())), preferred_element_type=F32)


NN, NT, TN = ((1,), (0,)), ((1,), (1,)), ((0,), (0,))
SCALE = 128**-0.5
ORDER = (4, 5, 2, 3, 6, 7, 1)
TILES = ((0, 0), (1, 1), (1, 0))


def step_kernel(
    q_hbm, k_hbm, v_hbm, lam_ref, proj_ref, og_hbm,
    out_ref, gq_ref, gk_ref, gv_ref, gl_ref, gp_ref,
    q, k, v, og, ogt, lamt, glt, glrow, shard_buf, full, states, score, prob, att32, att, mapped, ga, wt, gk32, gv32,
    tot, col, pair, quad, csum, xin, s3buf, s4buf,
    ubuf, ucol, asend, uxin, rsend, rcol, usib,
    g32, gbf, gsib, hbuf, rel, fin, gbuf, xg, zf, zsend, zin, zall,
    ld, ag_s, ag_r, c1_s, c1_r, st_s, st_r, x_s, x_r, sib_s, sib_r,
    u_s, u_r, ux_s, ux_r, ur_s, ur_r, us_s, us_r,
    gs_s, gs_r, rl_s, rl_r, fn_s, fn_r, gx_s, gx_r, z1_s, z1_r, z2_s, z2_r,
):
    s, bits = place()
    c, y0, y1, x0, x1 = bits
    z = lax.axis_index("dp")
    zbits = [lax.rem(lax.div(z, 2**b), 2) for b in range(3)] + [0, 0]
    r = lax.rem(s, COL)
    mine = rows(r, 64)
    off = chip_offsets(s, bits)
    have = [c == 1, y0 == 1, y1 == 1, x0 == 1, x1 == 1]
    sib_index = flipped(s, bits, 1)
    sibling = {"seq": sib_index}

    loads = [
        pltpu.make_async_copy(src, dst, ld.at[i])
        for i, (src, dst) in enumerate(((k_hbm, k), (v_hbm, v), (q_hbm, q), (og_hbm, og)))
    ]
    for cp in loads:
        cp.start()

    greeted = (
        [{"seq": flipped(s, bits, m)} for m in range(1, 8)]
        + [{"seq": flipped(s, bits, m << 3)} for m in range(1, 4)]
        + [{"dp": flipped(z, zbits, m)} for m in range(1, 8)]
    )
    barrier = pltpu.get_barrier_semaphore()
    for device in greeted:
        pl.semaphore_signal(barrier, inc=1, device_id=device, device_id_type=MESH)

    def lanes(h):
        return pl.ds(128 * h, 128)

    shard_buf[...] = proj_ref[...]
    for level in range(8):
        glrow[pl.ds(4 * level, 4)] = lam_ref[level]
    lamt[...] = glrow[...].T
    loads[0].wait()
    loads[1].wait()
    for h in range(4):
        tot[lanes(h)] = dot(k[:, lanes(h)], v[:, lanes(h)], TN).astype(BF)
    pl.semaphore_wait(barrier, len(greeted))

    first = []
    for m in ORDER:
        peer = flipped(s, bits, m)
        cp = send(tot.at[rows(lax.rem(peer, COL), 64)], col.at[m], c1_s.at[m], c1_r.at[m], {"seq": peer})
        cp.start()
        first.append(cp)
    sib = send(tot, states.at[0], sib_s, sib_r, sibling)

    @pl.when(c == 0)
    def _():
        sib.start()

    open_sends = []

    def block(index):
        return full.at[rows(index, 64)]

    def ag(slot, src, index, device):
        cp = send(src, block(index), ag_s.at[slot], ag_r.at[slot], device)
        cp.start()
        open_sends.append(cp)

    def ag_arrived(slot):
        send(shard_buf, block(s), ag_s.at[slot], ag_r.at[slot], sibling).wait_recv()

    def chip(a, b):
        return flipped(s, bits, a << 1 | b << 3)

    full[rows(s, 64)] = shard_buf[...]
    for a in (1, 3, 2):
        ag(a, shard_buf, s, {"seq": chip(a, 0)})
    for b in (1, 3):
        ag(4 + b, shard_buf, s, {"seq": chip(0, b)})
    ag(20, shard_buf, s, sibling)

    row = lax.broadcasted_iota(jnp.int32, (128, 128), 0)
    column = lax.broadcasted_iota(jnp.int32, (128, 128), 1)
    causal = column <= row
    near = causal & ((row < 64) | (column >= 64))
    far = causal & (row >= 64) & (column < 64)

    def half(i):
        return pl.ds(128 * i, 128)

    def lam(level, h, where):
        return lamt[where, pl.ds(4 * level + h, 1)]

    def weight(h, i, j):
        if i != j:
            return SCALE * lam(2, h, half(i))
        return SCALE * jnp.where(near, lam(0, h, half(i)), jnp.where(far, lam(1, h, half(i)), 0.0))

    def inside(h):
        for n, (i, j) in enumerate(TILES):
            value = dot(q[half(i), lanes(h)], k[half(j), lanes(h)], NT)
            score[h, n] = value
            prob[h, n] = (weight(h, i, j) * value).astype(BF)
        att32[half(0), lanes(h)] = dot(prob[h, 0], v[half(0), lanes(h)], NN)
        att32[half(1), lanes(h)] = dot(prob[h, 1], v[half(1), lanes(h)], NN) + dot(
            prob[h, 2], v[half(0), lanes(h)], NN
        )

    loads[2].wait()
    inside(0)
    inside(1)

    for cp in first:
        cp.wait_recv()
    col[0] = tot[mine]
    t = [col[m].astype(F32) for m in range(COL)]
    p = [t[2 * i] + t[2 * i + 1] for i in range(4)]
    qd = [p[0] + p[1], p[2] + p[3]]
    csum[...] = qd[0] + qd[1]
    xsend = [
        send(csum, xin.at[m], x_s.at[m], x_r.at[m], {"seq": flipped(s, bits, m << 3)}) for m in range(1, 4)
    ]
    x_out = [x0 == 0, x1 == 0, x1 == 0]
    for cp, cond in zip(xsend, x_out):

        @pl.when(cond)
        def _(cp=cp):
            cp.start()

    for i in range(4):
        pair[i] = p[i].astype(BF)
    for i in range(2):
        quad[i] = qd[i].astype(BF)

    def spread(j, m, src):
        return send(src, states.at[j, mine], st_s.at[j, m], st_r.at[j, m], {"seq": flipped(s, bits, m)})

    early = []
    for m in ORDER:
        early.append((spread(1, m, pair.at[(m >> 1) ^ 1]), bit_of(bits, 1, m) == 1))
        early.append((spread(2, m, quad.at[(m >> 2) ^ 1]), bit_of(bits, 2, m) == 1))
    for cp, cond in early:

        @pl.when(cond)
        def _(cp=cp):
            cp.start()

    for j in range(5):

        @pl.when(jnp.logical_not(have[j]))
        def _(j=j):
            states[j] = jnp.zeros((512, 128), BF)

    @pl.when(have[1])
    def _():
        states[1, mine] = pair[1]

    @pl.when(have[2])
    def _():
        states[2, mine] = quad[1]

    def first_axis(a):
        ag_arrived(a)
        for b in (1, 3):
            ag(4 + 4 * a + b, block(chip(a, 0)), chip(a, 0), {"seq": chip(0, b)})
        ag(20 + 4 * a, block(chip(a, 0)), chip(a, 0), sibling)

    def second_axis(a):
        for b in (1, 3):
            ag_arrived(4 + 4 * a + b)
            if (b == 1) == (a < 2):
                ag(4 + 4 * a + 2, block(chip(a, b)), chip(a, b), {"seq": chip(0, 4 - b)})
            ag(20 + 4 * a + b, block(chip(a, b)), chip(a, b), sibling)

    first_axis(1)
    first_axis(3)

    inside(2)

    late3 = [spread(3, m, s3buf) for m in ORDER]
    late4 = [spread(4, m, s4buf) for m in ORDER]

    @pl.when(have[3])
    def _():
        xsend[0].wait_recv()
        s3buf[...] = xin[1].astype(BF)
        for cp in late3:
            cp.start()
        states[3, mine] = s3buf[...]

    @pl.when(have[4])
    def _():
        xsend[1].wait_recv()
        xsend[2].wait_recv()
        s4buf[...] = (xin[2] + xin[3]).astype(BF)
        for cp in late4:
            cp.start()
        states[4, mine] = s4buf[...]

    first_axis(2)
    second_axis(0)
    second_axis(1)

    inside(3)
    loads[3].wait()
    for n in range(16):
        turned = og[:, pl.ds(128 * n, 128)].T
        ogt[0, n] = turned[:64]
        ogt[1, n] = turned[64:]

    second_axis(3)
    second_axis(2)

    @pl.when(have[0])
    def _():
        sib.wait_recv()

    for j in range(1, 5):

        @pl.when(have[j])
        def _(j=j):
            for m in ORDER:
                spread(j, m, s4buf).wait_recv()

    for h in range(4):
        cross = jnp.zeros((256, 128), F32)
        for j in range(5):
            image = dot(q[:, lanes(h)], states[j, lanes(h)], NN)
            mapped[h, j] = image
            cross = cross + lam(3 + j, h, pl.ds(0, 256)) * image
        att[:, lanes(h)] = (att32[:, lanes(h)] + SCALE * cross).astype(BF)

    other = 1 - c
    for n in range(4):
        part = pl.ds(4 * n, 4)
        gbf[part] = dot(ogt[other, part].reshape(256, 256), att[...], NN).astype(BF).reshape(4, 64, 512)
    gs = []
    for a in (2, 1, 3, 0):
        for b in range(4):
            slot = 4 * b + a
            cp = send(gbf.at[lax.div(off(a, b), 2)], gsib.at[slot], gs_s.at[slot], gs_r.at[slot], sibling)
            cp.start()
            gs.append(cp)
    for n in range(4):
        part = pl.ds(4 * n, 4)
        g32[part] = dot(ogt[c, part].reshape(256, 256), att[...], NN).reshape(4, 64, 512)

    for a in (0, 1, 3, 2):
        ag_arrived(4 + 4 * a + 2)
        ag(20 + 4 * a + 2, block(chip(a, 2)), chip(a, 2), sibling)

    def h_make(a, b):
        slot = 4 * a + b
        send(gbf.at[0], gsib.at[slot], gs_s.at[slot], gs_r.at[slot], sibling).wait_recv()
        hbuf[a, b] = (g32[lax.div(off(a, b), 2)] + gsib[slot].astype(F32)).astype(BF)

    dev_a = {1: {"seq": off(1, 0)}, 3: {"seq": off(3, 0)}}
    for b in range(4):
        h_make(2, b)
    rl = {
        1: send(hbuf.at[2, pl.ds(0, 2)], rel.at[0], rl_s.at[0], rl_r.at[0], dev_a[1]),
        3: send(hbuf.at[2, pl.ds(2, 2)], rel.at[1], rl_s.at[1], rl_r.at[1], dev_a[3]),
    }
    rl[1].start()
    rl[3].start()

    def final(m, part):
        n = 2 * (m // 2) + part
        return send(
            hbuf.at[m, pl.ds(2 * part, 2)], fin.at[m // 2, pl.ds(2 * part, 2)], fn_s.at[n], fn_r.at[n], dev_a[m]
        )

    h_make(1, 0)
    h_make(1, 1)
    f10 = final(1, 0)
    f10.start()
    h_make(3, 2)
    h_make(3, 3)
    f31 = final(3, 1)
    f31.start()

    for a in range(4):
        for b in range(4):
            ag_arrived(20 + 4 * a + b)
    ga[...] = dot(og[...], full[...], NN).astype(BF)
    for h in range(4):
        g = ga[:, lanes(h)].astype(F32)
        for j in range(5):
            wt[h, j] = (SCALE * lam(3 + j, h, pl.ds(0, 256)) * g).astype(BF)
            ubuf[j, lanes(h)] = dot(q[:, lanes(h)], wt[h, j], TN).astype(BF)

    usend = send(ubuf.at[0], usib, us_s, us_r, sibling)

    @pl.when(have[0])
    def _():
        usend.start()

    def slice_to(j, m):
        peer = flipped(s, bits, m)
        return send(
            ubuf.at[j, rows(lax.rem(peer, COL), 64)],
            ucol.at[j - 1, m],
            u_s.at[j - 1, m],
            u_r.at[j - 1, m],
            {"seq": peer},
        )

    for j in (4, 3, 2, 1):

        @pl.when(have[j])
        def _(j=j):
            for m in ORDER:
                slice_to(j, m).start()

    for b in range(2):
        h_make(3, b)
    rl[1].wait_recv()
    for b in range(2):
        hbuf[3, b] = (hbuf[3, b].astype(F32) + rel[0, b].astype(F32)).astype(BF)
    f30 = final(3, 0)
    f30.start()
    for b in range(2):
        h_make(1, 2 + b)
    rl[3].wait_recv()
    for b in range(2):
        hbuf[1, 2 + b] = (hbuf[1, 2 + b].astype(F32) + rel[1, b].astype(F32)).astype(BF)
    f11 = final(1, 1)
    f11.start()

    place_of = lax.broadcasted_iota(jnp.int32, (128, 128), 1)

    def sums(value):
        return jnp.sum(value, axis=1, keepdims=True)

    def backward(h):
        ds = []
        got = {}
        for n, (i, j) in enumerate(TILES):
            dp = dot(ga[half(i), lanes(h)], v[half(j), lanes(h)], NT)
            ds.append((weight(h, i, j) * dp).astype(BF))
            product = SCALE * score[h, n] * dp
            if i != j:
                got[2, i] = sums(product)
            else:
                got[0, i] = sums(jnp.where(near, product, 0.0))
                got[1, i] = sums(jnp.where(far, product, 0.0))
        for i in range(2):
            g = ga[half(i), lanes(h)].astype(F32)
            acc = glt[half(i)]
            for level in range(8):
                if level > 2:
                    value = SCALE * sums(g * mapped[h, level - 3, half(i)])
                elif (level, i) in got:
                    value = got[level, i]
                else:
                    continue
                acc = jnp.where(place_of == 4 * level + h, value, acc)
            glt[half(i)] = acc
        gq = [dot(ds[0], k[half(0), lanes(h)], NN), dot(ds[1], k[half(1), lanes(h)], NN)]
        gq[1] = gq[1] + dot(ds[2], k[half(0), lanes(h)], NN)
        for i in range(2):
            for j in range(5):
                gq[i] = gq[i] + dot(wt[h, j, half(i)], states[j, lanes(h)], NT)
            gq_ref[half(i), lanes(h)] = gq[i].astype(BF)
        q0, q1 = q[half(0), lanes(h)], q[half(1), lanes(h)]
        g0, g1 = ga[half(0), lanes(h)], ga[half(1), lanes(h)]
        gk32[half(0), lanes(h)] = dot(ds[0], q0, TN) + dot(ds[2], q1, TN)
        gk32[half(1), lanes(h)] = dot(ds[1], q1, TN)
        gv32[half(0), lanes(h)] = dot(prob[h, 0], g0, TN) + dot(prob[h, 2], g1, TN)
        gv32[half(1), lanes(h)] = dot(prob[h, 1], g1, TN)

    glt[...] = jnp.zeros_like(glt)
    backward(0)
    backward(1)

    for j in range(1, 5):
        for m in range(COL):
            cond = bit_of(bits, j, m) == 1 if j < 3 else have[j]

            @pl.when(cond)
            def _(j=j, m=m):
                if m:
                    slice_to(j, m).wait_recv()
                else:
                    ucol[j - 1, 0] = ubuf[j, mine]

            @pl.when(jnp.logical_not(cond))
            def _(j=j, m=m):
                ucol[j - 1, m] = jnp.zeros((64, 128), BF)

    def total(j, ms):
        value = ucol[j - 1, ms[0]].astype(F32)
        for m in ms[1:]:
            value = value + ucol[j - 1, m].astype(F32)
        return value

    asend[0] = total(3, list(range(COL)))
    asend[1] = total(4, list(range(COL)))
    ux = [
        send(asend.at[0 if m == 1 else 1], uxin.at[m], ux_s.at[m], ux_r.at[m], {"seq": flipped(s, bits, m << 3)})
        for m in range(1, 4)
    ]
    ux_out = [x0 == 1, x1 == 1, x1 == 1]
    for cp, cond in zip(ux, ux_out):

        @pl.when(cond)
        def _(cp=cp):
            cp.start()

    for b in range(4):
        h_make(0, b)
    for cp in (f10, f31, f30, f11):
        cp.wait_recv()
    for b in range(4):
        gbuf[b] = (hbuf[0, b].astype(F32) + fin[0, b].astype(F32) + fin[1, b].astype(F32)).astype(BF)
    gx = []
    for b in (2, 1, 3):
        cp = send(gbuf.at[b], xg.at[b], gx_s.at[b], gx_r.at[b], {"seq": off(0, b)})
        cp.start()
        gx.append(cp)

    backward(2)

    for cp, cond, m in zip(ux, ux_out, range(1, 4)):

        @pl.when(jnp.logical_not(cond))
        def _(cp=cp):
            cp.wait_recv()

        @pl.when(cond)
        def _(m=m):
            uxin[m] = jnp.zeros((64, 128), F32)

    beyond = uxin[1] + uxin[2] + uxin[3]
    for i in range(4):
        n = 4 * ((i >> 1) ^ 1)
        rsend[i] = (
            beyond + total(1, [2 * (i ^ 1), 2 * (i ^ 1) + 1]) + total(2, [n, n + 1, n + 2, n + 3])
        ).astype(BF)
    rc = []
    for m in ORDER:
        cp = send(rsend.at[m >> 1], rcol.at[mine], ur_s.at[m], ur_r.at[m], {"seq": flipped(s, bits, m)})
        cp.start()
        rc.append(cp)
    rcol[mine] = rsend[0]

    for cp in gx:
        cp.wait_recv()
    mean = gbuf[0].astype(F32) + xg[1].astype(F32) + xg[2].astype(F32) + xg[3].astype(F32)
    for i in range(8):
        part = mean[16 * (i // 2) : 16 * (i // 2) + 16, 256 * (i % 2) : 256 * (i % 2) + 256]
        zf[i] = part
        zsend[i] = part.astype(BF)
    z1 = []
    for m in ORDER:
        peer = flipped(z, zbits, m)
        cp = send(zsend.at[peer], zin.at[m], z1_s.at[m], z1_r.at[m], {"dp": peer})
        cp.start()
        z1.append(cp)

    backward(3)

    def output(n):
        at = pl.ds(512 * n, 512)
        out_ref[:, at] = dot(att[...], full[at], NT).astype(BF)

    output(0)
    output(1)

    for cp in z1:
        cp.wait_recv()
    value = zf[z]
    for m in range(1, 8):
        value = value + zin[m].astype(F32)
    zall[z] = value.astype(BF)
    z2 = []
    for m in ORDER:
        cp = send(zall.at[z], zall.at[z], z2_s.at[m], z2_r.at[m], {"dp": flipped(z, zbits, m)})
        cp.start()
        z2.append(cp)

    output(2)
    output(3)

    for cp in rc:
        cp.wait_recv()

    @pl.when(c == 0)
    def _():
        usend.wait_recv()

    @pl.when(have[0])
    def _():
        usib[...] = jnp.zeros((512, 128), BF)

    for h in range(4):
        back = (rcol[lanes(h)].astype(F32) + usib[lanes(h)].astype(F32)).astype(BF)
        gk_ref[:, lanes(h)] = (gk32[:, lanes(h)] + dot(v[:, lanes(h)], back, NT)).astype(BF)
        gv_ref[:, lanes(h)] = (gv32[:, lanes(h)] + dot(k[:, lanes(h)], back, NN)).astype(BF)
    glrow[...] = glt[...].T[:32]
    for level in range(8):
        gl_ref[level] = glrow[pl.ds(4 * level, 4)]

    for cp in z2:
        cp.wait_recv()
    for i in range(8):
        gp_ref[pl.ds(16 * (i // 2), 16), pl.ds(256 * (i % 2), 256)] = zall[i].astype(F32)

    for cp in first + open_sends + gs + [rl[1], rl[3], f10, f11, f30, f31] + rc + gx + z1 + z2:
        cp.wait_send()
    for cp, cond in early + list(zip(xsend, x_out)) + list(zip(ux, ux_out)):

        @pl.when(cond)
        def _(cp=cp):
            cp.wait_send()

    @pl.when(c == 0)
    def _():
        sib.wait_send()

    @pl.when(have[0])
    def _():
        usend.wait_send()

    for j in range(1, 5):

        @pl.when(have[j])
        def _(j=j):
            for m in ORDER:
                slice_to(j, m).wait_send()
            for cp in {3: late3, 4: late4}.get(j, []):
                cp.wait_send()


def step(query, key, value, lam, proj, grad_out):
    dma = pltpu.SemaphoreType.DMA
    any_space = pl.BlockSpec(memory_space=pl.ANY)
    inner = pl.BlockSpec(memory_space=pltpu.VMEM)
    wide = (256, 512)
    return pl.pallas_call(
        step_kernel,
        out_shape=(
            jax.ShapeDtypeStruct((256, 2048), BF),
            jax.ShapeDtypeStruct(wide, BF),
            jax.ShapeDtypeStruct(wide, BF),
            jax.ShapeDtypeStruct(wide, BF),
            jax.ShapeDtypeStruct((8, 4, 256), F32),
            jax.ShapeDtypeStruct((64, 512), F32),
        ),
        in_specs=[any_space, any_space, any_space, inner, inner, any_space],
        out_specs=(inner,) * 6,
        scratch_shapes=[
            pltpu.VMEM(wide, BF), pltpu.VMEM(wide, BF), pltpu.VMEM(wide, BF),
            pltpu.VMEM((256, 2048), BF),
            pltpu.VMEM((2, PIECES, 64, 256), BF),
            pltpu.VMEM((256, 32), F32),
            pltpu.VMEM((256, 128), F32),
            pltpu.VMEM((32, 256), F32),
            pltpu.VMEM((64, 512), BF),
            pltpu.VMEM((2048, 512), BF),
            pltpu.VMEM((5, 512, 128), BF),
            pltpu.VMEM((4, 3, 128, 128), F32),
            pltpu.VMEM((4, 3, 128, 128), BF),
            pltpu.VMEM(wide, F32),
            pltpu.VMEM(wide, BF),
            pltpu.VMEM((4, 5, 256, 128), F32),
            pltpu.VMEM(wide, BF),
            pltpu.VMEM((4, 5, 256, 128), BF),
            pltpu.VMEM(wide, F32),
            pltpu.VMEM(wide, F32),
            pltpu.VMEM((512, 128), BF),
            pltpu.VMEM((COL, 64, 128), BF),
            pltpu.VMEM((4, 64, 128), BF),
            pltpu.VMEM((2, 64, 128), BF),
            pltpu.VMEM((64, 128), F32),
            pltpu.VMEM((4, 64, 128), F32),
            pltpu.VMEM((64, 128), BF),
            pltpu.VMEM((64, 128), BF),
            pltpu.VMEM((5, 512, 128), BF),
            pltpu.VMEM((4, COL, 64, 128), BF),
            pltpu.VMEM((2, 64, 128), F32),
            pltpu.VMEM((4, 64, 128), F32),
            pltpu.VMEM((4, 64, 128), BF),
            pltpu.VMEM((512, 128), BF),
            pltpu.VMEM((512, 128), BF),
            pltpu.VMEM((PIECES, 64, 512), F32),
            pltpu.VMEM((PIECES, 64, 512), BF),
            pltpu.VMEM((PIECES, 64, 512), BF),
            pltpu.VMEM((4, 4, 64, 512), BF),
            pltpu.VMEM((2, 2, 64, 512), BF),
            pltpu.VMEM((2, 4, 64, 512), BF),
            pltpu.VMEM((4, 64, 512), BF),
            pltpu.VMEM((4, 64, 512), BF),
            pltpu.VMEM((8, 16, 256), F32),
            pltpu.VMEM((8, 16, 256), BF),
            pltpu.VMEM((8, 16, 256), BF),
            pltpu.VMEM((8, 16, 256), BF),
            dma((4,)),
            dma((36,)), dma((36,)), dma((COL,)), dma((COL,)),
            dma((5, COL)), dma((5, COL)), dma((4,)), dma((4,)), dma, dma,
            dma((4, COL)), dma((4, COL)), dma((4,)), dma((4,)), dma((COL,)), dma((COL,)), dma, dma,
            dma((PIECES,)), dma((PIECES,)), dma((2,)), dma((2,)), dma((4,)), dma((4,)),
            dma((4,)), dma((4,)), dma((8,)), dma((8,)), dma((8,)), dma((8,)),
        ],
        compiler_params=pltpu.CompilerParams(collective_id=0, has_side_effects=True),
        name="span_step",
    )(query, key, value, lam, proj, grad_out)


def shards(queries, keys, values, level_weights, proj, out_grad):
    out, gq, gk, gv, gl, gp = step(
        queries[0], keys[0], values[0], level_weights[0], proj.T, out_grad[0]
    )
    return out[None], gq[None], gk[None], gv[None], gl[None], gp.T


def solution(mesh):
    return jax.shard_map(
        shards,
        mesh=mesh,
        in_specs=(
            P("dp", "seq", None),
            P("dp", "seq", None),
            P("dp", "seq", None),
            P("dp", None, None, "seq"),
            P(None, "seq"),
            P("dp", "seq", None),
        ),
        out_specs=(
            P("dp", "seq", None),
            P("dp", "seq", None),
            P("dp", "seq", None),
            P("dp", "seq", None),
            P("dp", None, None, "seq"),
            P(None, "seq"),
        ),
        check_vma=False,
    )
```

```python
import jax
import jax.numpy as jnp
from jax import lax
from jax.experimental import pallas as pl
from jax.experimental.pallas import tpu as pltpu
from jax.sharding import PartitionSpec as P

BF = jnp.bfloat16
F32 = jnp.float32
MESH = pl.DeviceIdType.MESH
COL = 8
PIECES = 16


def place():
    s = lax.axis_index("seq")
    bits = [lax.rem(lax.div(s, 2**b), 2) for b in range(5)]
    return s, bits


def flipped(s, bits, mask):
    peer = s
    for b in range(5):
        if mask >> b & 1:
            peer = peer + 2**b * (1 - 2 * bits[b])
    return peer


def chip_offsets(s, bits):
    c, y0, y1, x0, x1 = bits
    dy0, dy1 = 2 * (1 - 2 * y0), 4 * (1 - 2 * y1)
    dx0, dx1 = 8 * (1 - 2 * x0), 16 * (1 - 2 * x1)
    da0, da1 = dy0 * (1 - c) + dx0 * c, dy1 * (1 - c) + dx1 * c
    db0, db1 = dx0 * (1 - c) + dy0 * c, dx1 * (1 - c) + dy1 * c

    def off(a, b):
        return s + (a & 1) * da0 + (a >> 1) * da1 + (b & 1) * db0 + (b >> 1) * db1

    return off


def rows(index, count):
    return pl.ds(pl.multiple_of(index * count, count), count)


def send(src, dst, ssem, rsem, device):
    return pltpu.make_async_remote_copy(
        src_ref=src, dst_ref=dst, send_sem=ssem, recv_sem=rsem, device_id=device, device_id_type=MESH
    )


def bit_of(bits, b, mask):
    return 1 - bits[b] if mask >> b & 1 else bits[b]


def dot(x, y, dims):
    return lax.dot_general(x, y, (dims, ((), ())), preferred_element_type=F32)


NN, NT, TN = ((1,), (0,)), ((1,), (1,)), ((0,), (0,))
SCALE = 128**-0.5
ORDER = (4, 5, 2, 3, 6, 7, 1)
TILES = ((0, 0), (1, 1), (1, 0))


def step_kernel(
    q_hbm, k_hbm, v_hbm, lam_hbm, proj_hbm, og_hbm,
    out_ref, gq_ref, gk_ref, gv_ref, gl_ref, gp_ref,
    q, k, v, og, ogt, lamt, glt, glrow, lam_in, shard_buf, full, states, score, prob, att32, att, mapped, ga, wt, gk32, gv32,
    tot, col, pair, quad, csum, xin, s3buf, s4buf,
    ubuf, ucol, asend, uxin, rsend, rcol, usib,
    g32, gbf, gsib, hbuf, rel, fin, gbuf, xg, zf, zsend, zin, zall,
    ld, ag_s, ag_r, c1_s, c1_r, st_s, st_r, x_s, x_r, sib_s, sib_r,
    u_s, u_r, ux_s, ux_r, ur_s, ur_r, us_s, us_r,
    gs_s, gs_r, rl_s, rl_r, fn_s, fn_r, gx_s, gx_r, z1_s, z1_r, z2_s, z2_r,
):
    s, bits = place()
    c, y0, y1, x0, x1 = bits
    z = lax.axis_index("dp")
    zbits = [lax.rem(lax.div(z, 2**b), 2) for b in range(3)] + [0, 0]
    r = lax.rem(s, COL)
    mine = rows(r, 64)
    off = chip_offsets(s, bits)
    have = [c == 1, y0 == 1, y1 == 1, x0 == 1, x1 == 1]
    sib_index = flipped(s, bits, 1)
    sibling = {"seq": sib_index}

    loads = [
        pltpu.make_async_copy(src, dst, ld.at[i])
        for i, (src, dst) in enumerate(
            ((k_hbm, k), (v_hbm, v), (q_hbm, q), (og_hbm, og), (proj_hbm, shard_buf), (lam_hbm, lam_in))
        )
    ]
    for cp in loads:
        cp.start()

    greeted = (
        [{"seq": flipped(s, bits, m)} for m in range(1, 8)]
        + [{"seq": flipped(s, bits, m << 3)} for m in range(1, 4)]
        + [{"dp": flipped(z, zbits, m)} for m in range(1, 8)]
    )
    barrier = pltpu.get_barrier_semaphore()
    for device in greeted:
        pl.semaphore_signal(barrier, inc=1, device_id=device, device_id_type=MESH)

    def lanes(h):
        return pl.ds(128 * h, 128)

    loads[0].wait()
    loads[1].wait()
    for h in range(4):
        tot[lanes(h)] = dot(k[:, lanes(h)], v[:, lanes(h)], TN).astype(BF)
    pl.semaphore_wait(barrier, len(greeted))

    first = []
    for m in ORDER:
        peer = flipped(s, bits, m)
        cp = send(tot.at[rows(lax.rem(peer, COL), 64)], col.at[m], c1_s.at[m], c1_r.at[m], {"seq": peer})
        cp.start()
        first.append(cp)
    sib = send(tot, states.at[0], sib_s, sib_r, sibling)

    @pl.when(c == 0)
    def _():
        sib.start()

    open_sends = []

    def block(index):
        return full.at[rows(index, 64)]

    def ag(slot, src, index, device):
        cp = send(src, block(index), ag_s.at[slot], ag_r.at[slot], device)
        cp.start()
        open_sends.append(cp)

    def ag_arrived(slot):
        send(shard_buf, block(s), ag_s.at[slot], ag_r.at[slot], sibling).wait_recv()

    def chip(a, b):
        return flipped(s, bits, a << 1 | b << 3)

    loads[4].wait()
    full[rows(s, 64)] = shard_buf[...]
    for a in (1, 3, 2):
        ag(a, shard_buf, s, {"seq": chip(a, 0)})
    for b in (1, 3):
        ag(4 + b, shard_buf, s, {"seq": chip(0, b)})
    ag(20, shard_buf, s, sibling)

    row = lax.broadcasted_iota(jnp.int32, (128, 128), 0)
    column = lax.broadcasted_iota(jnp.int32, (128, 128), 1)
    causal = column <= row
    near = causal & ((row < 64) | (column >= 64))
    far = causal & (row >= 64) & (column < 64)

    def half(i):
        return pl.ds(128 * i, 128)

    def lam(level, h, where):
        return lamt[where, pl.ds(4 * level + h, 1)]

    def weight(h, i, j):
        if i != j:
            return SCALE * lam(2, h, half(i))
        return SCALE * jnp.where(near, lam(0, h, half(i)), jnp.where(far, lam(1, h, half(i)), 0.0))

    def inside(h):
        for n, (i, j) in enumerate(TILES):
            value = dot(q[half(i), lanes(h)], k[half(j), lanes(h)], NT)
            score[h, n] = value
            prob[h, n] = (weight(h, i, j) * value).astype(BF)
        att32[half(0), lanes(h)] = dot(prob[h, 0], v[half(0), lanes(h)], NN)
        att32[half(1), lanes(h)] = dot(prob[h, 1], v[half(1), lanes(h)], NN) + dot(
            prob[h, 2], v[half(0), lanes(h)], NN
        )

    loads[5].wait()
    for level in range(8):
        glrow[pl.ds(4 * level, 4)] = lam_in[level]
    lamt[...] = glrow[...].T
    loads[2].wait()
    inside(0)
    inside(1)

    for cp in first:
        cp.wait_recv()
    col[0] = tot[mine]
    t = [col[m].astype(F32) for m in range(COL)]
    p = [t[2 * i] + t[2 * i + 1] for i in range(4)]
    qd = [p[0] + p[1], p[2] + p[3]]
    csum[...] = qd[0] + qd[1]
    xsend = [
        send(csum, xin.at[m], x_s.at[m], x_r.at[m], {"seq": flipped(s, bits, m << 3)}) for m in range(1, 4)
    ]
    x_out = [x0 == 0, x1 == 0, x1 == 0]
    for cp, cond in zip(xsend, x_out):

        @pl.when(cond)
        def _(cp=cp):
            cp.start()

    for i in range(4):
        pair[i] = p[i].astype(BF)
    for i in range(2):
        quad[i] = qd[i].astype(BF)

    def spread(j, m, src):
        return send(src, states.at[j, mine], st_s.at[j, m], st_r.at[j, m], {"seq": flipped(s, bits, m)})

    early = []
    for m in ORDER:
        early.append((spread(1, m, pair.at[(m >> 1) ^ 1]), bit_of(bits, 1, m) == 1))
        early.append((spread(2, m, quad.at[(m >> 2) ^ 1]), bit_of(bits, 2, m) == 1))
    for cp, cond in early:

        @pl.when(cond)
        def _(cp=cp):
            cp.start()

    for j in range(5):

        @pl.when(jnp.logical_not(have[j]))
        def _(j=j):
            states[j] = jnp.zeros((512, 128), BF)

    @pl.when(have[1])
    def _():
        states[1, mine] = pair[1]

    @pl.when(have[2])
    def _():
        states[2, mine] = quad[1]

    def first_axis(a):
        ag_arrived(a)
        for b in (1, 3):
            ag(4 + 4 * a + b, block(chip(a, 0)), chip(a, 0), {"seq": chip(0, b)})
        ag(20 + 4 * a, block(chip(a, 0)), chip(a, 0), sibling)

    def second_axis(a):
        for b in (1, 3):
            ag_arrived(4 + 4 * a + b)
            if (b == 1) == (a < 2):
                ag(4 + 4 * a + 2, block(chip(a, b)), chip(a, b), {"seq": chip(0, 4 - b)})
            ag(20 + 4 * a + b, block(chip(a, b)), chip(a, b), sibling)

    first_axis(1)
    first_axis(3)

    inside(2)

    late3 = [spread(3, m, s3buf) for m in ORDER]
    late4 = [spread(4, m, s4buf) for m in ORDER]

    @pl.when(have[3])
    def _():
        xsend[0].wait_recv()
        s3buf[...] = xin[1].astype(BF)
        for cp in late3:
            cp.start()
        states[3, mine] = s3buf[...]

    @pl.when(have[4])
    def _():
        xsend[1].wait_recv()
        xsend[2].wait_recv()
        s4buf[...] = (xin[2] + xin[3]).astype(BF)
        for cp in late4:
            cp.start()
        states[4, mine] = s4buf[...]

    first_axis(2)
    second_axis(0)

    inside(3)
    loads[3].wait()
    for n in range(16):
        turned = og[:, pl.ds(128 * n, 128)].T
        ogt[0, n] = turned[:64]
        ogt[1, n] = turned[64:]

    second_axis(1)

    @pl.when(have[0])
    def _():
        sib.wait_recv()

    for j in range(1, 5):

        @pl.when(have[j])
        def _(j=j):
            for m in ORDER:
                spread(j, m, s4buf).wait_recv()

    for h in range(4):
        cross = jnp.zeros((256, 128), F32)
        for j in range(5):
            image = dot(q[:, lanes(h)], states[j, lanes(h)], NN)
            mapped[h, j] = image
            cross = cross + lam(3 + j, h, pl.ds(0, 256)) * image
        att[:, lanes(h)] = (att32[:, lanes(h)] + SCALE * cross).astype(BF)

    other = 1 - c
    for n in range(4):
        part = pl.ds(4 * n, 4)
        gbf[part] = dot(ogt[other, part].reshape(256, 256), att[...], NN).astype(BF).reshape(4, 64, 512)
    gs = []
    for a in (2, 1, 3, 0):
        for b in range(4):
            slot = 4 * b + a
            cp = send(gbf.at[lax.div(off(a, b), 2)], gsib.at[slot], gs_s.at[slot], gs_r.at[slot], sibling)
            cp.start()
            gs.append(cp)
    for n in range(4):
        part = pl.ds(4 * n, 4)
        g32[part] = dot(ogt[c, part].reshape(256, 256), att[...], NN).reshape(4, 64, 512)

    second_axis(3)
    second_axis(2)

    def h_make(a, b):
        slot = 4 * a + b
        send(gbf.at[0], gsib.at[slot], gs_s.at[slot], gs_r.at[slot], sibling).wait_recv()
        hbuf[a, b] = (g32[lax.div(off(a, b), 2)] + gsib[slot].astype(F32)).astype(BF)

    dev_a = {1: {"seq": off(1, 0)}, 3: {"seq": off(3, 0)}}
    for b in range(4):
        h_make(2, b)
    rl = {
        1: send(hbuf.at[2, pl.ds(0, 2)], rel.at[0], rl_s.at[0], rl_r.at[0], dev_a[1]),
        3: send(hbuf.at[2, pl.ds(2, 2)], rel.at[1], rl_s.at[1], rl_r.at[1], dev_a[3]),
    }
    rl[1].start()
    rl[3].start()

    def final(m, part):
        n = 2 * (m // 2) + part
        return send(
            hbuf.at[m, pl.ds(2 * part, 2)], fin.at[m // 2, pl.ds(2 * part, 2)], fn_s.at[n], fn_r.at[n], dev_a[m]
        )

    h_make(1, 0)
    h_make(1, 1)
    f10 = final(1, 0)
    f10.start()
    h_make(3, 2)
    h_make(3, 3)
    f31 = final(3, 1)
    f31.start()

    for a in (0, 1, 3, 2):
        ag_arrived(4 + 4 * a + 2)
        ag(20 + 4 * a + 2, block(chip(a, 2)), chip(a, 2), sibling)

    for a in range(4):
        for b in range(4):
            ag_arrived(20 + 4 * a + b)
    for b in range(2):
        h_make(3, b)
    rl[1].wait_recv()
    for b in range(2):
        hbuf[3, b] = (hbuf[3, b].astype(F32) + rel[0, b].astype(F32)).astype(BF)
    f30 = final(3, 0)
    f30.start()
    for b in range(2):
        h_make(1, 2 + b)
    rl[3].wait_recv()
    for b in range(2):
        hbuf[1, 2 + b] = (hbuf[1, 2 + b].astype(F32) + rel[1, b].astype(F32)).astype(BF)
    f11 = final(1, 1)
    f11.start()

    ga[...] = dot(og[...], full[...], NN).astype(BF)
    for h in range(4):
        g = ga[:, lanes(h)].astype(F32)
        for j in range(5):
            wt[h, j] = (SCALE * lam(3 + j, h, pl.ds(0, 256)) * g).astype(BF)
            ubuf[j, lanes(h)] = dot(q[:, lanes(h)], wt[h, j], TN).astype(BF)

    usend = send(ubuf.at[0], usib, us_s, us_r, sibling)

    @pl.when(have[0])
    def _():
        usend.start()

    def slice_to(j, m):
        peer = flipped(s, bits, m)
        return send(
            ubuf.at[j, rows(lax.rem(peer, COL), 64)],
            ucol.at[j - 1, m],
            u_s.at[j - 1, m],
            u_r.at[j - 1, m],
            {"seq": peer},
        )

    for j in (4, 3, 2, 1):

        @pl.when(have[j])
        def _(j=j):
            for m in ORDER:
                slice_to(j, m).start()

    place_of = lax.broadcasted_iota(jnp.int32, (128, 128), 1)

    def sums(value):
        return jnp.sum(value, axis=1, keepdims=True)

    def backward(h):
        ds = []
        got = {}
        for n, (i, j) in enumerate(TILES):
            dp = dot(ga[half(i), lanes(h)], v[half(j), lanes(h)], NT)
            ds.append((weight(h, i, j) * dp).astype(BF))
            product = SCALE * score[h, n] * dp
            if i != j:
                got[2, i] = sums(product)
            else:
                got[0, i] = sums(jnp.where(near, product, 0.0))
                got[1, i] = sums(jnp.where(far, product, 0.0))
        for i in range(2):
            g = ga[half(i), lanes(h)].astype(F32)
            acc = glt[half(i)]
            for level in range(8):
                if level > 2:
                    value = SCALE * sums(g * mapped[h, level - 3, half(i)])
                elif (level, i) in got:
                    value = got[level, i]
                else:
                    continue
                acc = jnp.where(place_of == 4 * level + h, value, acc)
            glt[half(i)] = acc
        gq = [dot(ds[0], k[half(0), lanes(h)], NN), dot(ds[1], k[half(1), lanes(h)], NN)]
        gq[1] = gq[1] + dot(ds[2], k[half(0), lanes(h)], NN)
        for i in range(2):
            for j in range(5):
                gq[i] = gq[i] + dot(wt[h, j, half(i)], states[j, lanes(h)], NT)
            gq_ref[half(i), lanes(h)] = gq[i].astype(BF)
        q0, q1 = q[half(0), lanes(h)], q[half(1), lanes(h)]
        g0, g1 = ga[half(0), lanes(h)], ga[half(1), lanes(h)]
        gk32[half(0), lanes(h)] = dot(ds[0], q0, TN) + dot(ds[2], q1, TN)
        gk32[half(1), lanes(h)] = dot(ds[1], q1, TN)
        gv32[half(0), lanes(h)] = dot(prob[h, 0], g0, TN) + dot(prob[h, 2], g1, TN)
        gv32[half(1), lanes(h)] = dot(prob[h, 1], g1, TN)

    glt[...] = jnp.zeros_like(glt)
    backward(0)
    backward(1)

    for b in range(4):
        h_make(0, b)
    for cp in (f10, f31, f30, f11):
        cp.wait_recv()
    for b in range(4):
        gbuf[b] = (hbuf[0, b].astype(F32) + fin[0, b].astype(F32) + fin[1, b].astype(F32)).astype(BF)
    gx = []
    for b in (2, 1, 3):
        cp = send(gbuf.at[b], xg.at[b], gx_s.at[b], gx_r.at[b], {"seq": off(0, b)})
        cp.start()
        gx.append(cp)

    for j in range(1, 5):
        for m in range(COL):
            cond = bit_of(bits, j, m) == 1 if j < 3 else have[j]

            @pl.when(cond)
            def _(j=j, m=m):
                if m:
                    slice_to(j, m).wait_recv()
                else:
                    ucol[j - 1, 0] = ubuf[j, mine]

            @pl.when(jnp.logical_not(cond))
            def _(j=j, m=m):
                ucol[j - 1, m] = jnp.zeros((64, 128), BF)

    def total(j, ms):
        value = ucol[j - 1, ms[0]].astype(F32)
        for m in ms[1:]:
            value = value + ucol[j - 1, m].astype(F32)
        return value

    asend[0] = total(3, list(range(COL)))
    asend[1] = total(4, list(range(COL)))
    ux = [
        send(asend.at[0 if m == 1 else 1], uxin.at[m], ux_s.at[m], ux_r.at[m], {"seq": flipped(s, bits, m << 3)})
        for m in range(1, 4)
    ]
    ux_out = [x0 == 1, x1 == 1, x1 == 1]
    for cp, cond in zip(ux, ux_out):

        @pl.when(cond)
        def _(cp=cp):
            cp.start()

    backward(2)

    for cp in gx:
        cp.wait_recv()
    mean = gbuf[0].astype(F32) + xg[1].astype(F32) + xg[2].astype(F32) + xg[3].astype(F32)
    for i in range(8):
        part = mean[16 * (i // 2) : 16 * (i // 2) + 16, 256 * (i % 2) : 256 * (i % 2) + 256]
        zf[i] = part
        zsend[i] = part.astype(BF)
    z1 = []
    for m in ORDER:
        peer = flipped(z, zbits, m)
        cp = send(zsend.at[peer], zin.at[m], z1_s.at[m], z1_r.at[m], {"dp": peer})
        cp.start()
        z1.append(cp)

    for cp, cond, m in zip(ux, ux_out, range(1, 4)):

        @pl.when(jnp.logical_not(cond))
        def _(cp=cp):
            cp.wait_recv()

        @pl.when(cond)
        def _(m=m):
            uxin[m] = jnp.zeros((64, 128), F32)

    beyond = uxin[1] + uxin[2] + uxin[3]
    for i in range(4):
        n = 4 * ((i >> 1) ^ 1)
        rsend[i] = (
            beyond + total(1, [2 * (i ^ 1), 2 * (i ^ 1) + 1]) + total(2, [n, n + 1, n + 2, n + 3])
        ).astype(BF)
    rc = []
    for m in ORDER:
        cp = send(rsend.at[m >> 1], rcol.at[mine], ur_s.at[m], ur_r.at[m], {"seq": flipped(s, bits, m)})
        cp.start()
        rc.append(cp)
    rcol[mine] = rsend[0]

    backward(3)

    def output(n):
        at = pl.ds(512 * n, 512)
        out_ref[:, at] = dot(att[...], full[at], NT).astype(BF)

    output(0)
    output(1)

    for cp in z1:
        cp.wait_recv()
    value = zf[z]
    for m in range(1, 8):
        value = value + zin[m].astype(F32)
    zall[z] = value.astype(BF)
    z2 = []
    for m in ORDER:
        cp = send(zall.at[z], zall.at[z], z2_s.at[m], z2_r.at[m], {"dp": flipped(z, zbits, m)})
        cp.start()
        z2.append(cp)

    output(2)
    output(3)

    for cp in rc:
        cp.wait_recv()

    @pl.when(c == 0)
    def _():
        usend.wait_recv()

    @pl.when(have[0])
    def _():
        usib[...] = jnp.zeros((512, 128), BF)

    for h in range(4):
        back = (rcol[lanes(h)].astype(F32) + usib[lanes(h)].astype(F32)).astype(BF)
        gk_ref[:, lanes(h)] = (gk32[:, lanes(h)] + dot(v[:, lanes(h)], back, NT)).astype(BF)
        gv_ref[:, lanes(h)] = (gv32[:, lanes(h)] + dot(k[:, lanes(h)], back, NN)).astype(BF)
    glrow[...] = glt[...].T[:32]
    for level in range(8):
        gl_ref[level] = glrow[pl.ds(4 * level, 4)]

    for cp in z2:
        cp.wait_recv()
    for i in range(8):
        gp_ref[pl.ds(16 * (i // 2), 16), pl.ds(256 * (i % 2), 256)] = zall[i].astype(F32)

    for cp in first + open_sends + gs + [rl[1], rl[3], f10, f11, f30, f31] + rc + gx + z1 + z2:
        cp.wait_send()
    for cp, cond in early + list(zip(xsend, x_out)) + list(zip(ux, ux_out)):

        @pl.when(cond)
        def _(cp=cp):
            cp.wait_send()

    @pl.when(c == 0)
    def _():
        sib.wait_send()

    @pl.when(have[0])
    def _():
        usend.wait_send()

    for j in range(1, 5):

        @pl.when(have[j])
        def _(j=j):
            for m in ORDER:
                slice_to(j, m).wait_send()
            for cp in {3: late3, 4: late4}.get(j, []):
                cp.wait_send()


def step(query, key, value, lam, proj, grad_out):
    dma = pltpu.SemaphoreType.DMA
    outer = pl.BlockSpec(memory_space=pltpu.HBM)
    inner = pl.BlockSpec(memory_space=pltpu.VMEM)
    wide = (256, 512)
    return pl.pallas_call(
        step_kernel,
        out_shape=(
            jax.ShapeDtypeStruct((256, 2048), BF),
            jax.ShapeDtypeStruct(wide, BF),
            jax.ShapeDtypeStruct(wide, BF),
            jax.ShapeDtypeStruct(wide, BF),
            jax.ShapeDtypeStruct((8, 4, 256), F32),
            jax.ShapeDtypeStruct((64, 512), F32),
        ),
        in_specs=[outer] * 6,
        out_specs=(inner,) * 6,
        scratch_shapes=[
            pltpu.VMEM(wide, BF), pltpu.VMEM(wide, BF), pltpu.VMEM(wide, BF),
            pltpu.VMEM((256, 2048), BF),
            pltpu.VMEM((2, PIECES, 64, 256), BF),
            pltpu.VMEM((256, 32), F32),
            pltpu.VMEM((256, 128), F32),
            pltpu.VMEM((32, 256), F32),
            pltpu.VMEM((8, 4, 256), F32),
            pltpu.VMEM((64, 512), BF),
            pltpu.VMEM((2048, 512), BF),
            pltpu.VMEM((5, 512, 128), BF),
            pltpu.VMEM((4, 3, 128, 128), F32),
            pltpu.VMEM((4, 3, 128, 128), BF),
            pltpu.VMEM(wide, F32),
            pltpu.VMEM(wide, BF),
            pltpu.VMEM((4, 5, 256, 128), F32),
            pltpu.VMEM(wide, BF),
            pltpu.VMEM((4, 5, 256, 128), BF),
            pltpu.VMEM(wide, F32),
            pltpu.VMEM(wide, F32),
            pltpu.VMEM((512, 128), BF),
            pltpu.VMEM((COL, 64, 128), BF),
            pltpu.VMEM((4, 64, 128), BF),
            pltpu.VMEM((2, 64, 128), BF),
            pltpu.VMEM((64, 128), F32),
            pltpu.VMEM((4, 64, 128), F32),
            pltpu.VMEM((64, 128), BF),
            pltpu.VMEM((64, 128), BF),
            pltpu.VMEM((5, 512, 128), BF),
            pltpu.VMEM((4, COL, 64, 128), BF),
            pltpu.VMEM((2, 64, 128), F32),
            pltpu.VMEM((4, 64, 128), F32),
            pltpu.VMEM((4, 64, 128), BF),
            pltpu.VMEM((512, 128), BF),
            pltpu.VMEM((512, 128), BF),
            pltpu.VMEM((PIECES, 64, 512), F32),
            pltpu.VMEM((PIECES, 64, 512), BF),
            pltpu.VMEM((PIECES, 64, 512), BF),
            pltpu.VMEM((4, 4, 64, 512), BF),
            pltpu.VMEM((2, 2, 64, 512), BF),
            pltpu.VMEM((2, 4, 64, 512), BF),
            pltpu.VMEM((4, 64, 512), BF),
            pltpu.VMEM((4, 64, 512), BF),
            pltpu.VMEM((8, 16, 256), F32),
            pltpu.VMEM((8, 16, 256), BF),
            pltpu.VMEM((8, 16, 256), BF),
            pltpu.VMEM((8, 16, 256), BF),
            dma((6,)),
            dma((36,)), dma((36,)), dma((COL,)), dma((COL,)),
            dma((5, COL)), dma((5, COL)), dma((4,)), dma((4,)), dma, dma,
            dma((4, COL)), dma((4, COL)), dma((4,)), dma((4,)), dma((COL,)), dma((COL,)), dma, dma,
            dma((PIECES,)), dma((PIECES,)), dma((2,)), dma((2,)), dma((4,)), dma((4,)),
            dma((4,)), dma((4,)), dma((8,)), dma((8,)), dma((8,)), dma((8,)),
        ],
        compiler_params=pltpu.CompilerParams(collective_id=0, has_side_effects=True, vmem_limit_bytes=36 * 2**20),
        name="span_step",
    )(query, key, value, lam, proj, grad_out)


def deliver_kernel(*refs):
    count = len(refs) // 2
    sems = refs[-1]
    copies = [pltpu.make_async_copy(refs[i], refs[count + i], sems.at[i]) for i in range(count)]
    for cp in copies:
        cp.start()
    for cp in copies:
        cp.wait()


def deliver(arrays):
    return pl.pallas_call(
        deliver_kernel,
        out_shape=[jax.ShapeDtypeStruct(x.shape, x.dtype) for x in arrays],
        in_specs=[pl.BlockSpec(memory_space=pltpu.VMEM)] * len(arrays),
        out_specs=[pl.BlockSpec(memory_space=pltpu.HBM)] * len(arrays),
        scratch_shapes=[pltpu.SemaphoreType.DMA((len(arrays),))],
        compiler_params=pltpu.CompilerParams(vmem_limit_bytes=2**20),
        name="deliver",
    )(*arrays)


def shards(queries, keys, values, level_weights, proj, out_grad):
    out, gq, gk, gv, gl, gp = deliver(
        step(
            *[
                pltpu.with_memory_space_constraint(x, pltpu.HBM)
                for x in (queries[0], keys[0], values[0], level_weights[0], proj.T, out_grad[0])
            ]
        )
    )
    return out[None], gq[None], gk[None], gv[None], gl[None], gp.T


def solution(mesh):
    return jax.shard_map(
        shards,
        mesh=mesh,
        in_specs=(
            P("dp", "seq", None),
            P("dp", "seq", None),
            P("dp", "seq", None),
            P("dp", None, None, "seq"),
            P(None, "seq"),
            P("dp", "seq", None),
        ),
        out_specs=(
            P("dp", "seq", None),
            P("dp", "seq", None),
            P("dp", "seq", None),
            P("dp", "seq", None),
            P("dp", None, None, "seq"),
            P(None, "seq"),
        ),
        check_vma=False,
    )
```

```python
import jax
import jax.numpy as jnp
from jax import lax
from jax.experimental import pallas as pl
from jax.experimental.pallas import tpu as pltpu
from jax.sharding import PartitionSpec as P

BF = jnp.bfloat16
F32 = jnp.float32
MESH = pl.DeviceIdType.MESH
COL = 8
PIECES = 16


def place():
    s = lax.axis_index("seq")
    bits = [lax.rem(lax.div(s, 2**b), 2) for b in range(5)]
    return s, bits


def flipped(s, bits, mask):
    peer = s
    for b in range(5):
        if mask >> b & 1:
            peer = peer + 2**b * (1 - 2 * bits[b])
    return peer


def chip_offsets(s, bits):
    c, y0, y1, x0, x1 = bits
    dy0, dy1 = 2 * (1 - 2 * y0), 4 * (1 - 2 * y1)
    dx0, dx1 = 8 * (1 - 2 * x0), 16 * (1 - 2 * x1)
    da0, da1 = dy0 * (1 - c) + dx0 * c, dy1 * (1 - c) + dx1 * c
    db0, db1 = dx0 * (1 - c) + dy0 * c, dx1 * (1 - c) + dy1 * c

    def off(a, b):
        return s + (a & 1) * da0 + (a >> 1) * da1 + (b & 1) * db0 + (b >> 1) * db1

    return off


def rows(index, count):
    return pl.ds(pl.multiple_of(index * count, count), count)


def send(src, dst, ssem, rsem, device):
    return pltpu.make_async_remote_copy(
        src_ref=src, dst_ref=dst, send_sem=ssem, recv_sem=rsem, device_id=device, device_id_type=MESH
    )


def bit_of(bits, b, mask):
    return 1 - bits[b] if mask >> b & 1 else bits[b]


def dot(x, y, dims):
    return lax.dot_general(x, y, (dims, ((), ())), preferred_element_type=F32)


NN, NT, TN = ((1,), (0,)), ((1,), (1,)), ((0,), (0,))
SCALE = 128**-0.5
ORDER = (4, 5, 2, 3, 6, 7, 1)
TILES = ((0, 0), (1, 1), (1, 0))


def step_kernel(
    q_hbm, k_hbm, v_hbm, lam_hbm, proj_hbm, og_hbm,
    out_ref, gq_ref, gk_ref, gv_ref, gl_ref, gp_ref,
    q, k, v, og, ogt, lamt, glt, glrow, lam_in, shard_buf, full, states, score, prob, att32, att, mapped, ga, wt, gk32, gv32,
    tot, col, pair, quad, csum, xin, s3buf, s4buf,
    ubuf, upre, upsum, ucol, asend, uxin, rsend, rcol, usib,
    g32, gbf, gsib, hbuf, rel, fin, gbuf, xg, zf, zsend, zin, zall,
    ld, ag_s, ag_r, c1_s, c1_r, st_s, st_r, x_s, x_r, sib_s, sib_r,
    uh_s, uh_r, u_s, u_r, ux_s, ux_r, ur_s, ur_r, us_s, us_r, rj_s, rj_r,
    gs_s, gs_r, rl_s, rl_r, fn_s, fn_r, gx_s, gx_r, z1_s, z1_r, z2_s, z2_r,
):
    s, bits = place()
    c, y0, y1, x0, x1 = bits
    z = lax.axis_index("dp")
    zbits = [lax.rem(lax.div(z, 2**b), 2) for b in range(3)] + [0, 0]
    r = lax.rem(s, COL)
    mine = rows(r, 64)
    off = chip_offsets(s, bits)
    have = [c == 1, y0 == 1, y1 == 1, x0 == 1, x1 == 1]
    sib_index = flipped(s, bits, 1)
    sibling = {"seq": sib_index}

    loads = [
        pltpu.make_async_copy(src, dst, ld.at[i])
        for i, (src, dst) in enumerate(
            ((k_hbm, k), (v_hbm, v), (q_hbm, q), (og_hbm, og), (proj_hbm, shard_buf), (lam_hbm, lam_in))
        )
    ]
    for cp in loads:
        cp.start()

    greeted = (
        [{"seq": flipped(s, bits, m)} for m in range(1, 8)]
        + [{"seq": flipped(s, bits, m << 3)} for m in range(1, 4)]
        + [{"dp": flipped(z, zbits, m)} for m in range(1, 8)]
    )
    barrier = pltpu.get_barrier_semaphore()
    for device in greeted:
        pl.semaphore_signal(barrier, inc=1, device_id=device, device_id_type=MESH)

    def lanes(h):
        return pl.ds(128 * h, 128)

    loads[0].wait()
    loads[1].wait()
    for h in range(4):
        tot[lanes(h)] = dot(k[:, lanes(h)], v[:, lanes(h)], TN).astype(BF)
    pl.semaphore_wait(barrier, len(greeted))

    first = []
    for m in ORDER:
        peer = flipped(s, bits, m)
        cp = send(tot.at[rows(lax.rem(peer, COL), 64)], col.at[m], c1_s.at[m], c1_r.at[m], {"seq": peer})
        cp.start()
        first.append(cp)
    sib = send(tot, states.at[0], sib_s, sib_r, sibling)

    @pl.when(c == 0)
    def _():
        sib.start()

    open_sends = []

    def block(index):
        return full.at[rows(index, 64)]

    def ag(slot, src, index, device):
        cp = send(src, block(index), ag_s.at[slot], ag_r.at[slot], device)
        cp.start()
        open_sends.append(cp)

    def ag_arrived(slot):
        send(shard_buf, block(s), ag_s.at[slot], ag_r.at[slot], sibling).wait_recv()

    def chip(a, b):
        return flipped(s, bits, a << 1 | b << 3)

    loads[4].wait()
    full[rows(s, 64)] = shard_buf[...]
    for a in (1, 3, 2):
        ag(a, shard_buf, s, {"seq": chip(a, 0)})
    ag(20, shard_buf, s, sibling)

    odd = zbits[0]
    dz = ({"dp": lax.rem(z + 1, 8)}, {"dp": lax.rem(z + 7, 8)})

    def piece(a, b):
        turn = 1 - odd if a & 1 else odd
        return chip(a & 2, b) + 2 * (1 - 2 * y0) * turn

    along = {}
    for a in (0, 2):
        for b in (1, 3):
            slot = 4 + 4 * a + b
            at = block(piece(a, 0))
            along[a, b] = send(at, at, ag_s.at[slot], ag_r.at[slot], {"seq": chip(0, b)})
            open_sends.append(along[a, b])

    def set_out(*labels):
        for a in labels:
            along[a, 1].start()
            along[a, 3].start()

    @pl.when(odd == 0)
    def _():
        set_out(0)


    row = lax.broadcasted_iota(jnp.int32, (128, 128), 0)
    column = lax.broadcasted_iota(jnp.int32, (128, 128), 1)
    causal = column <= row
    near = causal & ((row < 64) | (column >= 64))
    far = causal & (row >= 64) & (column < 64)

    def half(i):
        return pl.ds(128 * i, 128)

    def lam(level, h, where):
        return lamt[where, pl.ds(4 * level + h, 1)]

    def weight(h, i, j):
        if i != j:
            return SCALE * lam(2, h, half(i))
        return SCALE * jnp.where(near, lam(0, h, half(i)), jnp.where(far, lam(1, h, half(i)), 0.0))

    def inside(h):
        for n, (i, j) in enumerate(TILES):
            value = dot(q[half(i), lanes(h)], k[half(j), lanes(h)], NT)
            score[h, n] = value
            prob[h, n] = (weight(h, i, j) * value).astype(BF)
        att32[half(0), lanes(h)] = dot(prob[h, 0], v[half(0), lanes(h)], NN)
        att32[half(1), lanes(h)] = dot(prob[h, 1], v[half(1), lanes(h)], NN) + dot(
            prob[h, 2], v[half(0), lanes(h)], NN
        )

    loads[5].wait()
    for level in range(8):
        glrow[pl.ds(4 * level, 4)] = lam_in[level]
    lamt[...] = glrow[...].T
    loads[2].wait()
    inside(0)
    inside(1)

    for cp in first:
        cp.wait_recv()
    col[0] = tot[mine]
    t = [col[m].astype(F32) for m in range(COL)]
    p = [t[2 * i] + t[2 * i + 1] for i in range(4)]
    qd = [p[0] + p[1], p[2] + p[3]]
    csum[...] = qd[0] + qd[1]
    xsend = [
        send(csum, xin.at[m], x_s.at[m], x_r.at[m], {"seq": flipped(s, bits, m << 3)}) for m in range(1, 4)
    ]
    x_out = [x0 == 0, x1 == 0, x1 == 0]
    for cp, cond in zip(xsend, x_out):

        @pl.when(cond)
        def _(cp=cp):
            cp.start()

    for i in range(4):
        pair[i] = p[i].astype(BF)
    for i in range(2):
        quad[i] = qd[i].astype(BF)

    def spread(j, m, src):
        return send(src, states.at[j, mine], st_s.at[j, m], st_r.at[j, m], {"seq": flipped(s, bits, m)})

    early = []
    for m in (4, 2, 6, 1):
        early.append((spread(1, m, pair.at[(m >> 1) ^ 1]), bit_of(bits, 1, m) == 1))
        early.append((spread(2, m, quad.at[(m >> 2) ^ 1]), bit_of(bits, 2, m) == 1))
    for cp, cond in early:

        @pl.when(cond)
        def _(cp=cp):
            cp.start()

    def hand_over(j, i):
        at = states.at[j, rows(lax.rem(flipped(s, bits, 2 * i), COL), 64)]
        return send(at, at, st_s.at[j, 2 * i + 1], st_r.at[j, 2 * i + 1], sibling)

    def handed(j):
        for i in (2, 1, 3):
            spread(j, 2 * i, s4buf).wait_recv()
            hand_over(j, i).start()

    for j in range(5):

        @pl.when(jnp.logical_not(have[j]))
        def _(j=j):
            states[j] = jnp.zeros((512, 128), BF)

    @pl.when(have[1])
    def _():
        states[1, mine] = pair[1]

    @pl.when(have[2])
    def _():
        states[2, mine] = quad[1]

    def first_axis(a):
        ag_arrived(a)
        ag(20 + 4 * a, block(chip(a, 0)), chip(a, 0), sibling)

    def pass_on(a, b):
        ag(36 + 2 * a + b, block(piece(a, b)), piece(a, b), dz[a >> 1])
        ag(20 + 4 * a + b, block(piece(a, b)), piece(a, b), sibling)

    def second_axis(a):
        for b in (1, 3):
            ag_arrived(4 + 4 * a + b)
            if (b == 1) == (a == 0):
                ag(4 + 4 * a + 2, block(piece(a, b)), piece(a, b), {"seq": chip(0, 4 - b)})
            pass_on(a, b)

    def far_chip(a):
        ag_arrived(4 + 4 * a + 2)
        pass_on(a, 2)

    def other_plane(a, b):
        ag_arrived(36 + 2 * a + b)
        ag(24 + 4 * a + b, block(piece(a + 1, b)), piece(a + 1, b), sibling)

    first_axis(1)
    first_axis(3)

    @pl.when(odd == 1)
    def _():
        set_out(0, 2)

    inside(2)

    late3 = [spread(3, m, s3buf) for m in ORDER]
    late4 = [spread(4, m, s4buf) for m in ORDER]

    @pl.when(have[3])
    def _():
        xsend[0].wait_recv()
        s3buf[...] = xin[1].astype(BF)
        for cp in late3:
            cp.start()
        states[3, mine] = s3buf[...]

    @pl.when(have[4])
    def _():
        xsend[1].wait_recv()
        xsend[2].wait_recv()
        s4buf[...] = (xin[2] + xin[3]).astype(BF)
        for cp in late4:
            cp.start()
        states[4, mine] = s4buf[...]

    first_axis(2)

    @pl.when(odd == 0)
    def _():
        set_out(2)

    inside(3)
    loads[3].wait()
    for a in range(4):
        for b in range(4):
            turned = og[:, rows(lax.div(off(a, b), 2), 128)].T
            ogt[0, a, b] = turned[:64]
            ogt[1, a, b] = turned[64:]

    for j in (1, 2):

        @pl.when(have[j])
        def _(j=j):
            handed(j)

    second_axis(0)
    second_axis(2)

    @pl.when(have[0])
    def _():
        sib.wait_recv()

    for j in range(1, 5):

        @pl.when(have[j])
        def _(j=j):
            for m in (1, 3, 5, 7) if j < 3 else ORDER:
                spread(j, m, s4buf).wait_recv()

    for h in range(4):
        cross = jnp.zeros((256, 128), F32)
        for j in range(5):
            image = dot(q[:, lanes(h)], states[j, lanes(h)], NN)
            mapped[h, j] = image
            cross = cross + lam(3 + j, h, pl.ds(0, 256)) * image
        att[:, lanes(h)] = (att32[:, lanes(h)] + SCALE * cross).astype(BF)

    gs = []

    def exchange(*firsts):
        for a in firsts:
            gbf[a] = dot(ogt[1 - c, a].reshape(256, 256), att[...], NN).astype(BF).reshape(4, 64, 512)
        for a in firsts:
            for b in range(4):
                slot = 4 * b + a
                cp = send(gbf.at[a, b], gsib.at[slot], gs_s.at[slot], gs_r.at[slot], sibling)
                cp.start()
                gs.append(cp)

    exchange(2)
    exchange(1, 3, 0)
    for a in (2, 1, 3, 0):
        g32[a] = dot(ogt[c, a].reshape(256, 256), att[...], NN).reshape(4, 64, 512)

    far_chip(0)
    far_chip(2)

    def h_make(a, b):
        slot = 4 * a + b
        send(gbf.at[0, 0], gsib.at[slot], gs_s.at[slot], gs_r.at[slot], sibling).wait_recv()
        hbuf[a, b] = (g32[a, b] + gsib[slot].astype(F32)).astype(BF)

    dev_a = {1: {"seq": off(1, 0)}, 3: {"seq": off(3, 0)}}
    for b in range(4):
        h_make(2, b)
    rl = {
        1: send(hbuf.at[2, pl.ds(0, 2)], rel.at[0], rl_s.at[0], rl_r.at[0], dev_a[1]),
        3: send(hbuf.at[2, pl.ds(2, 2)], rel.at[1], rl_s.at[1], rl_r.at[1], dev_a[3]),
    }
    rl[1].start()
    rl[3].start()

    def final(m, part):
        n = 2 * (m // 2) + part
        return send(
            hbuf.at[m, pl.ds(2 * part, 2)], fin.at[m // 2, pl.ds(2 * part, 2)], fn_s.at[n], fn_r.at[n], dev_a[m]
        )

    h_make(1, 0)
    h_make(1, 1)
    f10 = final(1, 0)
    f10.start()
    h_make(3, 2)
    h_make(3, 3)
    f31 = final(3, 1)
    f31.start()

    for b in (1, 3, 2):
        other_plane(0, b)
        other_plane(2, b)

    for b in range(2):
        h_make(3, b)
    rl[1].wait_recv()
    for b in range(2):
        hbuf[3, b] = (hbuf[3, b].astype(F32) + rel[0, b].astype(F32)).astype(BF)
    f30 = final(3, 0)
    f30.start()
    for b in range(2):
        h_make(1, 2 + b)
    rl[3].wait_recv()
    for b in range(2):
        hbuf[1, 2 + b] = (hbuf[1, 2 + b].astype(F32) + rel[1, b].astype(F32)).astype(BF)
    f11 = final(1, 1)
    f11.start()

    for a in range(4):
        for b in range(4):
            ag_arrived(20 + 4 * a + b)
    ga[...] = dot(og[...], full[...], NN).astype(BF)
    for h in range(4):
        g = ga[:, lanes(h)].astype(F32)
        for j in range(5):
            wt[h, j] = (SCALE * lam(3 + j, h, pl.ds(0, 256)) * g).astype(BF)
            ubuf[j, lanes(h)] = dot(q[:, lanes(h)], wt[h, j], TN).astype(BF)

    usend = send(ubuf.at[0], usib, us_s, us_r, sibling)

    @pl.when(have[0])
    def _():
        usend.start()

    y = y0 + 2 * y1
    kept = rows(c, 256)
    shared = [
        send(ubuf.at[j, rows(1 - c, 256)], upre.at[j - 1], uh_s.at[j - 1], uh_r.at[j - 1], sibling)
        for j in range(1, 5)
    ]
    for j in (4, 3, 2, 1):

        @pl.when(have[j])
        def _(j=j):
            shared[j - 1].start()

    def slice_to(j, i):
        peer = flipped(s, bits, 2 * i)
        at = rows(lax.div(lax.rem(peer, COL), 2), 64)
        return send(
            upsum.at[j - 1, at], ucol.at[j - 1, i], u_s.at[j - 1, i], u_r.at[j - 1, i], {"seq": peer}
        )

    def spread_updates():
        for j in (4, 3, 2, 1):

            @pl.when(have[j])
            def _(j=j):
                shared[j - 1].wait_recv()
                upsum[j - 1] = (ubuf[j, kept].astype(F32) + upre[j - 1].astype(F32)).astype(BF)
                for i in (2, 1, 3):
                    slice_to(j, i).start()

    place_of = lax.broadcasted_iota(jnp.int32, (128, 128), 1)

    def sums(value):
        return jnp.sum(value, axis=1, keepdims=True)

    def backward(h):
        ds = []
        got = {}
        for n, (i, j) in enumerate(TILES):
            dp = dot(ga[half(i), lanes(h)], v[half(j), lanes(h)], NT)
            ds.append((weight(h, i, j) * dp).astype(BF))
            product = SCALE * score[h, n] * dp
            if i != j:
                got[2, i] = sums(product)
            else:
                got[0, i] = sums(jnp.where(near, product, 0.0))
                got[1, i] = sums(jnp.where(far, product, 0.0))
        for i in range(2):
            g = ga[half(i), lanes(h)].astype(F32)
            acc = glt[half(i)]
            for level in range(8):
                if level > 2:
                    value = SCALE * sums(g * mapped[h, level - 3, half(i)])
                elif (level, i) in got:
                    value = got[level, i]
                else:
                    continue
                acc = jnp.where(place_of == 4 * level + h, value, acc)
            glt[half(i)] = acc
        gq = [dot(ds[0], k[half(0), lanes(h)], NN), dot(ds[1], k[half(1), lanes(h)], NN)]
        gq[1] = gq[1] + dot(ds[2], k[half(0), lanes(h)], NN)
        for i in range(2):
            for j in range(5):
                gq[i] = gq[i] + dot(wt[h, j, half(i)], states[j, lanes(h)], NT)
            gq_ref[half(i), lanes(h)] = gq[i].astype(BF)
        q0, q1 = q[half(0), lanes(h)], q[half(1), lanes(h)]
        g0, g1 = ga[half(0), lanes(h)], ga[half(1), lanes(h)]
        gk32[half(0), lanes(h)] = dot(ds[0], q0, TN) + dot(ds[2], q1, TN)
        gk32[half(1), lanes(h)] = dot(ds[1], q1, TN)
        gv32[half(0), lanes(h)] = dot(prob[h, 0], g0, TN) + dot(prob[h, 2], g1, TN)
        gv32[half(1), lanes(h)] = dot(prob[h, 1], g1, TN)

    glt[...] = jnp.zeros_like(glt)
    backward(0)

    spread_updates()

    backward(1)

    for b in range(4):
        h_make(0, b)
    for cp in (f10, f31, f30, f11):
        cp.wait_recv()
    for b in range(4):
        gbuf[b] = (hbuf[0, b].astype(F32) + fin[0, b].astype(F32) + fin[1, b].astype(F32)).astype(BF)
    gx = []
    for b in (2, 1, 3):
        cp = send(gbuf.at[b], xg.at[b], gx_s.at[b], gx_r.at[b], {"seq": off(0, b)})
        cp.start()
        gx.append(cp)

    for j in range(1, 5):
        for i in range(4):
            cond = bit_of(bits, j, 2 * i) == 1 if j < 3 else have[j]

            @pl.when(cond)
            def _(j=j, i=i):
                if i:
                    slice_to(j, i).wait_recv()
                else:
                    ucol[j - 1, 0] = upsum[j - 1, rows(y, 64)]

            @pl.when(jnp.logical_not(cond))
            def _(j=j, i=i):
                ucol[j - 1, i] = jnp.zeros((64, 128), BF)

    def total(j, chips):
        value = ucol[j - 1, chips[0]].astype(F32)
        for i in chips[1:]:
            value = value + ucol[j - 1, i].astype(F32)
        return value

    asend[0] = total(3, [0, 1, 2, 3])
    asend[1] = total(4, [0, 1, 2, 3])
    ux = [
        send(asend.at[0 if m == 1 else 1], uxin.at[m], ux_s.at[m], ux_r.at[m], {"seq": flipped(s, bits, m << 3)})
        for m in range(1, 4)
    ]
    ux_out = [x0 == 1, x1 == 1, x1 == 1]
    for cp, cond in zip(ux, ux_out):

        @pl.when(cond)
        def _(cp=cp):
            cp.start()

    backward(2)

    for cp in gx:
        cp.wait_recv()
    mean = gbuf[0].astype(F32) + xg[1].astype(F32) + xg[2].astype(F32) + xg[3].astype(F32)
    for i in range(8):
        part = mean[16 * (i // 2) : 16 * (i // 2) + 16, 256 * (i % 2) : 256 * (i % 2) + 256]
        zf[i] = part
        zsend[i] = part.astype(BF)
    z1 = []
    for m in ORDER:
        peer = flipped(z, zbits, m)
        cp = send(zsend.at[peer], zin.at[m], z1_s.at[m], z1_r.at[m], {"dp": peer})
        cp.start()
        z1.append(cp)

    for cp, cond, m in zip(ux, ux_out, range(1, 4)):

        @pl.when(jnp.logical_not(cond))
        def _(cp=cp):
            cp.wait_recv()

        @pl.when(cond)
        def _(m=m):
            uxin[m] = jnp.zeros((64, 128), F32)

    beyond = uxin[1] + uxin[2] + uxin[3]
    for i in range(4):
        n = 2 * ((i >> 1) ^ 1)
        rsend[i] = (beyond + total(1, [i ^ 1]) + total(2, [n, n + 1])).astype(BF)
    owned = rows(4 * c + y, 64)
    rc = []
    for i in (2, 1, 3):
        cp = send(rsend.at[i], rcol.at[owned], ur_s.at[i], ur_r.at[i], {"seq": flipped(s, bits, 2 * i)})
        cp.start()
        rc.append(cp)
    rcol[owned] = rsend[0]

    backward(3)

    def output(n):
        at = pl.ds(512 * n, 512)
        out_ref[:, at] = dot(att[...], full[at], NT).astype(BF)

    output(0)
    output(1)

    for cp in z1:
        cp.wait_recv()
    value = zf[z]
    for m in range(1, 8):
        value = value + zin[m].astype(F32)
    zall[z] = value.astype(BF)
    z2 = []
    for m in ORDER:
        cp = send(zall.at[z], zall.at[z], z2_s.at[m], z2_r.at[m], {"dp": flipped(z, zbits, m)})
        cp.start()
        z2.append(cp)

    output(2)

    for cp in rc:
        cp.wait_recv()
    join = send(rcol.at[kept], rcol.at[kept], rj_s, rj_r, sibling)
    join.start()

    output(3)

    join.wait_recv()

    @pl.when(c == 0)
    def _():
        usend.wait_recv()

    @pl.when(have[0])
    def _():
        usib[...] = jnp.zeros((512, 128), BF)

    for h in range(4):
        back = (rcol[lanes(h)].astype(F32) + usib[lanes(h)].astype(F32)).astype(BF)
        gk_ref[:, lanes(h)] = (gk32[:, lanes(h)] + dot(v[:, lanes(h)], back, NT)).astype(BF)
        gv_ref[:, lanes(h)] = (gv32[:, lanes(h)] + dot(k[:, lanes(h)], back, NN)).astype(BF)
    glrow[...] = glt[...].T[:32]
    for level in range(8):
        gl_ref[level] = glrow[pl.ds(4 * level, 4)]

    for cp in z2:
        cp.wait_recv()
    for i in range(8):
        gp_ref[pl.ds(16 * (i // 2), 16), pl.ds(256 * (i % 2), 256)] = zall[i].astype(F32)

    for cp in first + open_sends + gs + [rl[1], rl[3], f10, f11, f30, f31, join] + rc + gx + z1 + z2:
        cp.wait_send()
    for cp, cond in early + list(zip(xsend, x_out)) + list(zip(ux, ux_out)):

        @pl.when(cond)
        def _(cp=cp):
            cp.wait_send()

    @pl.when(c == 0)
    def _():
        sib.wait_send()

    @pl.when(have[0])
    def _():
        usend.wait_send()

    for j in range(1, 5):

        @pl.when(have[j])
        def _(j=j):
            shared[j - 1].wait_send()
            for i in (2, 1, 3):
                slice_to(j, i).wait_send()
            for cp in {3: late3, 4: late4}.get(j) or [hand_over(j, i) for i in (2, 1, 3)]:
                cp.wait_send()


def step(query, key, value, lam, proj, grad_out):
    dma = pltpu.SemaphoreType.DMA
    outer = pl.BlockSpec(memory_space=pltpu.HBM)
    inner = pl.BlockSpec(memory_space=pltpu.VMEM)
    wide = (256, 512)
    return pl.pallas_call(
        step_kernel,
        out_shape=(
            jax.ShapeDtypeStruct((256, 2048), BF),
            jax.ShapeDtypeStruct(wide, BF),
            jax.ShapeDtypeStruct(wide, BF),
            jax.ShapeDtypeStruct(wide, BF),
            jax.ShapeDtypeStruct((8, 4, 256), F32),
            jax.ShapeDtypeStruct((64, 512), F32),
        ),
        in_specs=[outer] * 6,
        out_specs=(inner,) * 6,
        scratch_shapes=[
            pltpu.VMEM(wide, BF), pltpu.VMEM(wide, BF), pltpu.VMEM(wide, BF),
            pltpu.VMEM((256, 2048), BF),
            pltpu.VMEM((2, 4, 4, 64, 256), BF),
            pltpu.VMEM((256, 32), F32),
            pltpu.VMEM((256, 128), F32),
            pltpu.VMEM((32, 256), F32),
            pltpu.VMEM((8, 4, 256), F32),
            pltpu.VMEM((64, 512), BF),
            pltpu.VMEM((2048, 512), BF),
            pltpu.VMEM((5, 512, 128), BF),
            pltpu.VMEM((4, 3, 128, 128), F32),
            pltpu.VMEM((4, 3, 128, 128), BF),
            pltpu.VMEM(wide, F32),
            pltpu.VMEM(wide, BF),
            pltpu.VMEM((4, 5, 256, 128), F32),
            pltpu.VMEM(wide, BF),
            pltpu.VMEM((4, 5, 256, 128), BF),
            pltpu.VMEM(wide, F32),
            pltpu.VMEM(wide, F32),
            pltpu.VMEM((512, 128), BF),
            pltpu.VMEM((COL, 64, 128), BF),
            pltpu.VMEM((4, 64, 128), BF),
            pltpu.VMEM((2, 64, 128), BF),
            pltpu.VMEM((64, 128), F32),
            pltpu.VMEM((4, 64, 128), F32),
            pltpu.VMEM((64, 128), BF),
            pltpu.VMEM((64, 128), BF),
            pltpu.VMEM((5, 512, 128), BF),
            pltpu.VMEM((4, 256, 128), BF),
            pltpu.VMEM((4, 256, 128), BF),
            pltpu.VMEM((4, 4, 64, 128), BF),
            pltpu.VMEM((2, 64, 128), F32),
            pltpu.VMEM((4, 64, 128), F32),
            pltpu.VMEM((4, 64, 128), BF),
            pltpu.VMEM((512, 128), BF),
            pltpu.VMEM((512, 128), BF),
            pltpu.VMEM((4, 4, 64, 512), F32),
            pltpu.VMEM((4, 4, 64, 512), BF),
            pltpu.VMEM((PIECES, 64, 512), BF),
            pltpu.VMEM((4, 4, 64, 512), BF),
            pltpu.VMEM((2, 2, 64, 512), BF),
            pltpu.VMEM((2, 4, 64, 512), BF),
            pltpu.VMEM((4, 64, 512), BF),
            pltpu.VMEM((4, 64, 512), BF),
            pltpu.VMEM((8, 16, 256), F32),
            pltpu.VMEM((8, 16, 256), BF),
            pltpu.VMEM((8, 16, 256), BF),
            pltpu.VMEM((8, 16, 256), BF),
            dma((6,)),
            dma((44,)), dma((44,)), dma((COL,)), dma((COL,)),
            dma((5, COL)), dma((5, COL)), dma((4,)), dma((4,)), dma, dma,
            dma((4,)), dma((4,)), dma((4, 4)), dma((4, 4)), dma((4,)), dma((4,)), dma((4,)), dma((4,)), dma, dma, dma, dma,
            dma((PIECES,)), dma((PIECES,)), dma((2,)), dma((2,)), dma((4,)), dma((4,)),
            dma((4,)), dma((4,)), dma((8,)), dma((8,)), dma((8,)), dma((8,)),
        ],
        compiler_params=pltpu.CompilerParams(collective_id=0, has_side_effects=True, vmem_limit_bytes=36 * 2**20),
        name="span_step",
    )(query, key, value, lam, proj, grad_out)


def deliver_kernel(*refs):
    count = len(refs) // 2
    sems = refs[-1]
    copies = [pltpu.make_async_copy(refs[i], refs[count + i], sems.at[i]) for i in range(count)]
    for cp in copies:
        cp.start()
    for cp in copies:
        cp.wait()


def deliver(arrays):
    return pl.pallas_call(
        deliver_kernel,
        out_shape=[jax.ShapeDtypeStruct(x.shape, x.dtype) for x in arrays],
        in_specs=[pl.BlockSpec(memory_space=pltpu.VMEM)] * len(arrays),
        out_specs=[pl.BlockSpec(memory_space=pltpu.HBM)] * len(arrays),
        scratch_shapes=[pltpu.SemaphoreType.DMA((len(arrays),))],
        compiler_params=pltpu.CompilerParams(vmem_limit_bytes=2**20),
        name="deliver",
    )(*arrays)


def shards(queries, keys, values, level_weights, proj, out_grad):
    out, gq, gk, gv, gl, gp = deliver(
        step(
            *[
                pltpu.with_memory_space_constraint(x, pltpu.HBM)
                for x in (queries[0], keys[0], values[0], level_weights[0], proj.T, out_grad[0])
            ]
        )
    )
    return out[None], gq[None], gk[None], gv[None], gl[None], gp.T


def solution(mesh):
    return jax.shard_map(
        shards,
        mesh=mesh,
        in_specs=(
            P("dp", "seq", None),
            P("dp", "seq", None),
            P("dp", "seq", None),
            P("dp", None, None, "seq"),
            P(None, "seq"),
            P("dp", "seq", None),
        ),
        out_specs=(
            P("dp", "seq", None),
            P("dp", "seq", None),
            P("dp", "seq", None),
            P("dp", "seq", None),
            P("dp", None, None, "seq"),
            P(None, "seq"),
        ),
        check_vma=False,
    )
```

```python
import jax
import jax.numpy as jnp
from jax import lax
from jax.experimental import pallas as pl
from jax.experimental.pallas import tpu as pltpu
from jax.sharding import PartitionSpec as P

BF = jnp.bfloat16
F32 = jnp.float32
MESH = pl.DeviceIdType.MESH
COL = 8
PIECES = 16


def place():
    s = lax.axis_index("seq")
    bits = [lax.rem(lax.div(s, 2**b), 2) for b in range(5)]
    return s, bits


def flipped(s, bits, mask):
    peer = s
    for b in range(5):
        if mask >> b & 1:
            peer = peer + 2**b * (1 - 2 * bits[b])
    return peer


def chip_offsets(s, bits):
    c, y0, y1, x0, x1 = bits
    dy0, dy1 = 2 * (1 - 2 * y0), 4 * (1 - 2 * y1)
    dx0, dx1 = 8 * (1 - 2 * x0), 16 * (1 - 2 * x1)
    da0, da1 = dy0 * (1 - c) + dx0 * c, dy1 * (1 - c) + dx1 * c
    db0, db1 = dx0 * (1 - c) + dy0 * c, dx1 * (1 - c) + dy1 * c

    def off(a, b):
        return s + (a & 1) * da0 + (a >> 1) * da1 + (b & 1) * db0 + (b >> 1) * db1

    return off


def rows(index, count):
    return pl.ds(pl.multiple_of(index * count, count), count)


def send(src, dst, ssem, rsem, device):
    return pltpu.make_async_remote_copy(
        src_ref=src, dst_ref=dst, send_sem=ssem, recv_sem=rsem, device_id=device, device_id_type=MESH
    )


def bit_of(bits, b, mask):
    return 1 - bits[b] if mask >> b & 1 else bits[b]


def dot(x, y, dims):
    return lax.dot_general(x, y, (dims, ((), ())), preferred_element_type=F32)


NN, NT, TN = ((1,), (0,)), ((1,), (1,)), ((0,), (0,))
SCALE = 128**-0.5
ORDER = (4, 5, 2, 3, 6, 7, 1)
TILES = ((0, 0), (1, 1), (1, 0))


def step_kernel(
    q_hbm, k_hbm, v_hbm, lam_hbm, proj_hbm, og_hbm,
    out_ref, gq_ref, gk_ref, gv_ref, gl_ref, gp_ref,
    q, k, v, og, ogt, lamt, glt, glrow, lam_in, shard_buf, full, states, score, prob, att32, att, mapped, ga, wt, gk32, gv32,
    tot, col, pair, quad, csum, xin, s3buf, s4buf,
    ubuf, upre, upsum, ucol, asend, uxin, rsend, rcol, usib,
    g32, gbf, gsib, hbuf, rel, fin, gbuf, xg, zf, zsend, zin, zall,
    ld, ag_s, ag_r, c1_s, c1_r, st_s, st_r, x_s, x_r, sib_s, sib_r,
    uh_s, uh_r, u_s, u_r, ux_s, ux_r, ur_s, ur_r, us_s, us_r,
    gs_s, gs_r, rl_s, rl_r, fn_s, fn_r, gx_s, gx_r, z1_s, z1_r, z2_s, z2_r,
):
    s, bits = place()
    c, y0, y1, x0, x1 = bits
    z = lax.axis_index("dp")
    zbits = [lax.rem(lax.div(z, 2**b), 2) for b in range(3)] + [0, 0]
    r = lax.rem(s, COL)
    mine = rows(r, 64)
    off = chip_offsets(s, bits)
    have = [c == 1, y0 == 1, y1 == 1, x0 == 1, x1 == 1]
    sib_index = flipped(s, bits, 1)
    sibling = {"seq": sib_index}

    loads = [
        pltpu.make_async_copy(src, dst, ld.at[i])
        for i, (src, dst) in enumerate(
            ((k_hbm, k), (v_hbm, v), (q_hbm, q), (og_hbm, og), (proj_hbm, shard_buf), (lam_hbm, lam_in))
        )
    ]
    for cp in loads:
        cp.start()

    greeted = (
        [{"seq": flipped(s, bits, m)} for m in range(1, 8)]
        + [{"seq": flipped(s, bits, m << 3)} for m in range(1, 4)]
        + [{"dp": flipped(z, zbits, m)} for m in range(1, 8)]
    )
    barrier = pltpu.get_barrier_semaphore()
    for device in greeted:
        pl.semaphore_signal(barrier, inc=1, device_id=device, device_id_type=MESH)

    def lanes(h):
        return pl.ds(128 * h, 128)

    loads[0].wait()
    loads[1].wait()
    for h in range(4):
        tot[lanes(h)] = dot(k[:, lanes(h)], v[:, lanes(h)], TN).astype(BF)
    pl.semaphore_wait(barrier, len(greeted))

    first = []
    for m in ORDER:
        peer = flipped(s, bits, m)
        cp = send(tot.at[rows(lax.rem(peer, COL), 64)], col.at[m], c1_s.at[m], c1_r.at[m], {"seq": peer})
        cp.start()
        first.append(cp)
    sib = send(tot, states.at[0], sib_s, sib_r, sibling)

    @pl.when(c == 0)
    def _():
        sib.start()

    open_sends = []

    def block(index):
        return full.at[rows(index, 64)]

    def ag(slot, src, index, device):
        cp = send(src, block(index), ag_s.at[slot], ag_r.at[slot], device)
        cp.start()
        open_sends.append(cp)

    def ag_arrived(slot):
        send(shard_buf, block(s), ag_s.at[slot], ag_r.at[slot], sibling).wait_recv()

    def chip(a, b):
        return flipped(s, bits, a << 1 | b << 3)

    loads[4].wait()
    full[rows(s, 64)] = shard_buf[...]
    starts = {a: send(shard_buf, block(s), ag_s.at[a], ag_r.at[a], {"seq": chip(a, 0)}) for a in (1, 3, 2)}
    open_sends.extend(starts.values())

    odd = zbits[0]
    dz = ({"dp": lax.rem(z + 1, 8)}, {"dp": lax.rem(z + 7, 8)})

    def piece(a, b):
        turn = 1 - odd if a & 1 else odd
        return chip(a & 2, b) + 2 * (1 - 2 * y0) * turn

    along = {}
    for a in (0, 2):
        for b in (1, 3):
            slot = 4 + 4 * a + b
            at = block(piece(a, 0))
            along[a, b] = send(at, at, ag_s.at[slot], ag_r.at[slot], {"seq": chip(0, b)})
            open_sends.append(along[a, b])

    def set_out(*labels):
        for a in labels:
            along[a, 1].start()
            along[a, 3].start()

    @pl.when(odd == 0)
    def _():
        for a in (2, 1, 3):
            starts[a].start()
        set_out(0)

    @pl.when(odd == 1)
    def _():
        for a in (1, 3, 2):
            starts[a].start()

    ag(20, shard_buf, s, sibling)


    row = lax.broadcasted_iota(jnp.int32, (128, 128), 0)
    column = lax.broadcasted_iota(jnp.int32, (128, 128), 1)
    causal = column <= row
    near = causal & ((row < 64) | (column >= 64))
    far = causal & (row >= 64) & (column < 64)

    def half(i):
        return pl.ds(128 * i, 128)

    def lam(level, h, where):
        return lamt[where, pl.ds(4 * level + h, 1)]

    def weight(h, i, j):
        if i != j:
            return SCALE * lam(2, h, half(i))
        return SCALE * jnp.where(near, lam(0, h, half(i)), jnp.where(far, lam(1, h, half(i)), 0.0))

    def inside(h):
        for n, (i, j) in enumerate(TILES):
            value = dot(q[half(i), lanes(h)], k[half(j), lanes(h)], NT)
            score[h, n] = value
            prob[h, n] = (weight(h, i, j) * value).astype(BF)
        att32[half(0), lanes(h)] = dot(prob[h, 0], v[half(0), lanes(h)], NN)
        att32[half(1), lanes(h)] = dot(prob[h, 1], v[half(1), lanes(h)], NN) + dot(
            prob[h, 2], v[half(0), lanes(h)], NN
        )

    loads[5].wait()
    for level in range(8):
        glrow[pl.ds(4 * level, 4)] = lam_in[level]
    lamt[...] = glrow[...].T
    loads[2].wait()
    inside(0)
    inside(1)

    for cp in first:
        cp.wait_recv()
    col[0] = tot[mine]
    t = [col[m].astype(F32) for m in range(COL)]
    p = [t[2 * i] + t[2 * i + 1] for i in range(4)]
    qd = [p[0] + p[1], p[2] + p[3]]
    csum[...] = qd[0] + qd[1]
    xsend = [
        send(csum, xin.at[m], x_s.at[m], x_r.at[m], {"seq": flipped(s, bits, m << 3)}) for m in range(1, 4)
    ]
    x_out = [x0 == 0, x1 == 0, x1 == 0]
    for cp, cond in zip(xsend, x_out):

        @pl.when(cond)
        def _(cp=cp):
            cp.start()

    for i in range(4):
        pair[i] = p[i].astype(BF)
    for i in range(2):
        quad[i] = qd[i].astype(BF)

    def spread(j, m, src):
        return send(src, states.at[j, mine], st_s.at[j, m], st_r.at[j, m], {"seq": flipped(s, bits, m)})

    early = []
    for m in (4, 2, 6, 1):
        early.append((spread(1, m, pair.at[(m >> 1) ^ 1]), bit_of(bits, 1, m) == 1))
        early.append((spread(2, m, quad.at[(m >> 2) ^ 1]), bit_of(bits, 2, m) == 1))
    for cp, cond in early:

        @pl.when(cond)
        def _(cp=cp):
            cp.start()

    def hand_over(j, i):
        at = states.at[j, rows(lax.rem(flipped(s, bits, 2 * i), COL), 64)]
        return send(at, at, st_s.at[j, 2 * i + 1], st_r.at[j, 2 * i + 1], sibling)

    def handed(j):
        for i in (2, 1, 3):
            spread(j, 2 * i, s4buf).wait_recv()
            hand_over(j, i).start()

    for j in range(5):

        @pl.when(jnp.logical_not(have[j]))
        def _(j=j):
            states[j] = jnp.zeros((512, 128), BF)

    @pl.when(have[1])
    def _():
        states[1, mine] = pair[1]

    @pl.when(have[2])
    def _():
        states[2, mine] = quad[1]

    def pass_on(a, b):
        ag(36 + 2 * a + b, block(piece(a, b)), piece(a, b), dz[a >> 1])
        ag(20 + 4 * a + b, block(piece(a, b)), piece(a, b), sibling)

    def second_axis(a):
        for b in (1, 3):
            ag_arrived(4 + 4 * a + b)
            if (b == 1) == (a == 0):
                ag(4 + 4 * a + 2, block(piece(a, b)), piece(a, b), {"seq": chip(0, 4 - b)})
            pass_on(a, b)

    def far_chip(a):
        ag_arrived(4 + 4 * a + 2)
        pass_on(a, 2)

    def other_plane(a, b):
        ag_arrived(36 + 2 * a + b)
        ag(24 + 4 * a + b, block(piece(a + 1, b)), piece(a + 1, b), sibling)

    @pl.when(odd == 1)
    def _():
        ag_arrived(1)
        ag_arrived(3)
        set_out(0, 2)

    @pl.when(odd == 0)
    def _():
        ag_arrived(2)
        set_out(2)

    inside(2)

    late3 = [spread(3, m, s3buf) for m in ORDER]
    late4 = [spread(4, m, s4buf) for m in ORDER]

    @pl.when(have[3])
    def _():
        xsend[0].wait_recv()
        s3buf[...] = xin[1].astype(BF)
        for cp in late3:
            cp.start()
        states[3, mine] = s3buf[...]

    @pl.when(have[4])
    def _():
        xsend[1].wait_recv()
        xsend[2].wait_recv()
        s4buf[...] = (xin[2] + xin[3]).astype(BF)
        for cp in late4:
            cp.start()
        states[4, mine] = s4buf[...]

    @pl.when(odd == 1)
    def _():
        ag_arrived(2)

    @pl.when(odd == 0)
    def _():
        ag_arrived(1)
        ag_arrived(3)

    for a in (1, 3, 2):
        ag(20 + 4 * a, block(chip(a, 0)), chip(a, 0), sibling)

    inside(3)
    loads[3].wait()
    for a in range(4):
        for b in range(4):
            turned = og[:, rows(lax.div(off(a, b), 2), 128)].T
            ogt[0, a, b] = turned[:64]
            ogt[1, a, b] = turned[64:]

    for j in (1, 2):

        @pl.when(have[j])
        def _(j=j):
            handed(j)

    second_axis(0)
    second_axis(2)

    @pl.when(have[0])
    def _():
        sib.wait_recv()

    for j in range(1, 5):

        @pl.when(have[j])
        def _(j=j):
            for m in (1, 3, 5, 7) if j < 3 else ORDER:
                spread(j, m, s4buf).wait_recv()

    for h in range(4):
        cross = jnp.zeros((256, 128), F32)
        for j in range(5):
            image = dot(q[:, lanes(h)], states[j, lanes(h)], NN)
            mapped[h, j] = image
            cross = cross + lam(3 + j, h, pl.ds(0, 256)) * image
        att[:, lanes(h)] = (att32[:, lanes(h)] + SCALE * cross).astype(BF)

    gs = []

    def exchange(*firsts):
        for a in firsts:
            gbf[a] = dot(ogt[1 - c, a].reshape(256, 256), att[...], NN).astype(BF).reshape(4, 64, 512)
        for a in firsts:
            for b in range(4):
                slot = 4 * b + a
                cp = send(gbf.at[a, b], gsib.at[slot], gs_s.at[slot], gs_r.at[slot], sibling)
                cp.start()
                gs.append(cp)

    exchange(2)
    exchange(1, 3, 0)
    for a in (2, 1, 3, 0):
        g32[a] = dot(ogt[c, a].reshape(256, 256), att[...], NN).reshape(4, 64, 512)

    far_chip(0)
    far_chip(2)

    def h_make(a, b):
        slot = 4 * a + b
        send(gbf.at[0, 0], gsib.at[slot], gs_s.at[slot], gs_r.at[slot], sibling).wait_recv()
        hbuf[a, b] = (g32[a, b] + gsib[slot].astype(F32)).astype(BF)

    dev_a = {1: {"seq": off(1, 0)}, 3: {"seq": off(3, 0)}}
    relayed = []
    for b in (0, 2, 1, 3):
        h_make(2, b)
        cp = send(hbuf.at[2, b], rel.at[b], rl_s.at[b], rl_r.at[b], dev_a[1 if b < 2 else 3])
        cp.start()
        relayed.append(cp)

    finals = []

    def final(m, b):
        n = 4 * (m // 2) + b
        cp = send(hbuf.at[m, b], fin.at[m // 2, b], fn_s.at[n], fn_r.at[n], dev_a[m])
        cp.start()
        finals.append(cp)

    for m, b in ((1, 0), (3, 2), (1, 1), (3, 3)):
        h_make(m, b)
        final(m, b)
    for m, b in ((3, 0), (1, 2), (3, 1), (1, 3)):
        h_make(m, b)

    for b in (1, 3, 2):
        other_plane(0, b)
        other_plane(2, b)

    for m, b, cp in zip((3, 1, 3, 1), (0, 2, 1, 3), relayed):
        cp.wait_recv()
        hbuf[m, b] = (hbuf[m, b].astype(F32) + rel[b].astype(F32)).astype(BF)
        final(m, b)

    for a in range(4):
        for b in range(4):
            ag_arrived(20 + 4 * a + b)
    ga[...] = dot(og[...], full[...], NN).astype(BF)
    for h in range(4):
        g = ga[:, lanes(h)].astype(F32)
        for j in range(5):
            wt[h, j] = (SCALE * lam(3 + j, h, pl.ds(0, 256)) * g).astype(BF)
            ubuf[j, lanes(h)] = dot(q[:, lanes(h)], wt[h, j], TN).astype(BF)

    usend = send(ubuf.at[0], usib, us_s, us_r, sibling)

    @pl.when(have[0])
    def _():
        usend.start()

    y = y0 + 2 * y1
    kept = rows(c, 256)
    shared = [
        send(ubuf.at[j, rows(1 - c, 256)], upre.at[j - 1], uh_s.at[j - 1], uh_r.at[j - 1], sibling)
        for j in range(1, 5)
    ]
    for j in (4, 3, 2, 1):

        @pl.when(have[j])
        def _(j=j):
            shared[j - 1].start()

    def slice_to(j, i):
        peer = flipped(s, bits, 2 * i)
        at = rows(lax.div(lax.rem(peer, COL), 2), 64)
        return send(
            upsum.at[j - 1, at], ucol.at[j - 1, i], u_s.at[j - 1, i], u_r.at[j - 1, i], {"seq": peer}
        )

    def spread_updates():
        for j in (4, 3, 2, 1):

            @pl.when(have[j])
            def _(j=j):
                shared[j - 1].wait_recv()
                upsum[j - 1] = (ubuf[j, kept].astype(F32) + upre[j - 1].astype(F32)).astype(BF)
                for i in (2, 1, 3):
                    slice_to(j, i).start()

    place_of = lax.broadcasted_iota(jnp.int32, (128, 128), 1)

    def sums(value):
        return jnp.sum(value, axis=1, keepdims=True)

    def backward(h):
        ds = []
        got = {}
        for n, (i, j) in enumerate(TILES):
            dp = dot(ga[half(i), lanes(h)], v[half(j), lanes(h)], NT)
            ds.append((weight(h, i, j) * dp).astype(BF))
            product = SCALE * score[h, n] * dp
            if i != j:
                got[2, i] = sums(product)
            else:
                got[0, i] = sums(jnp.where(near, product, 0.0))
                got[1, i] = sums(jnp.where(far, product, 0.0))
        for i in range(2):
            g = ga[half(i), lanes(h)].astype(F32)
            acc = glt[half(i)]
            for level in range(8):
                if level > 2:
                    value = SCALE * sums(g * mapped[h, level - 3, half(i)])
                elif (level, i) in got:
                    value = got[level, i]
                else:
                    continue
                acc = jnp.where(place_of == 4 * level + h, value, acc)
            glt[half(i)] = acc
        gq = [dot(ds[0], k[half(0), lanes(h)], NN), dot(ds[1], k[half(1), lanes(h)], NN)]
        gq[1] = gq[1] + dot(ds[2], k[half(0), lanes(h)], NN)
        for i in range(2):
            for j in range(5):
                gq[i] = gq[i] + dot(wt[h, j, half(i)], states[j, lanes(h)], NT)
            gq_ref[half(i), lanes(h)] = gq[i].astype(BF)
        q0, q1 = q[half(0), lanes(h)], q[half(1), lanes(h)]
        g0, g1 = ga[half(0), lanes(h)], ga[half(1), lanes(h)]
        gk32[half(0), lanes(h)] = dot(ds[0], q0, TN) + dot(ds[2], q1, TN)
        gk32[half(1), lanes(h)] = dot(ds[1], q1, TN)
        gv32[half(0), lanes(h)] = dot(prob[h, 0], g0, TN) + dot(prob[h, 2], g1, TN)
        gv32[half(1), lanes(h)] = dot(prob[h, 1], g1, TN)

    glt[...] = jnp.zeros_like(glt)
    backward(0)

    spread_updates()

    backward(1)

    for b in range(4):
        h_make(0, b)
    for cp in finals:
        cp.wait_recv()
    for b in range(4):
        gbuf[b] = (hbuf[0, b].astype(F32) + fin[0, b].astype(F32) + fin[1, b].astype(F32)).astype(BF)
    gx = []
    for b in (2, 1, 3):
        cp = send(gbuf.at[b], xg.at[b], gx_s.at[b], gx_r.at[b], {"seq": off(0, b)})
        cp.start()
        gx.append(cp)

    backward(2)

    for j in range(1, 5):
        for i in range(4):
            cond = bit_of(bits, j, 2 * i) == 1 if j < 3 else have[j]

            @pl.when(cond)
            def _(j=j, i=i):
                if i:
                    slice_to(j, i).wait_recv()
                else:
                    ucol[j - 1, 0] = upsum[j - 1, rows(y, 64)]

            @pl.when(jnp.logical_not(cond))
            def _(j=j, i=i):
                ucol[j - 1, i] = jnp.zeros((64, 128), BF)

    def total(j, chips):
        value = ucol[j - 1, chips[0]].astype(F32)
        for i in chips[1:]:
            value = value + ucol[j - 1, i].astype(F32)
        return value

    asend[0] = total(3, [0, 1, 2, 3])
    asend[1] = total(4, [0, 1, 2, 3])
    ux = [
        send(asend.at[0 if m == 1 else 1], uxin.at[m], ux_s.at[m], ux_r.at[m], {"seq": flipped(s, bits, m << 3)})
        for m in range(1, 4)
    ]
    ux_out = [x0 == 1, x1 == 1, x1 == 1]
    for cp, cond in zip(ux, ux_out):

        @pl.when(cond)
        def _(cp=cp):
            cp.start()

    for cp in gx:
        cp.wait_recv()
    mean = gbuf[0].astype(F32) + xg[1].astype(F32) + xg[2].astype(F32) + xg[3].astype(F32)
    for i in range(8):
        part = mean[16 * (i // 2) : 16 * (i // 2) + 16, 256 * (i % 2) : 256 * (i % 2) + 256]
        zf[i] = part
        zsend[i] = part.astype(BF)
    z1 = []
    for m in ORDER:
        peer = flipped(z, zbits, m)
        cp = send(zsend.at[peer], zin.at[m], z1_s.at[m], z1_r.at[m], {"dp": peer})
        cp.start()
        z1.append(cp)

    backward(3)

    def output(n):
        at = pl.ds(512 * n, 512)
        out_ref[:, at] = dot(att[...], full[at], NT).astype(BF)

    output(0)
    output(1)

    for cp, cond, m in zip(ux, ux_out, range(1, 4)):

        @pl.when(jnp.logical_not(cond))
        def _(cp=cp):
            cp.wait_recv()

        @pl.when(cond)
        def _(m=m):
            uxin[m] = jnp.zeros((64, 128), F32)

    beyond = uxin[1] + uxin[2] + uxin[3]
    for i in range(4):
        n = 2 * ((i >> 1) ^ 1)
        rsend[i] = (beyond + total(1, [i ^ 1]) + total(2, [n, n + 1])).astype(BF)
    owned = rows(4 * c + y, 64)
    rc = []
    for m in ORDER:
        cp = send(rsend.at[m >> 1], rcol.at[owned], ur_s.at[m], ur_r.at[m], {"seq": flipped(s, bits, m)})
        cp.start()
        rc.append(cp)
    rcol[owned] = rsend[0]

    for cp in z1:
        cp.wait_recv()
    value = zf[z]
    for m in range(1, 8):
        value = value + zin[m].astype(F32)
    zall[z] = value.astype(BF)
    z2 = []
    for m in ORDER:
        cp = send(zall.at[z], zall.at[z], z2_s.at[m], z2_r.at[m], {"dp": flipped(z, zbits, m)})
        cp.start()
        z2.append(cp)

    output(2)

    output(3)

    for cp in rc:
        cp.wait_recv()

    @pl.when(c == 0)
    def _():
        usend.wait_recv()

    @pl.when(have[0])
    def _():
        usib[...] = jnp.zeros((512, 128), BF)

    for h in range(4):
        back = (rcol[lanes(h)].astype(F32) + usib[lanes(h)].astype(F32)).astype(BF)
        gk_ref[:, lanes(h)] = (gk32[:, lanes(h)] + dot(v[:, lanes(h)], back, NT)).astype(BF)
        gv_ref[:, lanes(h)] = (gv32[:, lanes(h)] + dot(k[:, lanes(h)], back, NN)).astype(BF)
    glrow[...] = glt[...].T[:32]
    for level in range(8):
        gl_ref[level] = glrow[pl.ds(4 * level, 4)]

    for cp in z2:
        cp.wait_recv()
    for i in range(8):
        gp_ref[pl.ds(16 * (i // 2), 16), pl.ds(256 * (i % 2), 256)] = zall[i].astype(F32)

    for cp in first + open_sends + gs + relayed + finals + rc + gx + z1 + z2:
        cp.wait_send()
    for cp, cond in early + list(zip(xsend, x_out)) + list(zip(ux, ux_out)):

        @pl.when(cond)
        def _(cp=cp):
            cp.wait_send()

    @pl.when(c == 0)
    def _():
        sib.wait_send()

    @pl.when(have[0])
    def _():
        usend.wait_send()

    for j in range(1, 5):

        @pl.when(have[j])
        def _(j=j):
            shared[j - 1].wait_send()
            for i in (2, 1, 3):
                slice_to(j, i).wait_send()
            for cp in {3: late3, 4: late4}.get(j) or [hand_over(j, i) for i in (2, 1, 3)]:
                cp.wait_send()


def step(query, key, value, lam, proj, grad_out):
    dma = pltpu.SemaphoreType.DMA
    outer = pl.BlockSpec(memory_space=pltpu.HBM)
    inner = pl.BlockSpec(memory_space=pltpu.VMEM)
    wide = (256, 512)
    return pl.pallas_call(
        step_kernel,
        out_shape=(
            jax.ShapeDtypeStruct((256, 2048), BF),
            jax.ShapeDtypeStruct(wide, BF),
            jax.ShapeDtypeStruct(wide, BF),
            jax.ShapeDtypeStruct(wide, BF),
            jax.ShapeDtypeStruct((8, 4, 256), F32),
            jax.ShapeDtypeStruct((64, 512), F32),
        ),
        in_specs=[outer] * 6,
        out_specs=(inner,) * 6,
        scratch_shapes=[
            pltpu.VMEM(wide, BF), pltpu.VMEM(wide, BF), pltpu.VMEM(wide, BF),
            pltpu.VMEM((256, 2048), BF),
            pltpu.VMEM((2, 4, 4, 64, 256), BF),
            pltpu.VMEM((256, 32), F32),
            pltpu.VMEM((256, 128), F32),
            pltpu.VMEM((32, 256), F32),
            pltpu.VMEM((8, 4, 256), F32),
            pltpu.VMEM((64, 512), BF),
            pltpu.VMEM((2048, 512), BF),
            pltpu.VMEM((5, 512, 128), BF),
            pltpu.VMEM((4, 3, 128, 128), F32),
            pltpu.VMEM((4, 3, 128, 128), BF),
            pltpu.VMEM(wide, F32),
            pltpu.VMEM(wide, BF),
            pltpu.VMEM((4, 5, 256, 128), F32),
            pltpu.VMEM(wide, BF),
            pltpu.VMEM((4, 5, 256, 128), BF),
            pltpu.VMEM(wide, F32),
            pltpu.VMEM(wide, F32),
            pltpu.VMEM((512, 128), BF),
            pltpu.VMEM((COL, 64, 128), BF),
            pltpu.VMEM((4, 64, 128), BF),
            pltpu.VMEM((2, 64, 128), BF),
            pltpu.VMEM((64, 128), F32),
            pltpu.VMEM((4, 64, 128), F32),
            pltpu.VMEM((64, 128), BF),
            pltpu.VMEM((64, 128), BF),
            pltpu.VMEM((5, 512, 128), BF),
            pltpu.VMEM((4, 256, 128), BF),
            pltpu.VMEM((4, 256, 128), BF),
            pltpu.VMEM((4, 4, 64, 128), BF),
            pltpu.VMEM((2, 64, 128), F32),
            pltpu.VMEM((4, 64, 128), F32),
            pltpu.VMEM((4, 64, 128), BF),
            pltpu.VMEM((512, 128), BF),
            pltpu.VMEM((512, 128), BF),
            pltpu.VMEM((4, 4, 64, 512), F32),
            pltpu.VMEM((4, 4, 64, 512), BF),
            pltpu.VMEM((PIECES, 64, 512), BF),
            pltpu.VMEM((4, 4, 64, 512), BF),
            pltpu.VMEM((4, 64, 512), BF),
            pltpu.VMEM((2, 4, 64, 512), BF),
            pltpu.VMEM((4, 64, 512), BF),
            pltpu.VMEM((4, 64, 512), BF),
            pltpu.VMEM((8, 16, 256), F32),
            pltpu.VMEM((8, 16, 256), BF),
            pltpu.VMEM((8, 16, 256), BF),
            pltpu.VMEM((8, 16, 256), BF),
            dma((6,)),
            dma((44,)), dma((44,)), dma((COL,)), dma((COL,)),
            dma((5, COL)), dma((5, COL)), dma((4,)), dma((4,)), dma, dma,
            dma((4,)), dma((4,)), dma((4, 4)), dma((4, 4)), dma((4,)), dma((4,)), dma((COL,)), dma((COL,)), dma, dma,
            dma((PIECES,)), dma((PIECES,)), dma((4,)), dma((4,)), dma((8,)), dma((8,)),
            dma((4,)), dma((4,)), dma((8,)), dma((8,)), dma((8,)), dma((8,)),
        ],
        compiler_params=pltpu.CompilerParams(collective_id=0, has_side_effects=True, vmem_limit_bytes=36 * 2**20),
        name="span_step",
    )(query, key, value, lam, proj, grad_out)


def deliver_kernel(*refs):
    count = len(refs) // 2
    sems = refs[-1]
    copies = [pltpu.make_async_copy(refs[i], refs[count + i], sems.at[i]) for i in range(count)]
    for cp in copies:
        cp.start()
    for cp in copies:
        cp.wait()


def deliver(arrays):
    return pl.pallas_call(
        deliver_kernel,
        out_shape=[jax.ShapeDtypeStruct(x.shape, x.dtype) for x in arrays],
        in_specs=[pl.BlockSpec(memory_space=pltpu.VMEM)] * len(arrays),
        out_specs=[pl.BlockSpec(memory_space=pltpu.HBM)] * len(arrays),
        scratch_shapes=[pltpu.SemaphoreType.DMA((len(arrays),))],
        compiler_params=pltpu.CompilerParams(vmem_limit_bytes=2**20),
        name="deliver",
    )(*arrays)


def shards(queries, keys, values, level_weights, proj, out_grad):
    out, gq, gk, gv, gl, gp = deliver(
        step(
            *[
                pltpu.with_memory_space_constraint(x, pltpu.HBM)
                for x in (queries[0], keys[0], values[0], level_weights[0], proj.T, out_grad[0])
            ]
        )
    )
    return out[None], gq[None], gk[None], gv[None], gl[None], gp.T


def solution(mesh):
    return jax.shard_map(
        shards,
        mesh=mesh,
        in_specs=(
            P("dp", "seq", None),
            P("dp", "seq", None),
            P("dp", "seq", None),
            P("dp", None, None, "seq"),
            P(None, "seq"),
            P("dp", "seq", None),
        ),
        out_specs=(
            P("dp", "seq", None),
            P("dp", "seq", None),
            P("dp", "seq", None),
            P("dp", "seq", None),
            P("dp", None, None, "seq"),
            P(None, "seq"),
        ),
        check_vma=False,
    )
```

```python
import jax
import jax.numpy as jnp
from jax import lax
from jax.experimental import pallas as pl
from jax.experimental.pallas import tpu as pltpu
from jax.sharding import PartitionSpec as P

BF = jnp.bfloat16
F32 = jnp.float32
MESH = pl.DeviceIdType.MESH
COL = 8
PIECES = 16


def place():
    s = lax.axis_index("seq")
    bits = [lax.rem(lax.div(s, 2**b), 2) for b in range(5)]
    return s, bits


def flipped(s, bits, mask):
    peer = s
    for b in range(5):
        if mask >> b & 1:
            peer = peer + 2**b * (1 - 2 * bits[b])
    return peer


def chip_offsets(s, bits):
    c, y0, y1, x0, x1 = bits
    dy0, dy1 = 2 * (1 - 2 * y0), 4 * (1 - 2 * y1)
    dx0, dx1 = 8 * (1 - 2 * x0), 16 * (1 - 2 * x1)
    da0, da1 = dy0 * (1 - c) + dx0 * c, dy1 * (1 - c) + dx1 * c
    db0, db1 = dx0 * (1 - c) + dy0 * c, dx1 * (1 - c) + dy1 * c

    def off(a, b):
        return s + (a & 1) * da0 + (a >> 1) * da1 + (b & 1) * db0 + (b >> 1) * db1

    return off


def rows(index, count):
    return pl.ds(pl.multiple_of(index * count, count), count)


def send(src, dst, ssem, rsem, device):
    return pltpu.make_async_remote_copy(
        src_ref=src, dst_ref=dst, send_sem=ssem, recv_sem=rsem, device_id=device, device_id_type=MESH
    )


def bit_of(bits, b, mask):
    return 1 - bits[b] if mask >> b & 1 else bits[b]


def dot(x, y, dims):
    return lax.dot_general(x, y, (dims, ((), ())), preferred_element_type=F32)


NN, NT, TN = ((1,), (0,)), ((1,), (1,)), ((0,), (0,))
SCALE = 128**-0.5
ORDER = (4, 5, 2, 3, 6, 7, 1)
TILES = ((0, 0), (1, 1), (1, 0))


def step_kernel(
    q_hbm, k_hbm, v_hbm, lam_hbm, proj_hbm, og_hbm,
    out_ref, gq_ref, gk_ref, gv_ref, gl_ref, gp_ref,
    q, k, v, og, ogt, lamt, glt, glrow, lam_in, shard_buf, full, states, score, prob, att32, att, mapped, ga, wt, gk32, gv32,
    tot, col, pair, quad, csum, xin, s3buf, s4buf,
    ubuf, upre, upsum, ucol, asend, uxin, rsend, rcol, usib,
    g32, gbf, gsib, hbuf, rel, fin, gbuf, xg, zf, zsend, zin, zall,
    ld, ag_s, ag_r, c1_s, c1_r, st_s, st_r, x_s, x_r, sib_s, sib_r,
    uh_s, uh_r, u_s, u_r, ux_s, ux_r, ur_s, ur_r, us_s, us_r,
    gs_s, gs_r, rl_s, rl_r, fn_s, fn_r, gx_s, gx_r, z1_s, z1_r, z2_s, z2_r,
):
    s, bits = place()
    c, y0, y1, x0, x1 = bits
    z = lax.axis_index("dp")
    zbits = [lax.rem(lax.div(z, 2**b), 2) for b in range(3)] + [0, 0]
    r = lax.rem(s, COL)
    mine = rows(r, 64)
    off = chip_offsets(s, bits)
    have = [c == 1, y0 == 1, y1 == 1, x0 == 1, x1 == 1]
    sib_index = flipped(s, bits, 1)
    sibling = {"seq": sib_index}

    loads = [
        pltpu.make_async_copy(src, dst, ld.at[i])
        for i, (src, dst) in enumerate(
            ((k_hbm, k), (v_hbm, v), (q_hbm, q), (og_hbm, og), (proj_hbm, shard_buf), (lam_hbm, lam_in))
        )
    ]
    for i in (0, 1, 4, 5, 2):
        loads[i].start()

    greeted = (
        [{"seq": flipped(s, bits, m)} for m in range(1, 8)]
        + [{"seq": flipped(s, bits, m << 3)} for m in range(1, 4)]
        + [{"dp": flipped(z, zbits, m)} for m in range(1, 8)]
    )
    barrier = pltpu.get_barrier_semaphore()
    for device in greeted:
        pl.semaphore_signal(barrier, inc=1, device_id=device, device_id_type=MESH)

    def lanes(h):
        return pl.ds(128 * h, 128)

    loads[0].wait()
    loads[1].wait()
    for h in range(4):
        tot[lanes(h)] = dot(k[:, lanes(h)], v[:, lanes(h)], TN).astype(BF)
    pl.semaphore_wait(barrier, len(greeted))

    loads[3].start()
    first = []
    for m in ORDER:
        peer = flipped(s, bits, m)
        cp = send(tot.at[rows(lax.rem(peer, COL), 64)], col.at[m], c1_s.at[m], c1_r.at[m], {"seq": peer})
        cp.start()
        first.append(cp)
    sib = send(tot, states.at[0], sib_s, sib_r, sibling)

    @pl.when(c == 0)
    def _():
        sib.start()

    open_sends = []

    def block(index):
        return full.at[rows(index, 64)]

    def ag(slot, src, index, device):
        cp = send(src, block(index), ag_s.at[slot], ag_r.at[slot], device)
        cp.start()
        open_sends.append(cp)

    def ag_arrived(slot):
        send(shard_buf, block(s), ag_s.at[slot], ag_r.at[slot], sibling).wait_recv()

    def chip(a, b):
        return flipped(s, bits, a << 1 | b << 3)

    loads[4].wait()
    full[rows(s, 64)] = shard_buf[...]
    starts = {a: send(shard_buf, block(s), ag_s.at[a], ag_r.at[a], {"seq": chip(a, 0)}) for a in (1, 3, 2)}
    open_sends.extend(starts.values())

    odd = zbits[0]
    dz = ({"dp": lax.rem(z + 1, 8)}, {"dp": lax.rem(z + 7, 8)})

    def piece(a, b):
        turn = 1 - odd if a & 1 else odd
        return chip(a & 2, b) + 2 * (1 - 2 * y0) * turn

    along = {}
    for a in (0, 2):
        for b in (1, 3):
            slot = 4 + 4 * a + b
            at = block(piece(a, 0))
            along[a, b] = send(at, at, ag_s.at[slot], ag_r.at[slot], {"seq": chip(0, b)})
            open_sends.append(along[a, b])

    def set_out(*labels):
        for a in labels:
            along[a, 1].start()
            along[a, 3].start()

    @pl.when(odd == 0)
    def _():
        for a in (2, 1, 3):
            starts[a].start()
        set_out(0)

    @pl.when(odd == 1)
    def _():
        for a in (1, 3, 2):
            starts[a].start()

    ag(20, shard_buf, s, sibling)


    row = lax.broadcasted_iota(jnp.int32, (128, 128), 0)
    column = lax.broadcasted_iota(jnp.int32, (128, 128), 1)
    causal = column <= row
    near = causal & ((row < 64) | (column >= 64))
    far = causal & (row >= 64) & (column < 64)

    def half(i):
        return pl.ds(128 * i, 128)

    def lam(level, h, where):
        return lamt[where, pl.ds(4 * level + h, 1)]

    def weight(h, i, j):
        if i != j:
            return SCALE * lam(2, h, half(i))
        return SCALE * jnp.where(near, lam(0, h, half(i)), jnp.where(far, lam(1, h, half(i)), 0.0))

    def inside(h):
        for n, (i, j) in enumerate(TILES):
            value = dot(q[half(i), lanes(h)], k[half(j), lanes(h)], NT)
            score[h, n] = value
            prob[h, n] = (weight(h, i, j) * value).astype(BF)
        att32[half(0), lanes(h)] = dot(prob[h, 0], v[half(0), lanes(h)], NN)
        att32[half(1), lanes(h)] = dot(prob[h, 1], v[half(1), lanes(h)], NN) + dot(
            prob[h, 2], v[half(0), lanes(h)], NN
        )

    loads[5].wait()
    for level in range(8):
        glrow[pl.ds(4 * level, 4)] = lam_in[level]
    lamt[...] = glrow[...].T
    loads[2].wait()
    inside(0)
    inside(1)

    for cp in first:
        cp.wait_recv()
    col[0] = tot[mine]
    t = [col[m].astype(F32) for m in range(COL)]
    p = [t[2 * i] + t[2 * i + 1] for i in range(4)]
    qd = [p[0] + p[1], p[2] + p[3]]
    csum[...] = qd[0] + qd[1]
    xsend = [
        send(csum, xin.at[m], x_s.at[m], x_r.at[m], {"seq": flipped(s, bits, m << 3)}) for m in range(1, 4)
    ]
    x_out = [x0 == 0, x1 == 0, x1 == 0]
    for cp, cond in zip(xsend, x_out):

        @pl.when(cond)
        def _(cp=cp):
            cp.start()

    for i in range(4):
        pair[i] = p[i].astype(BF)
    for i in range(2):
        quad[i] = qd[i].astype(BF)

    def spread(j, m, src):
        return send(src, states.at[j, mine], st_s.at[j, m], st_r.at[j, m], {"seq": flipped(s, bits, m)})

    early = []
    for m in (4, 2, 6, 1):
        early.append((spread(1, m, pair.at[(m >> 1) ^ 1]), bit_of(bits, 1, m) == 1))
        early.append((spread(2, m, quad.at[(m >> 2) ^ 1]), bit_of(bits, 2, m) == 1))
    for cp, cond in early:

        @pl.when(cond)
        def _(cp=cp):
            cp.start()

    def hand_over(j, i):
        at = states.at[j, rows(lax.rem(flipped(s, bits, 2 * i), COL), 64)]
        return send(at, at, st_s.at[j, 2 * i + 1], st_r.at[j, 2 * i + 1], sibling)

    def handed(j):
        for i in (2, 1, 3):
            spread(j, 2 * i, s4buf).wait_recv()
            hand_over(j, i).start()

    for j in range(5):

        @pl.when(jnp.logical_not(have[j]))
        def _(j=j):
            states[j] = jnp.zeros((512, 128), BF)

    @pl.when(have[1])
    def _():
        states[1, mine] = pair[1]

    @pl.when(have[2])
    def _():
        states[2, mine] = quad[1]

    def pass_on(a, b):
        ag(36 + 2 * a + b, block(piece(a, b)), piece(a, b), dz[a >> 1])
        ag(20 + 4 * a + b, block(piece(a, b)), piece(a, b), sibling)

    def second_axis(a):
        for b in (1, 3):
            ag_arrived(4 + 4 * a + b)
            if (b == 1) == (a == 0):
                ag(4 + 4 * a + 2, block(piece(a, b)), piece(a, b), {"seq": chip(0, 4 - b)})
            pass_on(a, b)

    def far_chip(a):
        ag_arrived(4 + 4 * a + 2)
        pass_on(a, 2)

    def other_plane(a, b):
        ag_arrived(36 + 2 * a + b)
        ag(24 + 4 * a + b, block(piece(a + 1, b)), piece(a + 1, b), sibling)

    @pl.when(odd == 1)
    def _():
        ag_arrived(1)
        ag_arrived(3)
        set_out(0, 2)

    @pl.when(odd == 0)
    def _():
        ag_arrived(2)
        set_out(2)

    inside(2)

    late3 = [spread(3, m, s3buf) for m in ORDER]
    late4 = [spread(4, m, s4buf) for m in ORDER]

    @pl.when(have[3])
    def _():
        xsend[0].wait_recv()
        s3buf[...] = xin[1].astype(BF)
        for cp in late3:
            cp.start()
        states[3, mine] = s3buf[...]

    @pl.when(have[4])
    def _():
        xsend[1].wait_recv()
        xsend[2].wait_recv()
        s4buf[...] = (xin[2] + xin[3]).astype(BF)
        for cp in late4:
            cp.start()
        states[4, mine] = s4buf[...]

    @pl.when(odd == 1)
    def _():
        ag_arrived(2)

    @pl.when(odd == 0)
    def _():
        ag_arrived(1)
        ag_arrived(3)

    for a in (1, 3, 2):
        ag(20 + 4 * a, block(chip(a, 0)), chip(a, 0), sibling)

    inside(3)
    loads[3].wait()
    for a in range(4):
        for b in range(4):
            turned = og[:, rows(lax.div(off(a, b), 2), 128)].T
            ogt[0, 0, a, b] = ogt[1, 0, b, a] = turned[:64]
            ogt[0, 1, a, b] = ogt[1, 1, b, a] = turned[64:]

    for j in (1, 2):

        @pl.when(have[j])
        def _(j=j):
            handed(j)

    second_axis(0)
    second_axis(2)

    @pl.when(have[0])
    def _():
        sib.wait_recv()

    for j in range(1, 5):

        @pl.when(have[j])
        def _(j=j):
            for m in (1, 3, 5, 7) if j < 3 else ORDER:
                spread(j, m, s4buf).wait_recv()

    for h in range(4):
        cross = jnp.zeros((256, 128), F32)
        for j in range(5):
            image = dot(q[:, lanes(h)], states[j, lanes(h)], NN)
            mapped[h, j] = image
            cross = cross + lam(3 + j, h, pl.ds(0, 256)) * image
        att[:, lanes(h)] = (att32[:, lanes(h)] + SCALE * cross).astype(BF)

    gs = []

    def exchange(*groups):
        for b in groups:
            gbf[b] = dot(ogt[1, 1 - c, b].reshape(256, 256), att[...], NN).astype(BF).reshape(4, 64, 512)
        for b in groups:
            for a in range(4):
                slot = 4 * b + a
                cp = send(gbf.at[b, a], gsib.at[slot], gs_s.at[slot], gs_r.at[slot], sibling)
                cp.start()
                gs.append(cp)

    exchange(2)
    exchange(1, 3)

    def keep(a):
        g32[a] = dot(ogt[0, c, a].reshape(256, 256), att[...], NN).reshape(4, 64, 512)

    keep(2)

    far_chip(0)
    far_chip(2)

    def h_make(a, b):
        slot = 4 * a + b
        send(gbf.at[0, 0], gsib.at[slot], gs_s.at[slot], gs_r.at[slot], sibling).wait_recv()
        hbuf[a, b] = (g32[a, b] + gsib[slot].astype(F32)).astype(BF)

    dev_a = {1: {"seq": off(1, 0)}, 3: {"seq": off(3, 0)}}
    relayed = []
    for b in (0, 2, 1, 3):
        h_make(2, b)
        cp = send(hbuf.at[2, b], rel.at[b], rl_s.at[b], rl_r.at[b], dev_a[1 if b < 2 else 3])
        cp.start()
        relayed.append(cp)

    keep(1)
    keep(3)
    exchange(0)
    keep(0)
    finals = []

    def final(m, b):
        n = 4 * (m // 2) + b
        cp = send(hbuf.at[m, b], fin.at[m // 2, b], fn_s.at[n], fn_r.at[n], dev_a[m])
        cp.start()
        finals.append(cp)

    for m, b in ((1, 0), (3, 2), (1, 1), (3, 3)):
        h_make(m, b)
        final(m, b)
    for m, b in ((3, 0), (1, 2), (3, 1), (1, 3)):
        h_make(m, b)

    for b in (1, 3, 2):
        other_plane(0, b)
        other_plane(2, b)

    for m, b, cp in zip((3, 1, 3, 1), (0, 2, 1, 3), relayed):
        cp.wait_recv()
        hbuf[m, b] = (hbuf[m, b].astype(F32) + rel[b].astype(F32)).astype(BF)
        final(m, b)

    for a in range(4):
        for b in range(4):
            ag_arrived(20 + 4 * a + b)
    ga[...] = dot(og[...], full[...], NN).astype(BF)
    for h in range(4):
        g = ga[:, lanes(h)].astype(F32)
        for j in range(5):
            wt[h, j] = (SCALE * lam(3 + j, h, pl.ds(0, 256)) * g).astype(BF)
            ubuf[j, lanes(h)] = dot(q[:, lanes(h)], wt[h, j], TN).astype(BF)

    usend = send(ubuf.at[0], usib, us_s, us_r, sibling)

    @pl.when(have[0])
    def _():
        usend.start()

    y = y0 + 2 * y1
    kept = rows(c, 256)
    shared = [
        send(ubuf.at[j, rows(1 - c, 256)], upre.at[j - 1], uh_s.at[j - 1], uh_r.at[j - 1], sibling)
        for j in range(1, 5)
    ]
    for j in (4, 3, 2, 1):

        @pl.when(have[j])
        def _(j=j):
            shared[j - 1].start()

    def slice_to(j, i):
        peer = flipped(s, bits, 2 * i)
        at = rows(lax.div(lax.rem(peer, COL), 2), 64)
        return send(
            upsum.at[j - 1, at], ucol.at[j - 1, i], u_s.at[j - 1, i], u_r.at[j - 1, i], {"seq": peer}
        )

    def spread_updates():
        for j in (4, 3, 2, 1):

            @pl.when(have[j])
            def _(j=j):
                shared[j - 1].wait_recv()
                upsum[j - 1] = (ubuf[j, kept].astype(F32) + upre[j - 1].astype(F32)).astype(BF)
                for i in (2, 1, 3):
                    slice_to(j, i).start()

    place_of = lax.broadcasted_iota(jnp.int32, (128, 128), 1)

    def sums(value):
        return jnp.sum(value, axis=1, keepdims=True)

    def backward(h):
        ds = []
        got = {}
        for n, (i, j) in enumerate(TILES):
            dp = dot(ga[half(i), lanes(h)], v[half(j), lanes(h)], NT)
            ds.append((weight(h, i, j) * dp).astype(BF))
            product = SCALE * score[h, n] * dp
            if i != j:
                got[2, i] = sums(product)
            else:
                got[0, i] = sums(jnp.where(near, product, 0.0))
                got[1, i] = sums(jnp.where(far, product, 0.0))
        for i in range(2):
            g = ga[half(i), lanes(h)].astype(F32)
            acc = glt[half(i)]
            for level in range(8):
                if level > 2:
                    value = SCALE * sums(g * mapped[h, level - 3, half(i)])
                elif (level, i) in got:
                    value = got[level, i]
                else:
                    continue
                acc = jnp.where(place_of == 4 * level + h, value, acc)
            glt[half(i)] = acc
        gq = [dot(ds[0], k[half(0), lanes(h)], NN), dot(ds[1], k[half(1), lanes(h)], NN)]
        gq[1] = gq[1] + dot(ds[2], k[half(0), lanes(h)], NN)
        for i in range(2):
            for j in range(5):
                gq[i] = gq[i] + dot(wt[h, j, half(i)], states[j, lanes(h)], NT)
            gq_ref[half(i), lanes(h)] = gq[i].astype(BF)
        q0, q1 = q[half(0), lanes(h)], q[half(1), lanes(h)]
        g0, g1 = ga[half(0), lanes(h)], ga[half(1), lanes(h)]
        gk32[half(0), lanes(h)] = dot(ds[0], q0, TN) + dot(ds[2], q1, TN)
        gk32[half(1), lanes(h)] = dot(ds[1], q1, TN)
        gv32[half(0), lanes(h)] = dot(prob[h, 0], g0, TN) + dot(prob[h, 2], g1, TN)
        gv32[half(1), lanes(h)] = dot(prob[h, 1], g1, TN)

    glt[...] = jnp.zeros_like(glt)
    backward(0)

    spread_updates()

    backward(1)

    for b in range(4):
        h_make(0, b)
    for cp in finals:
        cp.wait_recv()
    for b in range(4):
        gbuf[b] = (hbuf[0, b].astype(F32) + fin[0, b].astype(F32) + fin[1, b].astype(F32)).astype(BF)
    gx = []
    for b in (2, 1, 3):
        cp = send(gbuf.at[b], xg.at[b], gx_s.at[b], gx_r.at[b], {"seq": off(0, b)})
        cp.start()
        gx.append(cp)

    backward(2)

    for j in range(1, 5):
        for i in range(4):
            cond = bit_of(bits, j, 2 * i) == 1 if j < 3 else have[j]

            @pl.when(cond)
            def _(j=j, i=i):
                if i:
                    slice_to(j, i).wait_recv()
                else:
                    ucol[j - 1, 0] = upsum[j - 1, rows(y, 64)]

            @pl.when(jnp.logical_not(cond))
            def _(j=j, i=i):
                ucol[j - 1, i] = jnp.zeros((64, 128), BF)

    def total(j, chips):
        value = ucol[j - 1, chips[0]].astype(F32)
        for i in chips[1:]:
            value = value + ucol[j - 1, i].astype(F32)
        return value

    asend[0] = total(3, [0, 1, 2, 3])
    asend[1] = total(4, [0, 1, 2, 3])
    ux = [
        send(asend.at[0 if m == 1 else 1], uxin.at[m], ux_s.at[m], ux_r.at[m], {"seq": flipped(s, bits, m << 3)})
        for m in range(1, 4)
    ]
    ux_out = [x0 == 1, x1 == 1, x1 == 1]
    for cp, cond in zip(ux, ux_out):

        @pl.when(cond)
        def _(cp=cp):
            cp.start()

    for cp in gx:
        cp.wait_recv()
    mean = gbuf[0].astype(F32) + xg[1].astype(F32) + xg[2].astype(F32) + xg[3].astype(F32)
    for i in range(8):
        part = mean[16 * (i // 2) : 16 * (i // 2) + 16, 256 * (i % 2) : 256 * (i % 2) + 256]
        zf[i] = part
        zsend[i] = part.astype(BF)
    z1 = []
    for m in ORDER:
        peer = flipped(z, zbits, m)
        cp = send(zsend.at[peer], zin.at[m], z1_s.at[m], z1_r.at[m], {"dp": peer})
        cp.start()
        z1.append(cp)

    backward(3)

    def output(n):
        at = pl.ds(512 * n, 512)
        out_ref[:, at] = dot(att[...], full[at], NT).astype(BF)

    output(0)
    output(1)

    for cp, cond, m in zip(ux, ux_out, range(1, 4)):

        @pl.when(jnp.logical_not(cond))
        def _(cp=cp):
            cp.wait_recv()

        @pl.when(cond)
        def _(m=m):
            uxin[m] = jnp.zeros((64, 128), F32)

    beyond = uxin[1] + uxin[2] + uxin[3]
    for i in range(4):
        n = 2 * ((i >> 1) ^ 1)
        rsend[i] = (beyond + total(1, [i ^ 1]) + total(2, [n, n + 1])).astype(BF)
    owned = rows(4 * c + y, 64)
    rc = []
    for m in ORDER:
        cp = send(rsend.at[m >> 1], rcol.at[owned], ur_s.at[m], ur_r.at[m], {"seq": flipped(s, bits, m)})
        cp.start()
        rc.append(cp)
    rcol[owned] = rsend[0]

    for cp in z1:
        cp.wait_recv()
    value = zf[z]
    for m in range(1, 8):
        value = value + zin[m].astype(F32)
    zall[z] = value.astype(BF)
    z2 = []
    for m in ORDER:
        cp = send(zall.at[z], zall.at[z], z2_s.at[m], z2_r.at[m], {"dp": flipped(z, zbits, m)})
        cp.start()
        z2.append(cp)

    output(2)

    output(3)

    for cp in rc:
        cp.wait_recv()

    @pl.when(c == 0)
    def _():
        usend.wait_recv()

    @pl.when(have[0])
    def _():
        usib[...] = jnp.zeros((512, 128), BF)

    for h in range(4):
        back = (rcol[lanes(h)].astype(F32) + usib[lanes(h)].astype(F32)).astype(BF)
        gk_ref[:, lanes(h)] = (gk32[:, lanes(h)] + dot(v[:, lanes(h)], back, NT)).astype(BF)
        gv_ref[:, lanes(h)] = (gv32[:, lanes(h)] + dot(k[:, lanes(h)], back, NN)).astype(BF)
    glrow[...] = glt[...].T[:32]
    for level in range(8):
        gl_ref[level] = glrow[pl.ds(4 * level, 4)]

    for cp in z2:
        cp.wait_recv()
    for i in range(8):
        gp_ref[pl.ds(16 * (i // 2), 16), pl.ds(256 * (i % 2), 256)] = zall[i].astype(F32)

    for cp in first + open_sends + gs + relayed + finals + rc + gx + z1 + z2:
        cp.wait_send()
    for cp, cond in early + list(zip(xsend, x_out)) + list(zip(ux, ux_out)):

        @pl.when(cond)
        def _(cp=cp):
            cp.wait_send()

    @pl.when(c == 0)
    def _():
        sib.wait_send()

    @pl.when(have[0])
    def _():
        usend.wait_send()

    for j in range(1, 5):

        @pl.when(have[j])
        def _(j=j):
            shared[j - 1].wait_send()
            for i in (2, 1, 3):
                slice_to(j, i).wait_send()
            for cp in {3: late3, 4: late4}.get(j) or [hand_over(j, i) for i in (2, 1, 3)]:
                cp.wait_send()


def step(query, key, value, lam, proj, grad_out):
    dma = pltpu.SemaphoreType.DMA
    outer = pl.BlockSpec(memory_space=pltpu.HBM)
    inner = pl.BlockSpec(memory_space=pltpu.VMEM)
    wide = (256, 512)
    return pl.pallas_call(
        step_kernel,
        out_shape=(
            jax.ShapeDtypeStruct((256, 2048), BF),
            jax.ShapeDtypeStruct(wide, BF),
            jax.ShapeDtypeStruct(wide, BF),
            jax.ShapeDtypeStruct(wide, BF),
            jax.ShapeDtypeStruct((8, 4, 256), F32),
            jax.ShapeDtypeStruct((64, 512), F32),
        ),
        in_specs=[outer] * 6,
        out_specs=(inner,) * 6,
        scratch_shapes=[
            pltpu.VMEM(wide, BF), pltpu.VMEM(wide, BF), pltpu.VMEM(wide, BF),
            pltpu.VMEM((256, 2048), BF),
            pltpu.VMEM((2, 2, 4, 4, 64, 256), BF),
            pltpu.VMEM((256, 32), F32),
            pltpu.VMEM((256, 128), F32),
            pltpu.VMEM((32, 256), F32),
            pltpu.VMEM((8, 4, 256), F32),
            pltpu.VMEM((64, 512), BF),
            pltpu.VMEM((2048, 512), BF),
            pltpu.VMEM((5, 512, 128), BF),
            pltpu.VMEM((4, 3, 128, 128), F32),
            pltpu.VMEM((4, 3, 128, 128), BF),
            pltpu.VMEM(wide, F32),
            pltpu.VMEM(wide, BF),
            pltpu.VMEM((4, 5, 256, 128), F32),
            pltpu.VMEM(wide, BF),
            pltpu.VMEM((4, 5, 256, 128), BF),
            pltpu.VMEM(wide, F32),
            pltpu.VMEM(wide, F32),
            pltpu.VMEM((512, 128), BF),
            pltpu.VMEM((COL, 64, 128), BF),
            pltpu.VMEM((4, 64, 128), BF),
            pltpu.VMEM((2, 64, 128), BF),
            pltpu.VMEM((64, 128), F32),
            pltpu.VMEM((4, 64, 128), F32),
            pltpu.VMEM((64, 128), BF),
            pltpu.VMEM((64, 128), BF),
            pltpu.VMEM((5, 512, 128), BF),
            pltpu.VMEM((4, 256, 128), BF),
            pltpu.VMEM((4, 256, 128), BF),
            pltpu.VMEM((4, 4, 64, 128), BF),
            pltpu.VMEM((2, 64, 128), F32),
            pltpu.VMEM((4, 64, 128), F32),
            pltpu.VMEM((4, 64, 128), BF),
            pltpu.VMEM((512, 128), BF),
            pltpu.VMEM((512, 128), BF),
            pltpu.VMEM((4, 4, 64, 512), F32),
            pltpu.VMEM((4, 4, 64, 512), BF),
            pltpu.VMEM((PIECES, 64, 512), BF),
            pltpu.VMEM((4, 4, 64, 512), BF),
            pltpu.VMEM((4, 64, 512), BF),
            pltpu.VMEM((2, 4, 64, 512), BF),
            pltpu.VMEM((4, 64, 512), BF),
            pltpu.VMEM((4, 64, 512), BF),
            pltpu.VMEM((8, 16, 256), F32),
            pltpu.VMEM((8, 16, 256), BF),
            pltpu.VMEM((8, 16, 256), BF),
            pltpu.VMEM((8, 16, 256), BF),
            dma((6,)),
            dma((44,)), dma((44,)), dma((COL,)), dma((COL,)),
            dma((5, COL)), dma((5, COL)), dma((4,)), dma((4,)), dma, dma,
            dma((4,)), dma((4,)), dma((4, 4)), dma((4, 4)), dma((4,)), dma((4,)), dma((COL,)), dma((COL,)), dma, dma,
            dma((PIECES,)), dma((PIECES,)), dma((4,)), dma((4,)), dma((8,)), dma((8,)),
            dma((4,)), dma((4,)), dma((8,)), dma((8,)), dma((8,)), dma((8,)),
        ],
        compiler_params=pltpu.CompilerParams(collective_id=0, has_side_effects=True, vmem_limit_bytes=36 * 2**20),
        name="span_step",
    )(query, key, value, lam, proj, grad_out)


def deliver_kernel(*refs):
    count = len(refs) // 2
    sems = refs[-1]
    copies = [pltpu.make_async_copy(refs[i], refs[count + i], sems.at[i]) for i in range(count)]
    for cp in copies:
        cp.start()
    for cp in copies:
        cp.wait()


def deliver(arrays):
    return pl.pallas_call(
        deliver_kernel,
        out_shape=[jax.ShapeDtypeStruct(x.shape, x.dtype) for x in arrays],
        in_specs=[pl.BlockSpec(memory_space=pltpu.VMEM)] * len(arrays),
        out_specs=[pl.BlockSpec(memory_space=pltpu.HBM)] * len(arrays),
        scratch_shapes=[pltpu.SemaphoreType.DMA((len(arrays),))],
        compiler_params=pltpu.CompilerParams(vmem_limit_bytes=2**20),
        name="deliver",
    )(*arrays)


def shards(queries, keys, values, level_weights, proj, out_grad):
    out, gq, gk, gv, gl, gp = deliver(
        step(
            *[
                pltpu.with_memory_space_constraint(x, pltpu.HBM)
                for x in (queries[0], keys[0], values[0], level_weights[0], proj.T, out_grad[0])
            ]
        )
    )
    return out[None], gq[None], gk[None], gv[None], gl[None], gp.T


def solution(mesh):
    return jax.shard_map(
        shards,
        mesh=mesh,
        in_specs=(
            P("dp", "seq", None),
            P("dp", "seq", None),
            P("dp", "seq", None),
            P("dp", None, None, "seq"),
            P(None, "seq"),
            P("dp", "seq", None),
        ),
        out_specs=(
            P("dp", "seq", None),
            P("dp", "seq", None),
            P("dp", "seq", None),
            P("dp", "seq", None),
            P("dp", None, None, "seq"),
            P(None, "seq"),
        ),
        check_vma=False,
    )
```
